32 devices in a mesh: row: 8 (over z, x), col: 4 (over y, core).
Axes of the slice: x: 2, y: 2, z: 4, core: 2. Of those that a mesh axis runs over, the one named last changes fastest.
Arguments:
- offsets: int32 [8, 4, 2], P('row', 'col'), may hold values from 1 to 3
- targets: float32 [3, 3, 256, 512], P(None, None, 'row', 'col'), may hold values from -60 to 60
- grid_fine: float32 [32, 256, 512], P(None, 'row', 'col'), may hold values from -6 to 6
- grid_coarse: float32 [32, 64, 128], P(None, 'row', 'col'), may hold values from -6 to 6
- weight_in: float32 [512, 64], replicated, may hold values from -0.75 to 0.75
- weight_mid: float32 [1, 512, 512], replicated, may hold values from -0.25 to 0.25
- weight_out: float32 [3, 512], replicated, may hold values from -0.397747564 to 0.397747564
- fine_first: float32 [32, 256, 512], P(None, 'row', 'col'), may hold values from -0.012 to 0.012
- fine_second: float32 [32, 256, 512], P(None, 'row', 'col'), may hold values from 1e-06 to 0.0001
- coarse_first: float32 [32, 64, 128], P(None, 'row', 'col'), may hold values from -0.012 to 0.012
- coarse_second: float32 [32, 64, 128], P(None, 'row', 'col'), may hold values from 1e-06 to 0.0001
- in_first: float32 [512, 64], replicated, may hold values from -0.012 to 0.012
- in_second: float32 [512, 64], replicated, may hold values from 1e-06 to 0.0001
- mid_first: float32 [1, 512, 512], replicated, may hold values from -0.012 to 0.012
- mid_second: float32 [1, 512, 512], replicated, may hold values from 1e-06 to 0.0001
- out_first: float32 [3, 512], replicated, may hold values from -0.012 to 0.012
- out_second: float32 [3, 512], replicated, may hold values from 1e-06 to 0.0001
Outputs:
- fine_step: float32 [32, 256, 512], P(None, 'row', 'col')
- coarse_step: float32 [32, 64, 128], P(None, 'row', 'col')
- input_step: float32 [512, 64], replicated
- middle_step: float32 [1, 512, 512], replicated
- output_step: float32 [3, 512], replicated
The draws below stay inside these ranges and needn't reach their ends.
All inputs are finite; a program needn't handle non-finite values.
Results may differ from the reference program's by a relative error of at most 0.0014.
The reference program's roundings to bfloat16 on the way count: a program that leaves them out, or rounds other values in their place, can miss the bound.
Values sent between devices are 32-bit elements; how exact they have to be, the bound alone decides.
A program may use at most 64 MiB of HBM per device.

```python
import math
import jax
import jax.numpy as jnp
from jax import lax

CH = 32
HID = 512
MID = 1
OUT = 3
SUB = 4
RATIO = 4
ADAM_STEP = 10
SR = 32
SC = 128
TILE_ROWS = 8
TILE_COLS = 4
ROWS = 256
COLS = 512
CROWS = 64
CCOLS = 128
N_ROW = 8
N_COL = 4


def draw_targets(key, part):
    row_level = jnp.arange(ROWS, dtype=jnp.float32) / ROWS
    col_level = jnp.arange(COLS, dtype=jnp.float32) / COLS
    exponent = 0.5 * (row_level[:, None] + col_level[None, :])
    noise = jnp.clip(jax.random.normal(key, (3, OUT, ROWS, COLS), jnp.float32), -4.0, 4.0)
    return noise * 10.0 ** exponent


def draw_weight_out(key, part):
    column_level = 0.3 * 10.0 ** (jnp.arange(HID, dtype=jnp.float32) / (HID - 1))
    noise = jnp.clip(jax.random.normal(key, (OUT, HID), jnp.float32), -3.0, 3.0)
    return noise * column_level[None, :] / HID ** 0.5


def set_ends(values, key, least, top_value):
    extent = values.shape
    index_at = [jax.random.randint(jax.random.fold_in(key, axis), (), 0, extent[axis]) for axis in range(len(extent))]
    values = values.at[tuple(index_at)].set(least)
    longest = extent.index(max(extent))
    index_at[longest] = (index_at[longest] + 1) % extent[longest]
    return values.at[tuple(index_at)].set(top_value)


def block_levels(key, extent, pieces, smallest, top_value):
    level = 1.0
    for axis_at, parts in pieces:
        steps = jax.random.uniform(jax.random.fold_in(jax.random.fold_in(key, 6), axis_at), (parts,), jnp.float32, smallest / len(pieces), top_value / len(pieces))
        level = level * jnp.repeat(jnp.exp(steps), extent[axis_at] // parts).reshape((-1,) + (1,) * (len(extent) - 1 - axis_at))
    return level


def scatter_about(own_key, dims, deviation, reach, split=(), held_as=jnp.bfloat16):
    result = deviation * jax.random.normal(own_key, dims, jnp.float32)
    if split:
        result = result * block_levels(own_key, dims, split, -0.22, 0.18)
    return jnp.clip(result, -reach, reach).astype(held_as)


def setup_inputs(seed: int = 0) -> dict:
    key_of = jax.random.split(jax.random.key(seed), 18)
    return {
        "offsets": set_ends(jax.random.randint(key_of[0], (TILE_ROWS, TILE_COLS, 2), 1, SUB), jax.random.fold_in(key_of[0], 1), 1, SUB - 1).astype(jnp.int32),
        "targets": draw_targets(jax.random.fold_in(key_of[17], 71), 0),
        "grid_fine": scatter_about(key_of[2], (CH, ROWS, COLS), 1.0, 6.0, ((1, 8), (2, 4)), jnp.float32),
        "grid_coarse": scatter_about(key_of[3], (CH, CROWS, CCOLS), 1.0, 6.0, ((1, 8), (2, 4)), jnp.float32),
        "weight_in": scatter_about(key_of[4], (HID, 2 * CH), (2 * CH) ** -0.5, 0.75, (), jnp.float32),
        "weight_mid": scatter_about(key_of[5], (MID, HID, HID), HID ** -0.5, 0.25, (), jnp.float32),
        "weight_out": draw_weight_out(jax.random.fold_in(key_of[17], 71), 0),
        "fine_first": scatter_about(key_of[7], (CH, ROWS, COLS), 0.002, 0.012, ((1, 8), (2, 4)), jnp.float32),
        "fine_second": jnp.clip(jnp.exp(math.log(0.0001) - 4.6051702 * jax.random.uniform(key_of[8], (CH, ROWS, COLS), jnp.float32) ** block_levels(key_of[8], (CH, ROWS, COLS), ((1, 8), (2, 4)), -0.2, 0.2)), 9.999999974752427e-07, 0.0001),
        "coarse_first": scatter_about(key_of[9], (CH, CROWS, CCOLS), 0.002, 0.012, ((1, 8), (2, 4)), jnp.float32),
        "coarse_second": jnp.clip(jnp.exp(math.log(0.0001) - 4.6051702 * jax.random.uniform(key_of[10], (CH, CROWS, CCOLS), jnp.float32) ** block_levels(key_of[10], (CH, CROWS, CCOLS), ((1, 8), (2, 4)), -0.2, 0.2)), 9.999999974752427e-07, 0.0001),
        "in_first": scatter_about(key_of[11], (HID, 2 * CH), 0.002, 0.012, (), jnp.float32),
        "in_second": jnp.clip(jnp.exp(jax.random.uniform(key_of[12], (HID, 2 * CH), jnp.float32, math.log(9.999999974752427e-07), math.log(0.0001))), 9.999999974752427e-07, 0.0001),
        "mid_first": scatter_about(key_of[13], (MID, HID, HID), 0.002, 0.012, (), jnp.float32),
        "mid_second": jnp.clip(jnp.exp(jax.random.uniform(key_of[14], (MID, HID, HID), jnp.float32, math.log(9.999999974752427e-07), math.log(0.0001))), 9.999999974752427e-07, 0.0001),
        "out_first": scatter_about(key_of[15], (OUT, HID), 0.002, 0.012, (), jnp.float32),
        "out_second": jnp.clip(jnp.exp(jax.random.uniform(key_of[16], (OUT, HID), jnp.float32, math.log(9.999999974752427e-07), math.log(0.0001))), 9.999999974752427e-07, 0.0001),
    }


BETA_ONE = 0.9
BETA_TWO = 0.99
ADAM_EPSILON = 1e-08
CLIP_RMS = 0.01
LOSS_VALUE = 0.25
MEAN_EPSILON = 1e-06

def interp_table(samples, level_ratio, offset):
    positions = jnp.arange(samples, dtype=jnp.int32)
    base_index = positions // level_ratio
    fraction = ((positions % level_ratio).astype(jnp.float32) + offset.astype(jnp.float32) / SUB) / level_ratio
    column = jnp.arange(samples // level_ratio + 1, dtype=jnp.int32)
    lower_hit = (column[None, :] == base_index[:, None]).astype(jnp.float32)
    upper_hit = (column[None, :] == base_index[:, None] + 1).astype(jnp.float32)
    return lower_hit * (1.0 - fraction)[:, None] + upper_hit * fraction[:, None]

def level_tables(row_count, col_count, shift_y, shift_x):
    return (interp_table(row_count, 1, shift_y), interp_table(col_count, 1, shift_x), interp_table(row_count, RATIO, shift_y), interp_table(col_count, RATIO, shift_x))

def sample_level(extended, row_table, col_table):
    across = jnp.einsum('kjl,ml->kjm', extended, col_table, precision=lax.Precision.HIGHEST)
    return jnp.einsum('ij,kjm->kim', row_table, across, precision=lax.Precision.HIGHEST)

def spread_level(cotangent, row_table, col_table):
    backward = jnp.einsum('ij,kim->kjm', row_table, cotangent, precision=lax.Precision.HIGHEST)
    return jnp.einsum('kjm,ml->kjl', backward, col_table, precision=lax.Precision.HIGHEST)

def sample_features(fine_ext, coarse_ext, tables):
    fine_feat = sample_level(fine_ext, tables[0], tables[1])
    coarse_feat = sample_level(coarse_ext, tables[2], tables[3])
    channels, row_count, col_count = fine_feat.shape
    return jnp.concatenate([fine_feat.reshape(channels, row_count * col_count), coarse_feat.reshape(channels, row_count * col_count)], axis=0).astype(jnp.bfloat16)

def spread_features(feature_grad, tables):
    channels = feature_grad.shape[0] // 2
    row_count = tables[0].shape[0]
    col_count = tables[1].shape[0]
    fine_cot = feature_grad[:channels].reshape(channels, row_count, col_count)
    coarse_cot = feature_grad[channels:].reshape(channels, row_count, col_count)
    return (spread_level(fine_cot, tables[0], tables[1]), spread_level(coarse_cot, tables[2], tables[3]))

def matmul(former, latter):
    return jnp.dot(former, latter, preferred_element_type=jnp.float32)

def contract_rows(former, latter):
    return lax.dot_general(former, latter, (((0,), (0,)), ((), ())), preferred_element_type=jnp.float32)

def contract_cols(former, latter):
    return lax.dot_general(former, latter, (((1,), (1,)), ((), ())), preferred_element_type=jnp.float32)

def silu_slope(pre_act):
    sigmoid = jax.nn.sigmoid(pre_act)
    return sigmoid * (1.0 + pre_act * (1.0 - sigmoid))

def decoder_forward(features, low_in, low_mid, low_out):
    pre_acts = [matmul(low_in, features)]
    activations = [jax.nn.silu(pre_acts[0]).astype(jnp.bfloat16)]
    for layer_index in range(low_mid.shape[0]):
        pre_acts.append(matmul(low_mid[layer_index], activations[-1]))
        activations.append(jax.nn.silu(pre_acts[-1]).astype(jnp.bfloat16))
    return (matmul(low_out, activations[-1]), pre_acts, activations)

def decoder_backward(features, pre_acts, activations, cotangent, low_in, low_mid, low_out):
    out_cotangent = cotangent.astype(jnp.bfloat16)
    grad_out = contract_cols(out_cotangent, activations[-1])
    upward = contract_rows(low_out, out_cotangent)
    grads_mid = []
    for layer_index in range(low_mid.shape[0] - 1, -1, -1):
        delta_low = (upward * silu_slope(pre_acts[layer_index + 1])).astype(jnp.bfloat16)
        grads_mid.insert(0, contract_cols(delta_low, activations[layer_index]))
        upward = contract_rows(low_mid[layer_index], delta_low)
    delta_low = (upward * silu_slope(pre_acts[0])).astype(jnp.bfloat16)
    grad_in = contract_cols(delta_low, features)
    feature_grad = contract_rows(low_in, delta_low)
    return (grad_in, jnp.stack(grads_mid), grad_out, feature_grad)

def pixel_cotangent(value_error, row_error, row_prior, col_error, col_prior):
    return 2.0 * LOSS_VALUE * value_error + 2.0 * (row_prior - row_error) + 2.0 * (col_prior - col_error)

def clip_factor(total, entries):
    return jnp.minimum(1.0, CLIP_RMS / jnp.sqrt(total / entries + MEAN_EPSILON))

def adam_step(gradient, moment_one, moment_two, clip_scale):
    clipped = gradient * clip_scale
    new_one = BETA_ONE * moment_one + (1.0 - BETA_ONE) * clipped
    new_two = BETA_TWO * moment_two + (1.0 - BETA_TWO) * clipped * clipped
    return new_one / (1.0 - BETA_ONE ** ADAM_STEP) / (jnp.sqrt(new_two / (1.0 - BETA_TWO ** ADAM_STEP)) + ADAM_EPSILON)

def reference(offsets, targets, grid_fine, grid_coarse, weight_in, weight_mid, weight_out, fine_first, fine_second, coarse_first, coarse_second, in_first, in_second, mid_first, mid_second, out_first, out_second):
    tile_count = N_ROW * N_COL
    coarse_tile_rows = SR // RATIO
    coarse_tile_cols = SC // RATIO
    fine_padded = jnp.pad(grid_fine, ((0, 0), (0, 1), (0, 1)))
    coarse_padded = jnp.pad(grid_coarse, ((0, 0), (0, 1), (0, 1)))
    low_in = weight_in.astype(jnp.bfloat16)
    low_mid = weight_mid.astype(jnp.bfloat16)
    low_out = weight_out.astype(jnp.bfloat16)
    zero_index = jnp.zeros((), jnp.int32)

    def tile_starts(tile_index):
        row_tile = (tile_index // N_COL).astype(jnp.int32)
        col_tile = (tile_index % N_COL).astype(jnp.int32)
        return (row_tile, col_tile)

    def tile_forward(tile_index):
        row_tile, col_tile = tile_starts(tile_index)
        fine_ext = lax.dynamic_slice(fine_padded, (zero_index, row_tile * SR, col_tile * SC), (CH, SR + 1, SC + 1))
        coarse_ext = lax.dynamic_slice(coarse_padded, (zero_index, row_tile * coarse_tile_rows, col_tile * coarse_tile_cols), (CH, coarse_tile_rows + 1, coarse_tile_cols + 1))
        tables = level_tables(SR, SC, offsets[row_tile, col_tile, 0], offsets[row_tile, col_tile, 1])
        features = sample_features(fine_ext, coarse_ext, tables)
        predicted, pre_acts, activations = decoder_forward(features, low_in, low_mid, low_out)
        return (predicted, features, pre_acts, activations, tables)
    tile_range = jnp.arange(tile_count, dtype=jnp.int32)
    tile_preds = lax.map(lambda tile_index: tile_forward(tile_index)[0], tile_range)
    predicted = tile_preds.reshape(N_ROW, N_COL, OUT, SR, SC).transpose(2, 0, 3, 1, 4).reshape(OUT, ROWS, COLS)
    value_error = predicted - targets[0]
    row_error = jnp.pad(predicted[:, 1:, :] - predicted[:, :-1, :] - targets[1][:, :-1, :], ((0, 0), (0, 1), (0, 0)))
    col_error = jnp.pad(predicted[:, :, 1:] - predicted[:, :, :-1] - targets[2][:, :, :-1], ((0, 0), (0, 0), (0, 1)))
    row_prior = jnp.pad(row_error[:, :-1, :], ((0, 0), (1, 0), (0, 0)))
    col_prior = jnp.pad(col_error[:, :, :-1], ((0, 0), (0, 0), (1, 0)))
    cotangent = pixel_cotangent(value_error, row_error, row_prior, col_error, col_prior)
    tile_cots = cotangent.reshape(OUT, N_ROW, SR, N_COL, SC).transpose(1, 3, 0, 2, 4).reshape(tile_count, OUT, SR * SC)

    def tile_backward(running, inputs):
        tile_index, tile_cot = inputs
        unused_pred, features, pre_acts, activations, tables = tile_forward(tile_index)
        grad_in, grad_mid, grad_out, feature_grad = decoder_backward(features, pre_acts, activations, tile_cot, low_in, low_mid, low_out)
        fine_back, coarse_back = spread_features(feature_grad, tables)
        sum_in, sum_mid, sum_out, fine_acc, coarse_acc = running
        row_tile, col_tile = tile_starts(tile_index)
        fine_start = (zero_index, row_tile * SR, col_tile * SC)
        coarse_start = (zero_index, row_tile * coarse_tile_rows, col_tile * coarse_tile_cols)
        fine_acc = lax.dynamic_update_slice(fine_acc, lax.dynamic_slice(fine_acc, fine_start, fine_back.shape) + fine_back, fine_start)
        coarse_acc = lax.dynamic_update_slice(coarse_acc, lax.dynamic_slice(coarse_acc, coarse_start, coarse_back.shape) + coarse_back, coarse_start)
        return ((sum_in + grad_in, sum_mid + grad_mid, sum_out + grad_out, fine_acc, coarse_acc), None)
    initial = (jnp.zeros(weight_in.shape, jnp.float32), jnp.zeros(weight_mid.shape, jnp.float32), jnp.zeros(weight_out.shape, jnp.float32), jnp.zeros((CH, ROWS + 1, COLS + 1), jnp.float32), jnp.zeros((CH, CROWS + 1, CCOLS + 1), jnp.float32))
    finals, unused_stack = lax.scan(tile_backward, initial, (tile_range, tile_cots))
    grad_in, grad_mid, grad_out, fine_acc, coarse_acc = finals
    fine_grad = fine_acc[:, :ROWS, :COLS]
    coarse_grad = coarse_acc[:, :CROWS, :CCOLS]
    grid_total = jnp.sum(fine_grad * fine_grad) + jnp.sum(coarse_grad * coarse_grad)
    grid_scale = clip_factor(grid_total, CH * (ROWS * COLS + CROWS * CCOLS))
    decoder_total = jnp.sum(grad_in * grad_in) + jnp.sum(grad_mid * grad_mid) + jnp.sum(grad_out * grad_out)
    decoder_scale = clip_factor(decoder_total, weight_in.size + weight_mid.size + weight_out.size)
    fine_step = adam_step(fine_grad, fine_first, fine_second, grid_scale)
    coarse_step = adam_step(coarse_grad, coarse_first, coarse_second, grid_scale)
    input_step = adam_step(grad_in, in_first, in_second, decoder_scale)
    middle_step = adam_step(grad_mid, mid_first, mid_second, decoder_scale)
    output_step = adam_step(grad_out, out_first, out_second, decoder_scale)
    return (fine_step, coarse_step, input_step, middle_step, output_step)
```

```python
import functools

import jax
import jax.numpy as jnp
from jax import lax
from jax.experimental import pallas as pl
from jax.experimental.pallas import tpu as pltpu
from jax.sharding import PartitionSpec as P

SUB = 4
RATIO = 4
ADAM_STEP = 10
BETA_ONE = 0.9
BETA_TWO = 0.99
ADAM_EPSILON = 1e-08
CLIP_RMS = 0.01
LOSS_VALUE = 0.25
MEAN_EPSILON = 1e-06

MESH = pl.DeviceIdType.MESH
LANES = 128
SUBLANES = 8
F32 = jnp.float32
BF16 = jnp.bfloat16


def clip_factor(total, entries):
    return jnp.minimum(1.0, CLIP_RMS / jnp.sqrt(total / entries + MEAN_EPSILON))


def adam_step(gradient, moment_one, moment_two, clip_scale):
    clipped = gradient * clip_scale
    new_one = BETA_ONE * moment_one + (1.0 - BETA_ONE) * clipped
    new_two = BETA_TWO * moment_two + (1.0 - BETA_TWO) * clipped * clipped
    return (
        new_one
        / (1.0 - BETA_ONE**ADAM_STEP)
        / (jnp.sqrt(new_two / (1.0 - BETA_TWO**ADAM_STEP)) + ADAM_EPSILON)
    )


def dot(former, latter, dims=((1,), (0,)), precision=None):
    return lax.dot_general(
        former, latter, (dims, ((), ())), preferred_element_type=F32, precision=precision
    )


def dot_t(former, latter, precision=None):
    return dot(former, latter, ((1,), (1,)), precision)


def gate(pre_act):
    sigmoid = 0.5 * jnp.tanh(0.5 * pre_act) + 0.5
    act = pre_act * sigmoid
    return act, sigmoid + act * (1.0 - sigmoid)


class Axis:
    def __init__(self, me, size, device):
        self.me, self.size, self.device = me, size, device

    def peer(self, step):
        return lax.rem(self.me + step, self.size)


def aligned(start):
    return pl.multiple_of(start, SUBLANES)


class Links:
    def __init__(self, send, recv):
        self.send, self.recv, self.used = send, recv, 0

    def take(self, count):
        first = self.used
        self.used += count
        return first

    def copy(self, source, target, device, slot):
        return pltpu.make_async_remote_copy(
            src_ref=source,
            dst_ref=target,
            send_sem=self.send.at[slot],
            recv_sem=self.recv.at[slot],
            device_id=device,
            device_id_type=MESH,
        )


class Scatter:
    def __init__(self, links, own, start, rows, axes, lands):
        self.links, self.own, self.axes, self.lands = links, own, axes, lands
        self.spans = [(start, rows)]
        for axis in axes:
            start, rows = self.spans[-1]
            part = rows // axis.size
            self.spans.append((start + axis.me * part, part))
        self.slots = [links.take(axis.size - 1) for axis in axes]

    def copies(self, stage):
        axis, land = self.axes[stage], self.lands[stage]
        start = self.spans[stage][0]
        part = self.spans[stage + 1][1]
        found = []
        for step in range(1, axis.size):
            peer = axis.peer(step)
            found.append(
                self.links.copy(
                    self.own.at[pl.ds(aligned(start + peer * part), part)],
                    land.at[step - 1],
                    axis.device(peer),
                    self.slots[stage] + step - 1,
                )
            )
        return found

    def start(self, stage):
        for copy in self.copies(stage):
            copy.start()

    def finish(self, stage):
        start, part = self.spans[stage + 1]
        span = pl.ds(aligned(start), part)
        for step, copy in enumerate(self.copies(stage)):
            copy.wait()
            self.own[span] += self.lands[stage][step]


class Gather:
    def __init__(self, scatter, full):
        self.scatter, self.full = scatter, full
        self.slots = [scatter.links.take(axis.size - 1) for axis in scatter.axes]

    def place(self):
        start, rows = self.scatter.spans[-1]
        span = pl.ds(aligned(start), rows)
        self.full[span] = self.scatter.own[span]

    def copies(self, stage):
        axis = self.scatter.axes[stage]
        start, rows = self.scatter.spans[stage + 1]
        block = self.full.at[pl.ds(aligned(start), rows)]
        return [
            self.scatter.links.copy(
                block, block, axis.device(axis.peer(step)), self.slots[stage] + step - 1
            )
            for step in range(1, axis.size)
        ]

    def start(self, stage):
        for copy in self.copies(stage):
            copy.start()

    def finish(self, stage):
        for copy in self.copies(stage):
            copy.wait()


def step_kernel(dims, *refs):
    refs = iter(refs)
    take = lambda count: [next(refs) for _ in range(count)]
    (offsets_ref,) = take(1)
    early_hbm = take(6)
    late_hbm = take(10)
    fine_out, coarse_out, in_out, mid_out, out_out = take(5)
    targets, fine, coarse, w_in, w_mid, w_out = early = take(6)
    late = take(10)
    (
        up_buf,
        cp_buf,
        below_buf,
        right_cp,
        diag_cp,
        coarse_s,
        across,
        across_c,
        b_in,
        b_in_t,
        b_mid,
        b_mid_t,
        b_out,
        b_out_t,
        feats,
        act_0,
        act_1,
        slope_0,
        slope_1,
        delta_1,
        pred,
        edge_send,
        edge_recv,
        cot_s,
        fgrad,
        down_buf,
        q_buf,
        above_buf,
        left_q,
        diag_q,
        fine_g,
        coarse_g,
        grad_in,
        grad_out,
        mid_away,
        mid_own,
        mid_pair,
        mid_full,
        rest_away,
        rest_own,
        rest_pair,
        rest_full,
        total_mine,
        total_land,
    ) = take(44)
    lands = take(12)
    load_sem, send_sem, recv_sem = take(3)

    rows_n, cols_n = lax.axis_size("row"), lax.axis_size("col")
    row, col = lax.axis_index("row"), lax.axis_index("col")
    CH, SR, SC, CR, CC, HID, OUT = (dims[k] for k in ("CH", "SR", "SC", "CR", "CC", "HID", "OUT"))
    S = SR * SC
    CHUNK = RATIO * SC
    CHUNKS = SR // RATIO

    core, plane = lax.rem(col, 2), lax.div(col, 2)
    x_at, z_at = lax.rem(row, 2), lax.div(row, 2)
    axis_core = Axis(core, 2, lambda p: (row, plane * 2 + p))
    axis_x = Axis(x_at, 2, lambda p: (z_at * 2 + p, col))
    axis_y = Axis(plane, cols_n // 2, lambda p: (row, p * 2 + core))
    axis_z = Axis(z_at, rows_n // 2, lambda p: (p * 2 + x_at, col))
    axes = (axis_core, axis_x, axis_y, axis_z)

    has_up, has_down = row > 0, row < rows_n - 1
    has_left, has_right = col > 0, col < cols_n - 1
    near = {
        "up": (has_up, (row - 1, col)),
        "down": (has_down, (row + 1, col)),
        "left": (has_left, (row, col - 1)),
        "right": (has_right, (row, col + 1)),
        "up_left": (jnp.logical_and(has_up, has_left), (row - 1, col - 1)),
        "down_right": (jnp.logical_and(has_down, has_right), (row + 1, col + 1)),
    }
    links = Links(send_sem, recv_sem)

    loads = [
        pltpu.make_async_copy(source, target, load_sem.at[place])
        for place, (source, target) in enumerate(zip(early_hbm + late_hbm, early + late))
    ]
    loads_early, loads_late = loads[:6], loads[6:]
    for place in (1, 2, 3, 4, 5, 0):
        loads_early[place].start()
    barrier = pltpu.get_barrier_semaphore()
    expected = sum(axis.size - 1 for axis in axes)
    for axis in axes:
        for step in range(1, axis.size):
            pl.semaphore_signal(
                barrier, inc=1, device_id=axis.device(axis.peer(step)), device_id_type=MESH
            )
    for there, device in near.values():
        expected = expected + there.astype(jnp.int32)

        @pl.when(there)
        def _():
            pl.semaphore_signal(barrier, inc=1, device_id=device, device_id_type=MESH)

    for load in loads_late:
        load.start()

    lane = lax.broadcasted_iota(jnp.int32, (CH, LANES), 1)
    lane_8 = lax.broadcasted_iota(jnp.int32, (SUBLANES, LANES), 1)
    off_y = offsets_ref[0, 0, 0].astype(F32) / SUB
    off_x = offsets_ref[0, 0, 1].astype(F32) / SUB

    def fine_row(r):
        return fine[pl.ds(r, CH, stride=SR), :]

    def roll(value, shift):
        return pltpu.roll(value, shift % LANES, 1)

    coarse_s[...] = jnp.zeros(coarse_s.shape, F32)
    up_buf[...] = jnp.zeros(up_buf.shape, F32)
    loads_early[1].wait()
    loads_early[2].wait()
    for r in range(CR):
        coarse_s[r, :, :CC] = coarse[pl.ds(r, CH, stride=CR), :]
    up_buf[0] = fine_row(0)
    up_buf[1] = coarse_s[0]
    packed = jnp.zeros((CH, LANES), F32)
    for r in range(SR):
        packed = jnp.where(lane == r, roll(fine_row(r), r), packed)
    for r in range(CR):
        packed = jnp.where(lane == SR + r, roll(coarse_s[r], SR + r), packed)
    cp_buf[...] = packed

    pl.semaphore_wait(barrier, expected)

    def halo(source, target, towards, back):
        slot = links.take(1)
        copy = links.copy(source, target, near[towards][1], slot)
        arriving = links.copy(source, target, near[back][1], slot)

        @pl.when(near[towards][0])
        def _():
            copy.start()

        def finish():
            @pl.when(near[towards][0])
            def _():
                copy.wait_send()

            @pl.when(near[back][0])
            def _():
                arriving.wait_recv()

        return finish

    waits = [
        halo(up_buf, below_buf, "up", "down"),
        halo(cp_buf, right_cp, "left", "right"),
        halo(cp_buf, diag_cp, "up_left", "down_right"),
    ]
    for target, back in ((below_buf, "down"), (right_cp, "right"), (diag_cp, "down_right")):

        @pl.when(jnp.logical_not(near[back][0]))
        def _():
            target[...] = jnp.zeros(target.shape, F32)

    loads_early[3].wait()
    loads_early[4].wait()
    loads_early[5].wait()
    b_in_t[...] = w_in[...].astype(BF16)
    b_in[...] = w_in[...].T.astype(BF16)
    b_mid[...] = w_mid[...].astype(BF16)
    b_mid_t[...] = w_mid[...].T.astype(BF16)
    padded_out = jnp.concatenate([w_out[...], jnp.zeros((SUBLANES - OUT, HID), F32)], axis=0)
    b_out[...] = padded_out.astype(BF16)
    b_out_t[...] = padded_out.T.astype(BF16)
    cot_s[...] = jnp.zeros(cot_s.shape, F32)
    vertex = lax.broadcasted_iota(jnp.int32, (LANES, LANES), 0)
    sample = lax.broadcasted_iota(jnp.int32, (LANES, LANES), 1)
    base = lax.div(sample, RATIO)
    fraction = (lax.rem(sample, RATIO).astype(F32) + off_x) / RATIO
    table = jnp.where(vertex == base, 1.0 - fraction, 0.0) + jnp.where(
        vertex == base + 1, fraction, 0.0
    )
    for wait in waits:
        wait()

    for r in range(SR + 1):
        value = fine_row(r) if r < SR else below_buf[0]
        edge = roll(right_cp[...], LANES - 1 - r) if r < SR else roll(diag_cp[...], LANES - 1)
        shifted = jnp.where(lane == LANES - 1, edge, roll(value, LANES - 1))
        across[r] = (1.0 - off_x) * value + off_x * shifted
    for r in range(CR + 1):
        value = coarse_s[r] if r < CR else below_buf[1]
        edge = roll(right_cp[...], CC - SR - r) if r < CR else roll(diag_cp[...], CC - SR)
        coarse_s[r] = jnp.where(lane == CC, edge, value)
    across_c[...] = dot(
        coarse_s[...].reshape((CR + 1) * CH, LANES), table, precision=lax.Precision.HIGHEST
    ).reshape(CR + 1, CH, LANES)

    def chunk_span(c):
        return pl.ds(pl.multiple_of(c * CHUNK, CHUNK), CHUNK)

    @pl.loop(0, CHUNKS)
    def _(c):
        for k in range(RATIO):
            i = c * RATIO + k
            span = pl.ds(pl.multiple_of(i * SC, SC), SC)
            part = (k + off_y) / RATIO
            feats[:CH, span] = ((1.0 - off_y) * across[i] + off_y * across[i + 1]).astype(BF16)
            feats[CH:, span] = ((1.0 - part) * across_c[c] + part * across_c[c + 1]).astype(BF16)
        span = chunk_span(c)
        act, slope = gate(dot(b_in[...], feats[:, span]))
        act_0[:, span] = act.astype(BF16)
        slope_0[:, span] = slope
        act, slope = gate(dot(b_mid[...], act_0[:, span]))
        act_1[:, span] = act.astype(BF16)
        slope_1[:, span] = slope
        colours = dot(b_out[...], act_1[:, span])
        for k in range(RATIO):
            pred[c * RATIO + k + 1] = colours[:, k * SC : (k + 1) * SC]

    loads_early[0].wait()

    def target_row(kind, r):
        found = targets[pl.ds(kind * OUT * SR + r, OUT, stride=SR), :]
        return jnp.concatenate([found, jnp.zeros((SUBLANES - OUT, LANES), F32)], axis=0)

    first_col = jnp.zeros((SUBLANES, LANES), F32)
    last_col = jnp.zeros((SUBLANES, LANES), F32)
    last_aim = jnp.zeros((SUBLANES, LANES), F32)
    for r in range(SR):
        first_col = jnp.where(lane_8 == r, roll(pred[r + 1], r), first_col)
        last_col = jnp.where(lane_8 == r, roll(pred[r + 1], r + 1), last_col)
        last_aim = jnp.where(lane_8 == r, roll(target_row(2, r), r + 1), last_aim)
    edge_send[0, 0] = pred[1]
    edge_send[1, 0] = first_col
    edge_send[2, 0] = pred[SR]
    edge_send[2, 1] = target_row(1, SR - 1)
    edge_send[3, 0] = last_col
    edge_send[3, 1] = last_aim
    waits = [
        halo(edge_send.at[0, 0], edge_recv.at[0, 0], "up", "down"),
        halo(edge_send.at[1, 0], edge_recv.at[1, 0], "left", "right"),
        halo(edge_send.at[2], edge_recv.at[2], "down", "up"),
        halo(edge_send.at[3], edge_recv.at[3], "right", "left"),
    ]
    for place, back in enumerate(("down", "right", "up", "left")):

        @pl.when(jnp.logical_not(near[back][0]))
        def _():
            edge_recv[place] = jnp.zeros(edge_recv.shape[1:], F32)

    for wait in waits:
        wait()

    pred[SR + 1] = edge_recv[0, 0]
    prior = jnp.where(has_up, (pred[1] - edge_recv[2, 0]) - edge_recv[2, 1], 0.0)
    for r in range(SR):
        here = pred[r + 1]
        row_error = (pred[r + 2] - here) - target_row(1, r)
        if r == SR - 1:
            row_error = jnp.where(has_down, row_error, 0.0)
        beside = jnp.where(lane_8 == LANES - 1, roll(edge_recv[1, 0], LANES - 1 - r), roll(here, -1))
        col_error = (beside - here) - target_row(2, r)
        closed = jnp.logical_and(lane_8 == LANES - 1, jnp.logical_not(has_right))
        col_error = jnp.where(closed, 0.0, col_error)
        before = (here - roll(edge_recv[3, 0], -r)) - roll(edge_recv[3, 1], -r)
        before = jnp.where(has_left, before, 0.0)
        col_prior = jnp.where(lane_8 == 0, before, roll(col_error, 1))
        value_error = here - target_row(0, r)
        cot = (
            2.0 * LOSS_VALUE * value_error
            + 2.0 * (prior - row_error)
            + 2.0 * (col_prior - col_error)
        )
        kept = lax.broadcasted_iota(jnp.int32, (SUBLANES, LANES), 0) < OUT
        cot_s[:, r * SC : (r + 1) * SC] = jnp.where(kept, cot, 0.0)
        prior = row_error

    grad_out[...] = jnp.zeros(grad_out.shape, F32)

    @pl.loop(0, CHUNKS)
    def _(c):
        span = chunk_span(c)
        cot = cot_s[:, span].astype(BF16)
        delta_1[:, span] = (dot(b_out_t[...], cot) * slope_1[:, span]).astype(BF16)
        grad_out[...] += dot_t(cot, act_1[:, span])

    half = HID // 2
    mid_rows = HID * half // LANES
    rest_rows = rest_own.shape[0]

    def mid_half(which, target):
        lower = act_0[pl.ds(pl.multiple_of(which * half, half), half), :]
        block = dot_t(delta_1[...], lower)
        for part in range(half // LANES):
            target[part * HID : (part + 1) * HID, :] = block[:, part * LANES : (part + 1) * LANES]

    partner = axis_core.device(1 - core)
    mid_half(1 - core, mid_away)
    pair_mid = links.copy(mid_away, mid_pair, partner, links.take(1))
    pair_mid.start()
    mid_half(core, mid_own)
    orders = ((axis_x, axis_y, axis_z), (axis_y, axis_x, axis_z))
    mids = [
        Scatter(links, mid_own, k * (mid_rows // 2), mid_rows // 2, orders[k], lands[k * 3 : k * 3 + 3])
        for k in range(2)
    ]
    rests = [
        Scatter(
            links,
            rest_own,
            k * (rest_rows // 2),
            rest_rows // 2,
            orders[k],
            lands[6 + k * 3 : 9 + k * 3],
        )
        for k in range(2)
    ]
    pair_mid.wait()
    mid_own[...] += mid_pair[...]
    for scatter in mids:
        scatter.start(0)

    grad_in[...] = jnp.zeros(grad_in.shape, F32)

    def lower_chunks(first, last):
        @pl.loop(first, last)
        def _(c):
            span = chunk_span(c)
            delta = (dot(b_mid_t[...], delta_1[:, span]) * slope_0[:, span]).astype(BF16)
            grad_in[...] += dot_t(feats[:, span], delta)
            spread = dot(b_in_t[...], delta)
            for k in range(RATIO):
                fgrad[c * RATIO + k] = spread[:, k * SC : (k + 1) * SC]

    lower_chunks(0, CHUNKS // 2)
    for scatter in mids:
        scatter.finish(0)
    for scatter in mids:
        scatter.start(1)
    lower_chunks(CHUNKS // 2, CHUNKS)
    for scatter in mids:
        scatter.finish(1)
    for scatter in mids:
        scatter.start(2)

    blocks = HID // LANES
    inputs = 2 * CH
    block_rows = rest_rows // (blocks // 2)

    def rest_half(which, target):
        for part in range(blocks // 2):
            for choice in range(2):

                @pl.when(which == choice)
                def _():
                    at = (choice * (blocks // 2) + part) * LANES
                    start = part * block_rows
                    target[start : start + inputs, :] = grad_in[:, at : at + LANES]
                    target[start + inputs : start + inputs + SUBLANES, :] = grad_out[:, at : at + LANES]
                    used = inputs + SUBLANES
                    target[start + used : start + block_rows, :] = jnp.zeros(
                        (block_rows - used, LANES), F32
                    )

    rest_half(1 - core, rest_away)
    pair_rest = links.copy(rest_away, rest_pair, partner, links.take(1))
    pair_rest.start()
    rest_half(core, rest_own)

    last = SR
    bottom = None
    packed = jnp.zeros((CH, LANES), F32)
    zero = jnp.zeros((CH, LANES), F32)
    for r in range(SR + 1):
        value = zero
        if r < SR:
            value = (1.0 - off_y) * fgrad[r, :CH]
        if r > 0:
            value = value + off_y * fgrad[r - 1, :CH]
        moved = off_x * roll(value, 1)
        out = (1.0 - off_x) * value + jnp.where(lane == 0, 0.0, moved)
        at = r if r < SR else SR + CR
        packed = jnp.where(lane == at, roll(moved, at), packed)
        if r < SR:
            fine_g[r] = out
        else:
            down_buf[0] = out
    for j in range(CR + 1):
        value = zero
        for k in range(RATIO):
            part = (k + off_y) / RATIO
            if j < CR:
                value = value + (1.0 - part) * fgrad[j * RATIO + k, CH:]
            if j > 0:
                value = value + part * fgrad[(j - 1) * RATIO + k, CH:]
        coarse_s[j] = value
    spread = dot_t(
        coarse_s[...].reshape((CR + 1) * CH, LANES), table, precision=lax.Precision.HIGHEST
    ).reshape(CR + 1, CH, LANES)
    for j in range(CR + 1):
        value = spread[j]
        at = SR + j if j < CR else SR + CR + 1
        packed = jnp.where(lane == at, roll(value, at - CC), packed)
        value = jnp.where(lane < CC, value, 0.0)
        if j < CR:
            coarse_g[j] = value
        else:
            down_buf[1] = value
    q_buf[...] = packed
    waits = [
        halo(down_buf, above_buf, "down", "up"),
        halo(q_buf, left_q, "right", "left"),
        halo(q_buf, diag_q, "down_right", "up_left"),
    ]
    for target, back in ((above_buf, "up"), (left_q, "left"), (diag_q, "up_left")):

        @pl.when(jnp.logical_not(near[back][0]))
        def _():
            target[...] = jnp.zeros(target.shape, F32)

    pair_rest.wait()
    rest_own[...] += rest_pair[...]
    for scatter in rests:
        scatter.start(0)

    for wait in waits:
        wait()
    fine_g[0] += above_buf[0] + jnp.where(lane == 0, roll(diag_q[...], -(SR + CR)), 0.0)
    coarse_g[0] += above_buf[1] + jnp.where(lane == 0, roll(diag_q[...], -(SR + CR + 1)), 0.0)
    squares = jnp.zeros((CH, LANES), F32)
    for r in range(SR):
        value = fine_g[r] + jnp.where(lane == 0, roll(left_q[...], -r), 0.0)
        fine_g[r] = value
        squares += value * value
    for j in range(CR):
        value = coarse_g[j] + jnp.where(lane == 0, roll(left_q[...], -(SR + j)), 0.0)
        coarse_g[j] = value
        squares += value * value
    total = squares[:SUBLANES]
    for part in range(1, CH // SUBLANES):
        total = total + squares[part * SUBLANES : (part + 1) * SUBLANES]
    total_mine[0] = total

    def total_copies(stage):
        axis = axes[stage]
        return [
            links.copy(
                total_mine.at[stage],
                total_land.at[total_slots[stage] - total_slots[0] + step - 1],
                axis.device(axis.peer(step)),
                total_slots[stage] + step - 1,
            )
            for step in range(1, axis.size)
        ]

    total_slots = [links.take(axis.size - 1) for axis in axes]

    def total_start(stage):
        for copy in total_copies(stage):
            copy.start()

    def total_finish(stage):
        found = total_mine[stage]
        for step, copy in enumerate(total_copies(stage)):
            copy.wait()
            found = found + total_land[total_slots[stage] - total_slots[0] + step]
        total_mine[stage + 1] = found

    total_start(0)
    gathers = [Gather(scatter, full) for scatter, full in zip(mids, (mid_full.at[core],) * 2)]
    gathers += [Gather(scatter, full) for scatter, full in zip(rests, (rest_full.at[core],) * 2)]
    for scatter in rests:
        scatter.finish(0)
    for scatter in rests:
        scatter.start(1)
    total_finish(0)
    total_start(1)
    for scatter, gather in zip(mids, gathers):
        scatter.finish(2)
        gather.place()
        gather.start(2)
    for scatter in rests:
        scatter.finish(1)
    for scatter in rests:
        scatter.start(2)
    total_finish(1)
    total_start(2)
    for scatter, gather in zip(rests, gathers[2:]):
        scatter.finish(2)
        gather.place()
        gather.start(2)
    total_finish(2)
    total_start(3)
    for gather in gathers:
        gather.finish(2)
        gather.start(1)
    total_finish(3)

    for load in loads_late:
        load.wait()
    fine_first, fine_second, coarse_first, coarse_second = late[:4]
    in_first, in_second, mid_first, mid_second, out_first, out_second = late[4:]
    entries = CH * (SR * SC + CR * CC) * rows_n * cols_n
    grid_scale = clip_factor(jnp.sum(total_mine[4], keepdims=True), entries)
    for r in range(SR):
        span = pl.ds(r, CH, stride=SR)
        fine_out[span, :] = adam_step(fine_g[r], fine_first[span, :], fine_second[span, :], grid_scale)
    for j in range(CR):
        span = pl.ds(j, CH, stride=CR)
        coarse_out[span, :] = adam_step(
            coarse_g[j, :, :CC], coarse_first[span, :], coarse_second[span, :], grid_scale
        )

    for gather in gathers:
        gather.finish(1)
        gather.start(0)
    for gather in gathers:
        gather.finish(0)
    last_mid = links.copy(mid_full.at[core], mid_full.at[core], partner, links.take(1))
    last_rest = links.copy(rest_full.at[core], rest_full.at[core], partner, links.take(1))
    last_mid.start()
    last_rest.start()
    last_mid.wait()
    last_rest.wait()

    squares = jnp.zeros((SUBLANES, LANES), F32)
    for which in range(2):
        for start in range(0, mid_rows, HID):
            value = mid_full[which, start : start + HID, :]
            value = (value * value).reshape(HID // SUBLANES, SUBLANES, LANES)
            squares += jnp.sum(value, axis=0)
        for part in range(blocks // 2):
            start = part * block_rows
            value = rest_full[which, start : start + inputs + SUBLANES, :]
            value = (value * value).reshape(inputs // SUBLANES + 1, SUBLANES, LANES)
            squares += jnp.sum(value, axis=0)
    scale = clip_factor(jnp.sum(squares, keepdims=True), HID * (HID + inputs + OUT))
    for which in range(2):
        for part in range(blocks // 2):
            at = (which * (blocks // 2) + part) * LANES
            lanes = slice(at, at + LANES)
            mid_out[:, lanes] = adam_step(
                mid_full[which, part * HID : (part + 1) * HID, :],
                mid_first[:, lanes],
                mid_second[:, lanes],
                scale,
            )
            start = part * block_rows
            in_out[:, lanes] = adam_step(
                rest_full[which, start : start + inputs, :],
                in_first[:, lanes],
                in_second[:, lanes],
                scale,
            )
            out_out[:, lanes] = adam_step(
                rest_full[which, start + inputs : start + inputs + OUT, :],
                out_first[:, lanes],
                out_second[:, lanes],
                scale,
            )
    assert links.used <= dims["COPIES"]


def shards(
    offsets,
    targets,
    grid_fine,
    grid_coarse,
    weight_in,
    weight_mid,
    weight_out,
    fine_first,
    fine_second,
    coarse_first,
    coarse_second,
    in_first,
    in_second,
    mid_first,
    mid_second,
    out_first,
    out_second,
):
    CH, SR, SC = grid_fine.shape
    CR, CC = grid_coarse.shape[1:]
    HID = weight_in.shape[0]
    OUT = weight_out.shape[0]
    S = SR * SC
    rows_n, cols_n = lax.axis_size("row"), lax.axis_size("col")
    sizes_x, sizes_y, sizes_z = 2, cols_n // 2, rows_n // 2
    peers = (sizes_x - 1) + (sizes_y - 1) + (sizes_z - 1)
    copies = 8 * peers + peers + 1 + 4 + 10
    owners = sizes_x * sizes_y * sizes_z
    half_blocks = HID // LANES // 2
    block_rows = -(-(2 * CH + SUBLANES) // SUBLANES) * SUBLANES
    rest_rows = half_blocks * block_rows
    rest_rows = -(-rest_rows // (owners * SUBLANES * half_blocks)) * owners * SUBLANES * half_blocks
    mid_rows = HID * HID // 2 // LANES
    dims = dict(CH=CH, SR=SR, SC=SC, CR=CR, CC=CC, HID=HID, OUT=OUT, COPIES=copies)

    flat = lambda grid: grid.reshape(-1, grid.shape[-1])
    early = (
        flat(targets),
        flat(grid_fine),
        flat(grid_coarse),
        weight_in.T,
        weight_mid[0],
        weight_out,
    )
    late = (
        flat(fine_first),
        flat(fine_second),
        flat(coarse_first),
        flat(coarse_second),
        in_first.T,
        in_second.T,
        mid_first[0],
        mid_second[0],
        out_first,
        out_second,
    )
    vmem = lambda *shape: pltpu.VMEM(shape, F32)
    low = lambda *shape: pltpu.VMEM(shape, BF16)

    def landing(rows, sizes):
        found = []
        for size in sizes:
            rows = rows // size
            found.append(vmem(max(size - 1, 1), rows, LANES))
        return found

    orders = ((sizes_x, sizes_y, sizes_z), (sizes_y, sizes_x, sizes_z))
    scratch = [pltpu.VMEM(a.shape, F32) for a in early + late]
    scratch += [
        vmem(2, CH, LANES),
        vmem(CH, LANES),
        vmem(2, CH, LANES),
        vmem(CH, LANES),
        vmem(CH, LANES),
        vmem(CR + 1, CH, LANES),
        vmem(SR + 1, CH, LANES),
        vmem(CR + 1, CH, LANES),
        low(HID, 2 * CH),
        low(2 * CH, HID),
        low(HID, HID),
        low(HID, HID),
        low(SUBLANES, HID),
        low(HID, SUBLANES),
        low(2 * CH, S),
        low(HID, S),
        low(HID, S),
        vmem(HID, S),
        vmem(HID, S),
        low(HID, S),
        vmem(SR + 2, SUBLANES, LANES),
        vmem(4, 2, SUBLANES, LANES),
        vmem(4, 2, SUBLANES, LANES),
        vmem(SUBLANES, S),
        vmem(SR, 2 * CH, LANES),
        vmem(2, CH, LANES),
        vmem(CH, LANES),
        vmem(2, CH, LANES),
        vmem(CH, LANES),
        vmem(CH, LANES),
        vmem(SR, CH, LANES),
        vmem(CR, CH, LANES),
        vmem(2 * CH, HID),
        vmem(SUBLANES, HID),
        vmem(mid_rows, LANES),
        vmem(mid_rows, LANES),
        vmem(mid_rows, LANES),
        vmem(2, mid_rows, LANES),
        vmem(rest_rows, LANES),
        vmem(rest_rows, LANES),
        vmem(rest_rows, LANES),
        vmem(2, rest_rows, LANES),
        vmem(5, SUBLANES, LANES),
        vmem(peers + 1, SUBLANES, LANES),
    ]
    for order in orders:
        scratch += landing(mid_rows // 2, order)
    for order in orders:
        scratch += landing(rest_rows // 2, order)
    scratch += [
        pltpu.SemaphoreType.DMA((len(early) + len(late),)),
        pltpu.SemaphoreType.DMA((copies,)),
        pltpu.SemaphoreType.DMA((copies,)),
    ]
    outs = (
        (CH * SR, SC),
        (CH * CR, CC),
        (2 * CH, HID),
        (HID, HID),
        (OUT, HID),
    )
    fine_step, coarse_step, in_step, mid_step, out_step = pl.pallas_call(
        functools.partial(step_kernel, dims),
        out_shape=[jax.ShapeDtypeStruct(shape, F32) for shape in outs],
        in_specs=[pl.BlockSpec(memory_space=pltpu.SMEM)]
        + [pl.BlockSpec(memory_space=pl.ANY)] * (len(early) + len(late)),
        out_specs=[pl.BlockSpec(memory_space=pltpu.VMEM)] * len(outs),
        scratch_shapes=scratch,
        compiler_params=pltpu.CompilerParams(
            collective_id=0, has_side_effects=True, vmem_limit_bytes=66 * 1024 * 1000
        ),
    )(offsets, *early, *late)
    return (
        fine_step.reshape(grid_fine.shape),
        coarse_step.reshape(grid_coarse.shape),
        in_step.T,
        mid_step[None],
        out_step,
    )


def solution(mesh):
    tile, copied = P(None, "row", "col"), P()
    placed = (P("row", "col", None), P(None, None, "row", "col"), tile, tile)
    placed += (copied,) * 3 + (tile,) * 4 + (copied,) * 6
    return jax.shard_map(
        shards,
        mesh=mesh,
        in_specs=placed,
        out_specs=(tile, tile, copied, copied, copied),
        check_vma=False,
    )
```

```python
import functools

import jax
import jax.numpy as jnp
from jax import lax
from jax.experimental import pallas as pl
from jax.experimental.pallas import tpu as pltpu
from jax.sharding import PartitionSpec as P

SUB = 4
RATIO = 4
ADAM_STEP = 10
BETA_ONE = 0.9
BETA_TWO = 0.99
ADAM_EPSILON = 1e-08
CLIP_RMS = 0.01
LOSS_VALUE = 0.25
MEAN_EPSILON = 1e-06

MESH = pl.DeviceIdType.MESH
LANES = 128
SUBLANES = 8
F32 = jnp.float32
BF16 = jnp.bfloat16


def clip_factor(total, entries):
    return jnp.minimum(1.0, CLIP_RMS / jnp.sqrt(total / entries + MEAN_EPSILON))


def adam_step(gradient, moment_one, moment_two, clip_scale):
    rise_one = 1.0 / (1.0 - BETA_ONE**ADAM_STEP)
    rise_two = 1.0 / (1.0 - BETA_TWO**ADAM_STEP)
    new_one = (BETA_ONE * rise_one) * moment_one + gradient * (
        clip_scale * ((1.0 - BETA_ONE) * rise_one)
    )
    root = gradient * (clip_scale * ((1.0 - BETA_TWO) * rise_two) ** 0.5)
    new_two = (BETA_TWO * rise_two) * moment_two + root * root
    return new_one / (jnp.sqrt(new_two) + ADAM_EPSILON)


def dot(former, latter, dims=((1,), (0,)), precision=None):
    return lax.dot_general(
        former, latter, (dims, ((), ())), preferred_element_type=F32, precision=precision
    )


def dot_t(former, latter, precision=None):
    return dot(former, latter, ((1,), (1,)), precision)


def gate(pre_act):
    sigmoid = 0.5 * jnp.tanh(0.5 * pre_act) + 0.5
    act = pre_act * sigmoid
    return act, sigmoid + act * (1.0 - sigmoid)


class Axis:
    def __init__(self, me, size, device):
        self.me, self.size, self.device = me, size, device

    def peer(self, step):
        return lax.rem(self.me + step, self.size)


def aligned(start):
    return pl.multiple_of(start, SUBLANES)


class Links:
    def __init__(self, send, recv):
        self.send, self.recv, self.used = send, recv, 0

    def take(self, count):
        first = self.used
        self.used += count
        return first

    def copy(self, source, target, device, slot):
        return pltpu.make_async_remote_copy(
            src_ref=source,
            dst_ref=target,
            send_sem=self.send.at[slot],
            recv_sem=self.recv.at[slot],
            device_id=device,
            device_id_type=MESH,
        )


class Scatter:
    def __init__(self, links, own, start, rows, axes, lands):
        self.links, self.own, self.axes, self.lands = links, own, axes, lands
        self.spans = [(start, rows)]
        for axis in axes:
            start, rows = self.spans[-1]
            part = rows // axis.size
            self.spans.append((start + axis.me * part, part))
        self.slots = [links.take(axis.size - 1) for axis in axes]

    def copies(self, stage):
        axis, land = self.axes[stage], self.lands[stage]
        start = self.spans[stage][0]
        part = self.spans[stage + 1][1]
        found = []
        for step in range(1, axis.size):
            peer = axis.peer(step)
            found.append(
                self.links.copy(
                    self.own.at[pl.ds(aligned(start + peer * part), part)],
                    land.at[step - 1],
                    axis.device(peer),
                    self.slots[stage] + step - 1,
                )
            )
        return found

    def start(self, stage):
        for copy in self.copies(stage):
            copy.start()

    def finish(self, stage):
        start, part = self.spans[stage + 1]
        span = pl.ds(aligned(start), part)
        for step, copy in enumerate(self.copies(stage)):
            copy.wait()
            self.own[span] += self.lands[stage][step]


class Gather:
    def __init__(self, scatter, full):
        self.scatter, self.full = scatter, full
        self.slots = [scatter.links.take(axis.size - 1) for axis in scatter.axes]

    def place(self):
        start, rows = self.scatter.spans[-1]
        span = pl.ds(aligned(start), rows)
        self.full[span] = self.scatter.own[span]

    def copies(self, stage):
        axis = self.scatter.axes[stage]
        start, rows = self.scatter.spans[stage + 1]
        block = self.full.at[pl.ds(aligned(start), rows)]
        return [
            self.scatter.links.copy(
                block, block, axis.device(axis.peer(step)), self.slots[stage] + step - 1
            )
            for step in range(1, axis.size)
        ]

    def start(self, stage):
        for copy in self.copies(stage):
            copy.start()

    def finish(self, stage):
        for copy in self.copies(stage):
            copy.wait()


class Crowd:
    def __init__(self, links, axis, source, target):
        self.links, self.axis, self.slot = links, axis, links.take(1)
        self.source, self.target = source, target

    def start(self):
        @pl.loop(1, self.axis.size)
        def _(step):
            peer = self.axis.peer(step)
            self.links.copy(
                self.source(peer), self.target(self.axis.me), self.axis.device(peer), self.slot
            ).start()

    def wait(self, sent, landed):
        if self.axis.size > 1:
            device = self.axis.device(self.axis.peer(1))
            self.links.copy(sent, sent, device, self.slot).wait_send()
            self.links.copy(landed, landed, device, self.slot).wait_recv()


class Total:
    def __init__(self, links, mine, lands, axes):
        self.mine, self.lands, self.axes = mine, lands, axes
        self.crowds = [
            Crowd(links, axis, lambda peer: mine, lambda me, land=land: land.at[me])
            for axis, land in zip(axes, lands)
        ]
        self.stage = 0

    def start(self):
        self.lands[self.stage][self.axes[self.stage].me] = self.mine[...]
        self.crowds[self.stage].start()

    def finish(self):
        land, count = self.lands[self.stage], self.axes[self.stage].size
        span = land.at[pl.ds(0, max(count - 1, 1))]
        self.crowds[self.stage].wait(span, span)
        total = land[0]
        for place in range(1, count):
            total = total + land[place]
        self.stage += 1
        if self.stage < len(self.axes):
            self.mine[...] = total
            self.start()
        return total


def step_kernel(dims, *refs):
    refs = iter(refs)
    take = lambda count: [next(refs) for _ in range(count)]
    (offsets_hbm,) = take(1)
    early_hbm = take(6)
    late_hbm = take(4)
    kept_hbm = take(6)
    fine_out, coarse_out, mid_full, in_full, out_full = take(5)
    kept = take(6)
    (offsets_ref,) = take(1)
    targets, fine, coarse, w_in, w_mid, w_out = early = take(6)
    late = take(4)
    (
        up_buf,
        cp_buf,
        below_buf,
        right_cp,
        diag_cp,
        coarse_s,
        across,
        across_c,
        b_in,
        b_in_t,
        b_mid,
        b_mid_t,
        b_out,
        b_out_t,
        feats,
        act_0,
        act_1,
        slope_0,
        slope_1,
        delta_1,
        pred,
        edge_send,
        edge_recv,
        col_send,
        col_recv,
        cot_s,
        fgrad,
        down_buf,
        q_buf,
        above_buf,
        left_q,
        diag_q,
        fine_g,
        coarse_g,
        grad_in,
        grad_out,
        mid_away,
        mid_own,
        mid_pair,
        in_away,
        in_own,
        in_pair,
        in_land,
        total_mine,
    ) = take(44)
    out_lands = take(4)
    total_lands = take(2)
    lands = take(12)
    load_sem, send_sem, recv_sem, know_sem = take(4)

    rows_n, cols_n = lax.axis_size("row"), lax.axis_size("col")
    row, col = lax.axis_index("row"), lax.axis_index("col")
    CH, SR, SC, CR, CC, HID, OUT = (dims[k] for k in ("CH", "SR", "SC", "CR", "CC", "HID", "OUT"))
    S = SR * SC
    CHUNK = dims["GROUP"] * SC
    CHUNKS = S // CHUNK
    GROUP = dims["GROUP"]

    core, plane = lax.rem(col, 2), lax.div(col, 2)
    x_at, z_at = lax.rem(row, 2), lax.div(row, 2)
    axis_core = Axis(core, 2, lambda p: (row, plane * 2 + p))
    axis_x = Axis(x_at, 2, lambda p: (z_at * 2 + p, col))
    axis_y = Axis(plane, cols_n // 2, lambda p: (row, p * 2 + core))
    axis_z = Axis(z_at, rows_n // 2, lambda p: (p * 2 + x_at, col))
    axes = (axis_core, axis_x, axis_y, axis_z)
    planes = cols_n // 2
    axis_chips = Axis(
        row * planes + plane,
        rows_n * planes,
        lambda p: (lax.div(p, planes), lax.rem(p, planes) * 2 + core),
    )

    has_up, has_down = row > 0, row < rows_n - 1
    has_left, has_right = col > 0, col < cols_n - 1
    near = {
        "up": (has_up, (row - 1, col)),
        "down": (has_down, (row + 1, col)),
        "left": (has_left, (row, col - 1)),
        "right": (has_right, (row, col + 1)),
        "up_left": (jnp.logical_and(has_up, has_left), (row - 1, col - 1)),
        "down_right": (jnp.logical_and(has_down, has_right), (row + 1, col + 1)),
    }
    links = Links(send_sem, recv_sem)

    loads = [
        pltpu.make_async_copy(source, target, load_sem.at[place])
        for place, (source, target) in enumerate(
            zip(
                early_hbm + late_hbm + kept_hbm + [offsets_hbm],
                early + late + kept + [offsets_ref],
            )
        )
    ]
    loads_early, loads_late, load_offsets = loads[:6], loads[6:-1], loads[-1]
    load_offsets.start()
    for place in (1, 2, 3, 4, 5, 0):
        loads_early[place].start()
    barrier = pltpu.get_barrier_semaphore()
    expected = sum(axis.size - 1 for axis in axes)
    for axis in axes:
        for step in range(1, axis.size):
            pl.semaphore_signal(
                barrier, inc=1, device_id=axis.device(axis.peer(step)), device_id_type=MESH
            )
    for there, device in near.values():
        expected = expected + there.astype(jnp.int32)

        @pl.when(there)
        def _():
            pl.semaphore_signal(barrier, inc=1, device_id=device, device_id_type=MESH)

    for load in loads_late:
        load.start()

    lane = lax.broadcasted_iota(jnp.int32, (CH, LANES), 1)
    lane_8 = lax.broadcasted_iota(jnp.int32, (SUBLANES, LANES), 1)
    load_offsets.wait()
    off_y = offsets_ref[0, 0, 0].astype(F32) / SUB
    off_x = offsets_ref[0, 0, 1].astype(F32) / SUB

    def fine_row(r):
        return fine[pl.ds(r, CH, stride=SR), :]

    def roll(value, shift):
        return pltpu.roll(value, shift % LANES, 1)

    coarse_s[...] = jnp.zeros(coarse_s.shape, F32)
    up_buf[...] = jnp.zeros(up_buf.shape, F32)
    loads_early[1].wait()
    loads_early[2].wait()
    for r in range(CR):
        coarse_s[r, :, :CC] = coarse[pl.ds(r, CH, stride=CR), :]
    up_buf[0] = fine_row(0)
    up_buf[1] = coarse_s[0]
    packed = jnp.zeros((CH, LANES), F32)
    for r in range(SR):
        packed = jnp.where(lane == r, roll(fine_row(r), r), packed)
    for r in range(CR):
        packed = jnp.where(lane == SR + r, roll(coarse_s[r], SR + r), packed)
    cp_buf[...] = packed

    pl.semaphore_wait(barrier, expected)

    def halo(source, target, towards, back):
        slot = links.take(1)
        copy = links.copy(source, target, near[towards][1], slot)
        arriving = links.copy(source, target, near[back][1], slot)

        @pl.when(near[towards][0])
        def _():
            copy.start()

        def finish():
            @pl.when(near[towards][0])
            def _():
                copy.wait_send()

            @pl.when(near[back][0])
            def _():
                arriving.wait_recv()

        return finish

    waits = [
        halo(up_buf, below_buf, "up", "down"),
        halo(cp_buf, right_cp, "left", "right"),
        halo(cp_buf, diag_cp, "up_left", "down_right"),
    ]
    for target, back in ((below_buf, "down"), (right_cp, "right"), (diag_cp, "down_right")):

        @pl.when(jnp.logical_not(near[back][0]))
        def _():
            target[...] = jnp.zeros(target.shape, F32)

    loads_early[3].wait()
    loads_early[4].wait()
    loads_early[5].wait()
    b_in_t[...] = w_in[...].astype(BF16)
    b_in[...] = w_in[...].T.astype(BF16)
    b_mid[...] = w_mid[...].astype(BF16)
    b_mid_t[...] = w_mid[...].T.astype(BF16)
    padded_out = jnp.concatenate([w_out[...], jnp.zeros((SUBLANES - OUT, HID), F32)], axis=0)
    b_out[...] = padded_out.astype(BF16)
    b_out_t[...] = padded_out.T.astype(BF16)
    cot_s[...] = jnp.zeros(cot_s.shape, BF16)
    vertex = lax.broadcasted_iota(jnp.int32, (LANES, LANES), 0)
    sample = lax.broadcasted_iota(jnp.int32, (LANES, LANES), 1)
    base = lax.div(sample, RATIO)
    fraction = (lax.rem(sample, RATIO).astype(F32) + off_x) / RATIO
    table = jnp.where(vertex == base, 1.0 - fraction, 0.0) + jnp.where(
        vertex == base + 1, fraction, 0.0
    )
    for wait in waits:
        wait()

    for r in range(SR + 1):
        value = fine_row(r) if r < SR else below_buf[0]
        edge = roll(right_cp[...], LANES - 1 - r) if r < SR else roll(diag_cp[...], LANES - 1)
        shifted = jnp.where(lane == LANES - 1, edge, roll(value, LANES - 1))
        across[r] = (1.0 - off_x) * value + off_x * shifted
    for r in range(CR + 1):
        value = coarse_s[r] if r < CR else below_buf[1]
        edge = roll(right_cp[...], CC - SR - r) if r < CR else roll(diag_cp[...], CC - SR)
        coarse_s[r] = jnp.where(lane == CC, edge, value)
    across_c[...] = dot(
        coarse_s[...].reshape((CR + 1) * CH, LANES), table, precision=lax.Precision.HIGHEST
    ).reshape(CR + 1, CH, LANES)

    def chunk_span(c):
        return pl.ds(pl.multiple_of(c * CHUNK, CHUNK), CHUNK)

    def spread_word(place, axis):
        for step in range(1, axis.size):
            pl.semaphore_signal(
                know_sem.at[place],
                inc=1,
                device_id=axis.device(axis.peer(step)),
                device_id_type=MESH,
            )

    def hear_word(place, axis):
        pl.semaphore_wait(know_sem.at[place], axis.size - 1)

    def forward(c):
        for k in range(GROUP):
            i = c * GROUP + k
            j = c * (GROUP // RATIO) + k // RATIO
            span = pl.ds(pl.multiple_of(i * SC, SC), SC)
            part = (k % RATIO + off_y) / RATIO
            feats[:CH, span] = ((1.0 - off_y) * across[i] + off_y * across[i + 1]).astype(BF16)
            feats[CH:, span] = ((1.0 - part) * across_c[j] + part * across_c[j + 1]).astype(BF16)
        span = chunk_span(c)
        act, slope = gate(dot(b_in[...], feats[:, span]))
        act_0[:, span] = act.astype(BF16)
        slope_0[:, span] = slope
        act, slope = gate(dot(b_mid[...], act_0[:, span]))
        act_1[:, span] = act.astype(BF16)
        slope_1[:, span] = slope
        colours = dot(b_out[...], act_1[:, span])
        for k in range(GROUP):
            pred[c * GROUP + k + 1] = colours[:, k * SC : (k + 1) * SC]

    order = [0, CHUNKS - 1] + list(range(1, CHUNKS - 1))

    def target_row(kind, r):
        found = targets[pl.ds(kind * OUT * SR + r, OUT, stride=SR), :]
        return jnp.concatenate([found, jnp.zeros((SUBLANES - OUT, LANES), F32)], axis=0)

    def send_columns(batch, groups):
        first_col = last_col = last_aim = jnp.zeros((SUBLANES, LANES), F32)
        for c in groups:
            for r in range(c * GROUP, (c + 1) * GROUP):
                first_col = jnp.where(lane_8 == r, roll(pred[r + 1], r), first_col)
                last_col = jnp.where(lane_8 == r, roll(pred[r + 1], r + 1), last_col)
                last_aim = jnp.where(lane_8 == r, roll(target_row(2, r), r + 1), last_aim)
        col_send[batch, 0] = first_col
        col_send[batch, 1] = last_col
        col_send[batch, 2] = last_aim
        return [
            halo(col_send.at[batch, 0], col_recv.at[batch, 0], "left", "right"),
            halo(col_send.at[batch, pl.ds(1, 2)], col_recv.at[batch, pl.ds(1, 2)], "right", "left"),
        ]

    spread_word(0, axis_x)
    for place in range(CHUNKS - 1):
        forward(order[place])
        if place == 0:
            hear_word(0, axis_x)
            spread_word(1, axis_y)
    hear_word(1, axis_y)
    loads_early[0].wait()
    edge_send[0, 0] = pred[1]
    edge_send[1, 0] = pred[SR]
    edge_send[1, 1] = target_row(1, SR - 1)
    early_waits = [
        halo(edge_send.at[0, 0], edge_recv.at[0, 0], "up", "down"),
        halo(edge_send.at[1], edge_recv.at[1], "down", "up"),
    ]
    early_waits += send_columns(0, order[:-1])
    for place, back in enumerate(("down", "up")):

        @pl.when(jnp.logical_not(near[back][0]))
        def _():
            edge_recv[place] = jnp.zeros(edge_recv.shape[1:], F32)

    forward(order[-1])
    last_waits = send_columns(1, order[-1:])
    for place, back in ((0, "right"), (1, "left"), (2, "left")):

        @pl.when(jnp.logical_not(near[back][0]))
        def _():
            for batch in range(2):
                col_recv[batch, place] = jnp.zeros(col_recv.shape[2:], F32)

    for wait in early_waits:
        wait()
    pred[SR + 1] = edge_recv[0, 0]
    above_error = jnp.where(has_up, (pred[1] - edge_recv[1, 0]) - edge_recv[1, 1], 0.0)

    def row_error(r):
        if r < 0:
            return above_error
        error = (pred[r + 2] - pred[r + 1]) - target_row(1, r)
        return jnp.where(has_down, error, 0.0) if r == SR - 1 else error

    def cotangent(c, batch):
        prior = row_error(c * GROUP - 1)
        for r in range(c * GROUP, (c + 1) * GROUP):
            here = pred[r + 1]
            error = row_error(r)
            edge = roll(col_recv[batch, 0], LANES - 1 - r)
            beside = jnp.where(lane_8 == LANES - 1, edge, roll(here, -1))
            col_error = (beside - here) - target_row(2, r)
            closed = jnp.logical_and(lane_8 == LANES - 1, jnp.logical_not(has_right))
            col_error = jnp.where(closed, 0.0, col_error)
            before = (here - roll(col_recv[batch, 1], -r)) - roll(col_recv[batch, 2], -r)
            before = jnp.where(has_left, before, 0.0)
            col_prior = jnp.where(lane_8 == 0, before, roll(col_error, 1))
            value_error = here - target_row(0, r)
            cot = (
                2.0 * LOSS_VALUE * value_error
                + 2.0 * (prior - error)
                + 2.0 * (col_prior - col_error)
            )
            kept = lax.broadcasted_iota(jnp.int32, (SUBLANES, LANES), 0) < OUT
            cot_s[:, r * SC : (r + 1) * SC] = jnp.where(kept, cot, 0.0).astype(BF16)
            prior = error

    def upper(c):
        span = chunk_span(c)
        delta_1[:, span] = (dot(b_out_t[...], cot_s[:, span]) * slope_1[:, span]).astype(BF16)

    for c in order[:-1]:
        cotangent(c, 0)
    for c in order[:-1]:
        upper(c)
    for wait in last_waits:
        wait()
    cotangent(order[-1], 1)
    upper(order[-1])
    grad_out[...] = dot_t(cot_s[...], act_1[...])
    outs = Total(links, grad_out, out_lands, axes)
    outs.start()

    half = HID // 2
    mid_rows = HID * half // LANES
    parts = 4
    part_rows = mid_rows // parts
    orders = ((axis_x, axis_y, axis_z), (axis_y, axis_x, axis_z))
    mids = [
        Scatter(links, mid_own, k * part_rows, part_rows, orders[k % 2], lands[k * 3 : k * 3 + 3])
        for k in range(parts)
    ]

    def mid_half(which, target):
        upper = delta_1[pl.ds(pl.multiple_of(which * half, half), half), :]
        block = dot_t(upper, act_0[...])
        for part in range(HID // LANES):
            target[part * half : (part + 1) * half, :] = block[:, part * LANES : (part + 1) * LANES]

    partner = axis_core.device(1 - core)
    part_span = lambda k: pl.ds(k * part_rows, part_rows)
    pairs = [
        links.copy(
            mid_away.at[part_span(k)], mid_pair.at[part_span(k)], partner, links.take(1)
        )
        for k in range(parts)
    ]
    mid_half(1 - core, mid_away)
    for pair in pairs:
        pair.start()
    mid_half(core, mid_own)
    for k in range(parts):
        pairs[k].wait()
        mid_own[part_span(k)] += mid_pair[part_span(k)]
        mids[k].start(0)

    grad_in[...] = jnp.zeros(grad_in.shape, F32)

    def lower(c):
        span = chunk_span(c)
        delta = (dot(b_mid_t[...], delta_1[:, span]) * slope_0[:, span]).astype(BF16)
        grad_in[...] += dot_t(feats[:, span], delta)
        spread = dot(b_in_t[...], delta)
        for k in range(GROUP):
            fgrad[c * GROUP + k] = spread[:, k * SC : (k + 1) * SC]

    def advance(which, stage):
        for k in which:
            mids[k].finish(stage)
            if stage < 2:
                mids[k].start(stage + 1)

    half_chunks = CHUNKS // 2
    for c in range(half_chunks):
        lower(c)
    outs.finish()
    advance((0, 1), 0)
    for c in range(half_chunks, CHUNKS - 1):
        lower(c)
    outs.finish()
    advance((2, 3), 0)
    lower(CHUNKS - 1)

    blocks = HID // LANES
    inputs = 2 * CH
    in_rows = inputs * blocks // 2
    own_rows = in_own.shape[0] // axis_chips.size

    def in_half(which, target):
        for choice in range(2):

            @pl.when(which == choice)
            def _():
                for part in range(blocks // 2):
                    at = (choice * (blocks // 2) + part) * LANES
                    target[part * inputs : (part + 1) * inputs, :] = grad_in[:, at : at + LANES]
        if target.shape[0] > in_rows:
            target[in_rows:, :] = jnp.zeros((target.shape[0] - in_rows, LANES), F32)

    in_half(1 - core, in_away)
    pair_in = links.copy(in_away, in_pair, partner, links.take(1))
    pair_in.start()
    in_half(core, in_own)

    def own_span(place):
        return pl.ds(aligned(place * own_rows), own_rows)

    in_crowd = Crowd(
        links, axis_chips, lambda peer: in_own.at[own_span(peer)], lambda me: in_land.at[me]
    )
    advance((0, 1), 1)

    last = SR
    bottom = None
    packed = jnp.zeros((CH, LANES), F32)
    zero = jnp.zeros((CH, LANES), F32)
    for r in range(SR + 1):
        value = zero
        if r < SR:
            value = (1.0 - off_y) * fgrad[r, :CH]
        if r > 0:
            value = value + off_y * fgrad[r - 1, :CH]
        moved = off_x * roll(value, 1)
        out = (1.0 - off_x) * value + jnp.where(lane == 0, 0.0, moved)
        at = r if r < SR else SR + CR
        packed = jnp.where(lane == at, roll(moved, at), packed)
        if r < SR:
            fine_g[r] = out
        else:
            down_buf[0] = out
    for j in range(CR + 1):
        value = zero
        for k in range(RATIO):
            part = (k + off_y) / RATIO
            if j < CR:
                value = value + (1.0 - part) * fgrad[j * RATIO + k, CH:]
            if j > 0:
                value = value + part * fgrad[(j - 1) * RATIO + k, CH:]
        coarse_s[j] = value
    spread = dot_t(
        coarse_s[...].reshape((CR + 1) * CH, LANES), table, precision=lax.Precision.HIGHEST
    ).reshape(CR + 1, CH, LANES)
    for j in range(CR + 1):
        value = spread[j]
        at = SR + j if j < CR else SR + CR + 1
        packed = jnp.where(lane == at, roll(value, at - CC), packed)
        value = jnp.where(lane < CC, value, 0.0)
        if j < CR:
            coarse_g[j] = value
        else:
            down_buf[1] = value
    q_buf[...] = packed
    waits = [
        halo(down_buf, above_buf, "down", "up"),
        halo(q_buf, left_q, "right", "left"),
        halo(q_buf, diag_q, "down_right", "up_left"),
    ]
    for target, back in ((above_buf, "up"), (left_q, "left"), (diag_q, "up_left")):

        @pl.when(jnp.logical_not(near[back][0]))
        def _():
            target[...] = jnp.zeros(target.shape, F32)

    outs.finish()
    pair_in.wait()
    in_own[...] += in_pair[...]
    in_crowd.start()
    advance((2, 3), 1)
    for wait in waits:
        wait()
    fine_g[0] += above_buf[0] + jnp.where(lane == 0, roll(diag_q[...], -(SR + CR)), 0.0)
    coarse_g[0] += above_buf[1] + jnp.where(lane == 0, roll(diag_q[...], -(SR + CR + 1)), 0.0)
    squares = jnp.zeros((CH, LANES), F32)
    for r in range(SR):
        value = fine_g[r] + jnp.where(lane == 0, roll(left_q[...], -r), 0.0)
        fine_g[r] = value
        squares += value * value
    for j in range(CR):
        value = coarse_g[j] + jnp.where(lane == 0, roll(left_q[...], -(SR + j)), 0.0)
        coarse_g[j] = value
        squares += value * value
    total = squares[:SUBLANES]
    for part in range(1, CH // SUBLANES):
        total = total + squares[part * SUBLANES : (part + 1) * SUBLANES]
    total_mine[...] = total
    totals = Total(links, total_mine, total_lands, (axis_core, axis_chips))
    totals.start()
    gathers = [Gather(scatter, mid_full.at[core]) for scatter in mids]

    def settle(which):
        for k in which:
            mids[k].finish(2)
            gathers[k].place()
            gathers[k].start(2)

    def regain(which, stage):
        for k in which:
            gathers[k].finish(stage)
            if stage > 0:
                gathers[k].start(stage - 1)

    settle((0, 1))
    mine = own_span(axis_chips.me)
    in_land[axis_chips.me] = in_own[mine]
    count = axis_chips.size - 1
    in_crowd.wait(in_own.at[pl.ds(0, count * own_rows)], in_land.at[pl.ds(0, count)])
    found = in_land[0]
    for place in range(1, axis_chips.size):
        found = found + in_land[place]
    in_full[core, mine] = found
    in_block = in_full.at[core, mine]
    in_back = Crowd(links, axis_chips, lambda peer: in_block, lambda me: in_block)
    in_back.start()
    settle((2, 3))
    totals.finish()
    out_full[...] = outs.finish()
    regain((0, 1), 2)
    regain((2, 3), 2)
    grid_total = totals.finish()

    for load in loads_late:
        load.wait()
    fine_first, fine_second, coarse_first, coarse_second = late
    entries = CH * (SR * SC + CR * CC) * rows_n * cols_n
    grid_scale = clip_factor(jnp.sum(grid_total, keepdims=True), entries)
    for r in range(SR):
        span = pl.ds(r, CH, stride=SR)
        fine_out[span, :] = adam_step(fine_g[r], fine_first[span, :], fine_second[span, :], grid_scale)
    for j in range(CR):
        span = pl.ds(j, CH, stride=CR)
        coarse_out[span, :] = adam_step(
            coarse_g[j, :, :CC], coarse_first[span, :], coarse_second[span, :], grid_scale
        )
    in_span = in_full.at[core, pl.ds(0, count * own_rows)]
    in_back.wait(in_span, in_span)
    last_in = links.copy(in_full.at[core], in_full.at[core], partner, links.take(1))
    last_in.start()
    regain((0, 1), 1)
    regain((2, 3), 1)

    def across_pair(k):
        block = mid_full.at[core, part_span(k)]
        copy = links.copy(block, block, partner, links.take(1))
        copy.start()
        return copy

    lasts = []
    for k in range(parts):
        gathers[k].finish(0)
        lasts.append(across_pair(k))
    last_in.wait()
    for copy in lasts:
        copy.wait()
    assert links.used <= dims["COPIES"]


def adam_kernel(
    fine_step,
    coarse_step,
    mid_full,
    in_full,
    out_full,
    in_first,
    in_second,
    mid_first,
    mid_second,
    out_first,
    out_second,
    fine_out,
    coarse_out,
    in_out,
    mid_out,
    out_out,
    in_step,
    mid_step,
    out_step,
    sems,
):
    writes = []

    def write(source, target):
        copy = pltpu.make_async_copy(source, target, sems.at[len(writes)])
        copy.start()
        writes.append(copy)

    write(fine_step, fine_out)
    write(coarse_step, coarse_out)
    inputs, hidden = in_step.shape
    outputs = out_step.shape[0]
    half, blocks = hidden // 2, hidden // LANES
    parts = [mid_full[which, :, :] for which in range(2)]
    parts += [in_full[which, : inputs * blocks // 2, :] for which in range(2)]
    parts += [out_full[:, part * LANES : (part + 1) * LANES] for part in range(blocks)]
    squares = jnp.zeros((SUBLANES, LANES), F32)
    for value in parts:
        value = (value * value).reshape(-1, SUBLANES, LANES)
        squares += jnp.sum(value, axis=0)
    scale = clip_factor(jnp.sum(squares, keepdims=True), hidden * (hidden + inputs + outputs))
    for which in range(2):
        span = slice(which * half, (which + 1) * half)
        for part in range(blocks):
            lanes = slice(part * LANES, (part + 1) * LANES)
            mid_step[span, lanes] = adam_step(
                mid_full[which, part * half : (part + 1) * half, :],
                mid_first[span, lanes],
                mid_second[span, lanes],
                scale,
            )
        write(mid_step.at[pl.ds(which * half, half)], mid_out.at[pl.ds(which * half, half)])
    out_step[...] = adam_step(out_full[:outputs, :], out_first[...], out_second[...], scale)
    write(out_step, out_out)
    for which in range(2):
        for part in range(blocks // 2):
            at = (which * (blocks // 2) + part) * LANES
            lanes = slice(at, at + LANES)
            in_step[:, lanes] = adam_step(
                in_full[which, part * inputs : (part + 1) * inputs, :],
                in_first[:, lanes],
                in_second[:, lanes],
                scale,
            )
    write(in_step, in_out)
    for copy in writes:
        copy.wait()


def shards(
    offsets,
    targets,
    grid_fine,
    grid_coarse,
    weight_in,
    weight_mid,
    weight_out,
    fine_first,
    fine_second,
    coarse_first,
    coarse_second,
    in_first,
    in_second,
    mid_first,
    mid_second,
    out_first,
    out_second,
):
    CH, SR, SC = grid_fine.shape
    CR, CC = grid_coarse.shape[1:]
    HID = weight_in.shape[0]
    OUT = weight_out.shape[0]
    S = SR * SC
    rows_n, cols_n = lax.axis_size("row"), lax.axis_size("col")
    sizes_x, sizes_y, sizes_z = 2, cols_n // 2, rows_n // 2
    peers = (sizes_x - 1) + (sizes_y - 1) + (sizes_z - 1)
    parts = 4
    copies = 2 * parts * (peers + 1) + 24
    chips = sizes_x * sizes_y * sizes_z
    in_rows = CH * HID // LANES
    in_rows = -(-in_rows // (chips * SUBLANES)) * chips * SUBLANES
    mid_rows = HID * HID // 2 // LANES
    dims = dict(CH=CH, SR=SR, SC=SC, CR=CR, CC=CC, HID=HID, OUT=OUT, COPIES=copies, GROUP=8)

    flat = lambda grid: grid.reshape(-1, grid.shape[-1])
    early = (
        flat(targets),
        flat(grid_fine),
        flat(grid_coarse),
        weight_in.T,
        weight_mid[0],
        weight_out,
    )
    late = (flat(fine_first), flat(fine_second), flat(coarse_first), flat(coarse_second))
    vmem = lambda *shape: pltpu.VMEM(shape, F32)
    low = lambda *shape: pltpu.VMEM(shape, BF16)

    def landing(rows, sizes):
        found = []
        for size in sizes:
            rows = rows // size
            found.append(vmem(max(size - 1, 1), rows, LANES))
        return found

    orders = ((sizes_x, sizes_y, sizes_z), (sizes_y, sizes_x, sizes_z))
    kept = (in_first.T, in_second.T, mid_first[0], mid_second[0], out_first, out_second)
    scratch = [pltpu.SMEM(offsets.shape, jnp.int32)]
    scratch += [pltpu.VMEM(a.shape, F32) for a in early + late]
    scratch += [
        vmem(2, CH, LANES),
        vmem(CH, LANES),
        vmem(2, CH, LANES),
        vmem(CH, LANES),
        vmem(CH, LANES),
        vmem(CR + 1, CH, LANES),
        vmem(SR + 1, CH, LANES),
        vmem(CR + 1, CH, LANES),
        low(HID, 2 * CH),
        low(2 * CH, HID),
        low(HID, HID),
        low(HID, HID),
        low(SUBLANES, HID),
        low(HID, SUBLANES),
        low(2 * CH, S),
        low(HID, S),
        low(HID, S),
        vmem(HID, S),
        vmem(HID, S),
        low(HID, S),
        vmem(SR + 2, SUBLANES, LANES),
        vmem(2, 2, SUBLANES, LANES),
        vmem(2, 2, SUBLANES, LANES),
        vmem(2, 3, SUBLANES, LANES),
        vmem(2, 3, SUBLANES, LANES),
        low(SUBLANES, S),
        vmem(SR, 2 * CH, LANES),
        vmem(2, CH, LANES),
        vmem(CH, LANES),
        vmem(2, CH, LANES),
        vmem(CH, LANES),
        vmem(CH, LANES),
        vmem(SR, CH, LANES),
        vmem(CR, CH, LANES),
        vmem(2 * CH, HID),
        vmem(SUBLANES, HID),
        vmem(mid_rows, LANES),
        vmem(mid_rows, LANES),
        vmem(mid_rows, LANES),
        vmem(in_rows, LANES),
        vmem(in_rows, LANES),
        vmem(in_rows, LANES),
        vmem(chips, in_rows // chips, LANES),
        vmem(SUBLANES, LANES),
    ]
    scratch += [vmem(size, SUBLANES, HID) for size in (2, sizes_x, sizes_y, sizes_z)]
    scratch += [vmem(size, SUBLANES, LANES) for size in (2, chips)]
    for part in range(parts):
        scratch += landing(mid_rows // parts, orders[part % 2])
    scratch += [
        pltpu.SemaphoreType.DMA((len(early) + len(late) + len(kept) + 1,)),
        pltpu.SemaphoreType.DMA((copies,)),
        pltpu.SemaphoreType.DMA((copies,)),
        pltpu.SemaphoreType.REGULAR((2,)),
    ]
    outs = (
        (CH * SR, SC),
        (CH * CR, CC),
        (2, mid_rows, LANES),
        (2, in_rows, LANES),
        (SUBLANES, HID),
    ) + tuple(a.shape for a in kept)
    far = pl.BlockSpec(memory_space=pltpu.HBM)
    whole = pl.BlockSpec(memory_space=pltpu.VMEM)
    found = pl.pallas_call(
        functools.partial(step_kernel, dims),
        out_shape=[jax.ShapeDtypeStruct(shape, F32) for shape in outs],
        in_specs=[far] * (1 + len(early) + len(late) + len(kept)),
        out_specs=[whole] * len(outs),
        scratch_shapes=scratch,
        compiler_params=pltpu.CompilerParams(
            collective_id=0, has_side_effects=True, vmem_limit_bytes=48 * 1024 * 1024
        ),
        name="field",
    )(*[pltpu.with_memory_space_constraint(a, pltpu.HBM) for a in (offsets, *early, *late, *kept)])
    steps = ((CH * SR, SC), (CH * CR, CC), (2 * CH, HID), (HID, HID), (OUT, HID))
    fine_step, coarse_step, in_step, mid_step, out_step = pl.pallas_call(
        adam_kernel,
        out_shape=[jax.ShapeDtypeStruct(shape, F32) for shape in steps],
        in_specs=[whole] * len(found),
        out_specs=[far] * len(steps),
        scratch_shapes=[pltpu.VMEM(shape, F32) for shape in steps[2:]]
        + [pltpu.SemaphoreType.DMA((4 + 2 * HID // LANES,))],
        compiler_params=pltpu.CompilerParams(vmem_limit_bytes=8 * 1024 * 1024),
        name="adam",
    )(*found)
    return (
        fine_step.reshape(grid_fine.shape),
        coarse_step.reshape(grid_coarse.shape),
        in_step.T,
        mid_step[None],
        out_step,
    )


def solution(mesh):
    tile, copied = P(None, "row", "col"), P()
    placed = (P("row", "col", None), P(None, None, "row", "col"), tile, tile)
    placed += (copied,) * 3 + (tile,) * 4 + (copied,) * 6
    return jax.shard_map(
        shards,
        mesh=mesh,
        in_specs=placed,
        out_specs=(tile, tile, copied, copied, copied),
        check_vma=False,
    )
```

```python
import functools

import jax
import jax.numpy as jnp
from jax import lax
from jax.experimental import pallas as pl
from jax.experimental.pallas import tpu as pltpu
from jax.sharding import PartitionSpec as P

SUB = 4
RATIO = 4
ADAM_STEP = 10
BETA_ONE = 0.9
BETA_TWO = 0.99
ADAM_EPSILON = 1e-08
CLIP_RMS = 0.01
LOSS_VALUE = 0.25
MEAN_EPSILON = 1e-06

MESH = pl.DeviceIdType.MESH
LANES = 128
SUBLANES = 8
F32 = jnp.float32
BF16 = jnp.bfloat16


def clip_factor(total, entries):
    return jnp.minimum(1.0, CLIP_RMS / jnp.sqrt(total / entries + MEAN_EPSILON))


def adam_step(gradient, moment_one, moment_two, clip_scale):
    rise_one = 1.0 / (1.0 - BETA_ONE**ADAM_STEP)
    rise_two = 1.0 / (1.0 - BETA_TWO**ADAM_STEP)
    new_one = (BETA_ONE * rise_one) * moment_one + gradient * (
        clip_scale * ((1.0 - BETA_ONE) * rise_one)
    )
    root = gradient * (clip_scale * ((1.0 - BETA_TWO) * rise_two) ** 0.5)
    new_two = (BETA_TWO * rise_two) * moment_two + root * root
    return new_one / (jnp.sqrt(new_two) + ADAM_EPSILON)


def dot(former, latter, dims=((1,), (0,)), precision=None):
    return lax.dot_general(
        former, latter, (dims, ((), ())), preferred_element_type=F32, precision=precision
    )


def dot_t(former, latter, precision=None):
    return dot(former, latter, ((1,), (1,)), precision)


def silu_of_half(half):
    return half + half * jnp.tanh(half)


def slope_of_half(half):
    bend = jnp.tanh(half)
    return (1.0 + bend) * ((1.0 + half) - half * bend)


class Axis:
    def __init__(self, me, size, device):
        self.me, self.size, self.device = me, size, device

    def peer(self, step):
        return lax.rem(self.me + step, self.size)


def aligned(start):
    return pl.multiple_of(start, SUBLANES)


class Links:
    def __init__(self, send, recv):
        self.send, self.recv, self.used = send, recv, 0

    def take(self, count):
        first = self.used
        self.used += count
        return first

    def copy(self, source, target, device, slot):
        return pltpu.make_async_remote_copy(
            src_ref=source,
            dst_ref=target,
            send_sem=self.send.at[slot],
            recv_sem=self.recv.at[slot],
            device_id=device,
            device_id_type=MESH,
        )


class Scatter:
    def __init__(self, links, own, start, rows, axes, lands):
        self.links, self.own, self.axes, self.lands = links, own, axes, lands
        self.spans = [(start, rows)]
        for axis in axes:
            start, rows = self.spans[-1]
            part = rows // axis.size
            self.spans.append((start + axis.me * part, part))
        self.slots = [links.take(axis.size - 1) for axis in axes]

    def copies(self, stage):
        axis, land = self.axes[stage], self.lands[stage]
        start = self.spans[stage][0]
        part = self.spans[stage + 1][1]
        found = []
        for step in range(1, axis.size):
            peer = axis.peer(step)
            found.append(
                self.links.copy(
                    self.own.at[pl.ds(aligned(start + peer * part), part)],
                    land.at[step - 1],
                    axis.device(peer),
                    self.slots[stage] + step - 1,
                )
            )
        return found

    def start(self, stage):
        for copy in self.copies(stage):
            copy.start()

    def finish(self, stage):
        start, part = self.spans[stage + 1]
        span = pl.ds(aligned(start), part)
        for step, copy in enumerate(self.copies(stage)):
            copy.wait()
            self.own[span] += self.lands[stage][step]


class Gather:
    def __init__(self, scatter, full):
        self.scatter, self.full = scatter, full
        self.slots = [scatter.links.take(axis.size - 1) for axis in scatter.axes]

    def place(self):
        start, rows = self.scatter.spans[-1]
        span = pl.ds(aligned(start), rows)
        self.full[span] = self.scatter.own[span]

    def copies(self, stage):
        axis = self.scatter.axes[stage]
        start, rows = self.scatter.spans[stage + 1]
        block = self.full.at[pl.ds(aligned(start), rows)]
        return [
            self.scatter.links.copy(
                block, block, axis.device(axis.peer(step)), self.slots[stage] + step - 1
            )
            for step in range(1, axis.size)
        ]

    def start(self, stage):
        for copy in self.copies(stage):
            copy.start()

    def finish(self, stage):
        for copy in self.copies(stage):
            copy.wait()


class Crowd:
    def __init__(self, links, axis, source, target):
        self.links, self.axis, self.slot = links, axis, links.take(1)
        self.source, self.target = source, target

    def start(self):
        @pl.loop(1, self.axis.size)
        def _(step):
            peer = self.axis.peer(step)
            self.links.copy(
                self.source(peer), self.target(self.axis.me), self.axis.device(peer), self.slot
            ).start()

    def wait(self, sent, landed):
        if self.axis.size > 1:
            device = self.axis.device(self.axis.peer(1))
            self.links.copy(sent, sent, device, self.slot).wait_send()
            self.links.copy(landed, landed, device, self.slot).wait_recv()


class Total:
    def __init__(self, links, mine, lands, axes):
        self.mine, self.lands, self.axes = mine, lands, axes
        self.crowds = [
            Crowd(links, axis, lambda peer: mine, lambda me, land=land: land.at[me])
            for axis, land in zip(axes, lands)
        ]
        self.stage = 0

    def start(self):
        self.lands[self.stage][self.axes[self.stage].me] = self.mine[...]
        self.crowds[self.stage].start()

    def finish(self):
        land, count = self.lands[self.stage], self.axes[self.stage].size
        span = land.at[pl.ds(0, max(count - 1, 1))]
        self.crowds[self.stage].wait(span, span)
        total = land[0]
        for place in range(1, count):
            total = total + land[place]
        self.stage += 1
        if self.stage < len(self.axes):
            self.mine[...] = total
            self.start()
        return total


def step_kernel(dims, *refs):
    refs = iter(refs)
    take = lambda count: [next(refs) for _ in range(count)]
    (offsets_hbm,) = take(1)
    early_hbm = take(6)
    late_hbm = take(4)
    kept_hbm = take(6)
    fine_out, coarse_out, mid_full, in_full, out_full = take(5)
    kept = take(6)
    (offsets_ref,) = take(1)
    targets, fine, coarse, w_in, w_mid, w_out = early = take(6)
    late = take(4)
    (
        up_buf,
        cp_buf,
        below_buf,
        right_cp,
        diag_cp,
        coarse_s,
        across,
        across_c,
        b_in,
        b_in_t,
        b_mid,
        b_mid_t,
        b_out,
        b_out_t,
        feats,
        act_0,
        act_1,
        half_0,
        half_1,
        delta_1,
        pred,
        edge_send,
        edge_recv,
        col_send,
        col_recv,
        cot_s,
        fgrad,
        down_buf,
        q_buf,
        above_buf,
        left_q,
        diag_q,
        fine_g,
        coarse_g,
        grad_in,
        grad_out,
        mid_away,
        mid_own,
        mid_pair,
        in_away,
        in_own,
        in_pair,
        total_mine,
    ) = take(43)
    out_lands = take(4)
    total_lands = take(2)
    lands = take(14)
    load_sem, send_sem, recv_sem, know_sem = take(4)

    rows_n, cols_n = lax.axis_size("row"), lax.axis_size("col")
    row, col = lax.axis_index("row"), lax.axis_index("col")
    CH, SR, SC, CR, CC, HID, OUT = (dims[k] for k in ("CH", "SR", "SC", "CR", "CC", "HID", "OUT"))
    S = SR * SC
    CHUNK = dims["GROUP"] * SC
    CHUNKS = S // CHUNK
    GROUP = dims["GROUP"]

    core, plane = lax.rem(col, 2), lax.div(col, 2)
    x_at, z_at = lax.rem(row, 2), lax.div(row, 2)
    axis_core = Axis(core, 2, lambda p: (row, plane * 2 + p))
    axis_x = Axis(x_at, 2, lambda p: (z_at * 2 + p, col))
    axis_y = Axis(plane, cols_n // 2, lambda p: (row, p * 2 + core))
    axis_z = Axis(z_at, rows_n // 2, lambda p: (p * 2 + x_at, col))
    axes = (axis_core, axis_x, axis_y, axis_z)
    planes = cols_n // 2
    axis_plane = Axis(
        x_at * planes + plane,
        2 * planes,
        lambda p: (z_at * 2 + lax.div(p, planes), lax.rem(p, planes) * 2 + core),
    )
    axis_chips = Axis(
        row * planes + plane,
        rows_n * planes,
        lambda p: (lax.div(p, planes), lax.rem(p, planes) * 2 + core),
    )

    has_up, has_down = row > 0, row < rows_n - 1
    has_left, has_right = col > 0, col < cols_n - 1
    near = {
        "up": (has_up, (row - 1, col)),
        "down": (has_down, (row + 1, col)),
        "left": (has_left, (row, col - 1)),
        "right": (has_right, (row, col + 1)),
        "up_left": (jnp.logical_and(has_up, has_left), (row - 1, col - 1)),
        "down_right": (jnp.logical_and(has_down, has_right), (row + 1, col + 1)),
    }
    links = Links(send_sem, recv_sem)

    loads = [
        pltpu.make_async_copy(source, target, load_sem.at[place])
        for place, (source, target) in enumerate(
            zip(
                early_hbm + late_hbm + kept_hbm + [offsets_hbm],
                early + late + kept + [offsets_ref],
            )
        )
    ]
    loads_early, loads_late, load_offsets = loads[:6], loads[6:-1], loads[-1]
    load_offsets.start()
    for place in (1, 2, 3, 4, 5, 0):
        loads_early[place].start()
    barrier = pltpu.get_barrier_semaphore()
    expected = sum(axis.size - 1 for axis in axes)
    for axis in axes:
        for step in range(1, axis.size):
            pl.semaphore_signal(
                barrier, inc=1, device_id=axis.device(axis.peer(step)), device_id_type=MESH
            )
    for there, device in near.values():
        expected = expected + there.astype(jnp.int32)

        @pl.when(there)
        def _():
            pl.semaphore_signal(barrier, inc=1, device_id=device, device_id_type=MESH)

    for load in loads_late:
        load.start()

    lane = lax.broadcasted_iota(jnp.int32, (CH, LANES), 1)
    lane_8 = lax.broadcasted_iota(jnp.int32, (SUBLANES, LANES), 1)
    load_offsets.wait()
    off_y = offsets_ref[0, 0, 0].astype(F32) / SUB
    off_x = offsets_ref[0, 0, 1].astype(F32) / SUB

    def fine_row(r):
        return fine[pl.ds(r, CH, stride=SR), :]

    def roll(value, shift):
        return pltpu.roll(value, shift % LANES, 1)

    coarse_s[...] = jnp.zeros(coarse_s.shape, F32)
    up_buf[...] = jnp.zeros(up_buf.shape, F32)
    loads_early[1].wait()
    loads_early[2].wait()
    for r in range(CR):
        coarse_s[r, :, :CC] = coarse[pl.ds(r, CH, stride=CR), :]
    up_buf[0] = fine_row(0)
    up_buf[1] = coarse_s[0]
    packed = jnp.zeros((CH, LANES), F32)
    for r in range(SR):
        packed = jnp.where(lane == r, roll(fine_row(r), r), packed)
    for r in range(CR):
        packed = jnp.where(lane == SR + r, roll(coarse_s[r], SR + r), packed)
    cp_buf[...] = packed

    pl.semaphore_wait(barrier, expected)

    def halo(source, target, towards, back):
        slot = links.take(1)
        copy = links.copy(source, target, near[towards][1], slot)
        arriving = links.copy(source, target, near[back][1], slot)

        @pl.when(near[towards][0])
        def _():
            copy.start()

        def finish():
            @pl.when(near[towards][0])
            def _():
                copy.wait_send()

            @pl.when(near[back][0])
            def _():
                arriving.wait_recv()

        return finish

    waits = [
        halo(up_buf, below_buf, "up", "down"),
        halo(cp_buf, right_cp, "left", "right"),
        halo(cp_buf, diag_cp, "up_left", "down_right"),
    ]
    for target, back in ((below_buf, "down"), (right_cp, "right"), (diag_cp, "down_right")):

        @pl.when(jnp.logical_not(near[back][0]))
        def _():
            target[...] = jnp.zeros(target.shape, F32)

    loads_early[3].wait()
    loads_early[4].wait()
    loads_early[5].wait()
    b_in_t[...] = w_in[...].astype(BF16)
    b_in[...] = (0.5 * w_in[...]).T.astype(BF16)
    halved = 0.5 * w_mid[...]
    b_mid[...] = halved.astype(BF16)
    b_mid_t[...] = halved.T.astype(BF16)
    padded_out = jnp.concatenate([w_out[...], jnp.zeros((SUBLANES - OUT, HID), F32)], axis=0)
    b_out[...] = padded_out.astype(BF16)
    b_out_t[...] = (0.5 * padded_out).T.astype(BF16)
    cot_s[...] = jnp.zeros(cot_s.shape, BF16)
    vertex = lax.broadcasted_iota(jnp.int32, (LANES, LANES), 0)
    sample = lax.broadcasted_iota(jnp.int32, (LANES, LANES), 1)
    base = lax.div(sample, RATIO)
    fraction = (lax.rem(sample, RATIO).astype(F32) + off_x) / RATIO
    table = jnp.where(vertex == base, 1.0 - fraction, 0.0) + jnp.where(
        vertex == base + 1, fraction, 0.0
    )
    for wait in waits:
        wait()

    for r in range(SR + 1):
        value = fine_row(r) if r < SR else below_buf[0]
        edge = roll(right_cp[...], LANES - 1 - r) if r < SR else roll(diag_cp[...], LANES - 1)
        shifted = jnp.where(lane == LANES - 1, edge, roll(value, LANES - 1))
        across[r] = (1.0 - off_x) * value + off_x * shifted
    for r in range(CR + 1):
        value = coarse_s[r] if r < CR else below_buf[1]
        edge = roll(right_cp[...], CC - SR - r) if r < CR else roll(diag_cp[...], CC - SR)
        coarse_s[r] = jnp.where(lane == CC, edge, value)
    across_c[...] = dot(
        coarse_s[...].reshape((CR + 1) * CH, LANES), table, precision=lax.Precision.HIGHEST
    ).reshape(CR + 1, CH, LANES)

    def chunk_span(c):
        return slice(c * CHUNK, (c + 1) * CHUNK)

    def spread_word(place, axis):
        for step in range(1, axis.size):
            pl.semaphore_signal(
                know_sem.at[place],
                inc=1,
                device_id=axis.device(axis.peer(step)),
                device_id_type=MESH,
            )

    def hear_word(place, axis):
        pl.semaphore_wait(know_sem.at[place], axis.size - 1)

    def forward(c):
        for k in range(GROUP):
            i = c * GROUP + k
            j = c * (GROUP // RATIO) + k // RATIO
            span = slice(i * SC, (i + 1) * SC)
            part = (k % RATIO + off_y) / RATIO
            feats[:CH, span] = ((1.0 - off_y) * across[i] + off_y * across[i + 1]).astype(BF16)
            feats[CH:, span] = ((1.0 - part) * across_c[j] + part * across_c[j + 1]).astype(BF16)
        span = chunk_span(c)
        half_0[:, span] = dot(b_in[...], feats[:, span])
        act_0[:, span] = silu_of_half(half_0[:, span]).astype(BF16)
        half_1[:, span] = dot(b_mid[...], act_0[:, span])
        act_1[:, span] = silu_of_half(half_1[:, span]).astype(BF16)
        colours = dot(b_out[...], act_1[:, span])
        for k in range(GROUP):
            pred[c * GROUP + k + 1] = colours[:, k * SC : (k + 1) * SC]

    order = [0, CHUNKS - 1] + list(range(1, CHUNKS - 1))

    def target_row(kind, r):
        found = targets[pl.ds(kind * OUT * SR + r, OUT, stride=SR), :]
        return jnp.concatenate([found, jnp.zeros((SUBLANES - OUT, LANES), F32)], axis=0)

    def send_columns(batch, groups):
        first_col = last_col = last_aim = jnp.zeros((SUBLANES, LANES), F32)
        for c in groups:
            for r in range(c * GROUP, (c + 1) * GROUP):
                first_col = jnp.where(lane_8 == r, roll(pred[r + 1], r), first_col)
                last_col = jnp.where(lane_8 == r, roll(pred[r + 1], r + 1), last_col)
                last_aim = jnp.where(lane_8 == r, roll(target_row(2, r), r + 1), last_aim)
        col_send[batch, 0] = first_col
        col_send[batch, 1] = last_col
        col_send[batch, 2] = last_aim
        return [
            halo(col_send.at[batch, 0], col_recv.at[batch, 0], "left", "right"),
            halo(col_send.at[batch, pl.ds(1, 2)], col_recv.at[batch, pl.ds(1, 2)], "right", "left"),
        ]

    spread_word(0, axis_x)
    for place in range(CHUNKS - 1):
        forward(order[place])
        if place == 0:
            hear_word(0, axis_x)
            spread_word(1, axis_y)
    hear_word(1, axis_y)
    loads_early[0].wait()
    edge_send[0, 0] = pred[1]
    edge_send[1, 0] = pred[SR]
    edge_send[1, 1] = target_row(1, SR - 1)
    early_waits = [
        halo(edge_send.at[0, 0], edge_recv.at[0, 0], "up", "down"),
        halo(edge_send.at[1], edge_recv.at[1], "down", "up"),
    ]
    early_waits += send_columns(0, order[:-1])
    for place, back in enumerate(("down", "up")):

        @pl.when(jnp.logical_not(near[back][0]))
        def _():
            edge_recv[place] = jnp.zeros(edge_recv.shape[1:], F32)

    forward(order[-1])
    last_waits = send_columns(1, order[-1:])
    for place, back in ((0, "right"), (1, "left"), (2, "left")):

        @pl.when(jnp.logical_not(near[back][0]))
        def _():
            for batch in range(2):
                col_recv[batch, place] = jnp.zeros(col_recv.shape[2:], F32)

    for wait in early_waits:
        wait()
    pred[SR + 1] = edge_recv[0, 0]
    above_error = jnp.where(has_up, (pred[1] - edge_recv[1, 0]) - edge_recv[1, 1], 0.0)

    def row_error(r):
        if r < 0:
            return above_error
        error = (pred[r + 2] - pred[r + 1]) - target_row(1, r)
        return jnp.where(has_down, error, 0.0) if r == SR - 1 else error

    def cotangent(c, batch):
        prior = row_error(c * GROUP - 1)
        for r in range(c * GROUP, (c + 1) * GROUP):
            here = pred[r + 1]
            error = row_error(r)
            edge = roll(col_recv[batch, 0], LANES - 1 - r)
            beside = jnp.where(lane_8 == LANES - 1, edge, roll(here, -1))
            col_error = (beside - here) - target_row(2, r)
            closed = jnp.logical_and(lane_8 == LANES - 1, jnp.logical_not(has_right))
            col_error = jnp.where(closed, 0.0, col_error)
            before = (here - roll(col_recv[batch, 1], -r)) - roll(col_recv[batch, 2], -r)
            before = jnp.where(has_left, before, 0.0)
            col_prior = jnp.where(lane_8 == 0, before, roll(col_error, 1))
            value_error = here - target_row(0, r)
            cot = (
                2.0 * LOSS_VALUE * value_error
                + 2.0 * (prior - error)
                + 2.0 * (col_prior - col_error)
            )
            kept = lax.broadcasted_iota(jnp.int32, (SUBLANES, LANES), 0) < OUT
            cot_s[:, r * SC : (r + 1) * SC] = jnp.where(kept, cot, 0.0).astype(BF16)
            prior = error

    def upper(c):
        span = chunk_span(c)
        slope = slope_of_half(half_1[:, span])
        delta_1[:, span] = (dot(b_out_t[...], cot_s[:, span]) * slope).astype(BF16)

    for c in order[:-1]:
        cotangent(c, 0)
    for c in order[:-1]:
        upper(c)
    for wait in last_waits:
        wait()
    cotangent(order[-1], 1)
    upper(order[-1])

    half = HID // 2
    mid_rows = HID * half // LANES
    parts = 4
    part_rows = mid_rows // parts
    orders = ((axis_x, axis_y, axis_z), (axis_y, axis_x, axis_z))
    mids = [
        Scatter(links, mid_own, k * part_rows, part_rows, orders[k % 2], lands[k * 3 : k * 3 + 3])
        for k in range(parts)
    ]
    mids.append(
        Scatter(links, in_own, 0, in_own.shape[0], (axis_plane, axis_z), lands[3 * parts :])
    )

    def mid_half(which, target):
        upper = delta_1[pl.ds(pl.multiple_of(which * half, half), half), :]
        block = dot_t(upper, act_0[...])
        for part in range(HID // LANES):
            target[part * half : (part + 1) * half, :] = block[:, part * LANES : (part + 1) * LANES]

    partner = axis_core.device(1 - core)
    part_span = lambda k: pl.ds(k * part_rows, part_rows)
    pairs = [
        links.copy(
            mid_away.at[part_span(k)], mid_pair.at[part_span(k)], partner, links.take(1)
        )
        for k in range(parts)
    ]
    mid_half(1 - core, mid_away)
    for pair in pairs:
        pair.start()
    mid_half(core, mid_own)
    for k in range(parts):
        pairs[k].wait()
        mid_own[part_span(k)] += mid_pair[part_span(k)]
        mids[k].start(0)

    grad_out[...] = dot_t(cot_s[...], act_1[...])[:OUT]
    outs = Total(links, grad_out, out_lands, axes)
    outs.start()
    grad_in[...] = jnp.zeros(grad_in.shape, F32)

    def lower(c):
        span = chunk_span(c)
        slope = slope_of_half(half_0[:, span])
        delta = (dot(b_mid_t[...], delta_1[:, span]) * slope).astype(BF16)
        grad_in[...] += dot_t(feats[:, span], delta)
        spread = dot(b_in_t[...], delta)
        for k in range(GROUP):
            fgrad[c * GROUP + k] = spread[:, k * SC : (k + 1) * SC]

    def advance(which, stage):
        for k in which:
            mids[k].finish(stage)
            if stage + 1 < len(mids[k].axes):
                mids[k].start(stage + 1)

    half_chunks = CHUNKS // 2
    for c in range(half_chunks):
        lower(c)
    outs.finish()
    advance((0, 1), 0)
    for c in range(half_chunks, CHUNKS - 1):
        lower(c)
    outs.finish()
    advance((2, 3), 0)
    lower(CHUNKS - 1)

    blocks = HID // LANES
    inputs = 2 * CH
    in_rows = inputs * blocks // 2

    def in_half(which, target):
        for choice in range(2):

            @pl.when(which == choice)
            def _():
                for part in range(blocks // 2):
                    at = (choice * (blocks // 2) + part) * LANES
                    target[part * inputs : (part + 1) * inputs, :] = grad_in[:, at : at + LANES]
        if target.shape[0] > in_rows:
            target[in_rows:, :] = jnp.zeros((target.shape[0] - in_rows, LANES), F32)

    in_half(1 - core, in_away)
    pair_in = links.copy(in_away, in_pair, partner, links.take(1))
    pair_in.start()
    in_half(core, in_own)

    advance((0, 1), 1)

    last = SR
    bottom = None
    packed = jnp.zeros((CH, LANES), F32)
    zero = jnp.zeros((CH, LANES), F32)
    for r in range(SR + 1):
        value = zero
        if r < SR:
            value = (1.0 - off_y) * fgrad[r, :CH]
        if r > 0:
            value = value + off_y * fgrad[r - 1, :CH]
        moved = off_x * roll(value, 1)
        out = (1.0 - off_x) * value + jnp.where(lane == 0, 0.0, moved)
        at = r if r < SR else SR + CR
        packed = jnp.where(lane == at, roll(moved, at), packed)
        if r < SR:
            fine_g[r] = out
        else:
            down_buf[0] = out
    for j in range(CR + 1):
        value = zero
        for k in range(RATIO):
            part = (k + off_y) / RATIO
            if j < CR:
                value = value + (1.0 - part) * fgrad[j * RATIO + k, CH:]
            if j > 0:
                value = value + part * fgrad[(j - 1) * RATIO + k, CH:]
        coarse_s[j] = value
    spread = dot_t(
        coarse_s[...].reshape((CR + 1) * CH, LANES), table, precision=lax.Precision.HIGHEST
    ).reshape(CR + 1, CH, LANES)
    for j in range(CR + 1):
        value = spread[j]
        at = SR + j if j < CR else SR + CR + 1
        packed = jnp.where(lane == at, roll(value, at - CC), packed)
        value = jnp.where(lane < CC, value, 0.0)
        if j < CR:
            coarse_g[j] = value
        else:
            down_buf[1] = value
    q_buf[...] = packed
    waits = [
        halo(down_buf, above_buf, "down", "up"),
        halo(q_buf, left_q, "right", "left"),
        halo(q_buf, diag_q, "down_right", "up_left"),
    ]
    for target, back in ((above_buf, "up"), (left_q, "left"), (diag_q, "up_left")):

        @pl.when(jnp.logical_not(near[back][0]))
        def _():
            target[...] = jnp.zeros(target.shape, F32)

    advance((2, 3), 1)
    outs.finish()
    pair_in.wait()
    in_own[...] += in_pair[...]
    mids[parts].start(0)
    gathers = [Gather(scatter, mid_full.at[core]) for scatter in mids[:parts]]
    gathers.append(Gather(mids[parts], in_full.at[core]))

    def settle(which):
        for k in which:
            last_stage = len(mids[k].axes) - 1
            mids[k].finish(last_stage)
            gathers[k].place()
            gathers[k].start(last_stage)

    def regain(which, stage):
        for k in which:
            gathers[k].finish(stage)
            if stage > 0:
                gathers[k].start(stage - 1)

    settle((0, 1))
    for wait in waits:
        wait()
    fine_g[0] += above_buf[0] + jnp.where(lane == 0, roll(diag_q[...], -(SR + CR)), 0.0)
    coarse_g[0] += above_buf[1] + jnp.where(lane == 0, roll(diag_q[...], -(SR + CR + 1)), 0.0)
    squares = jnp.zeros((CH, LANES), F32)
    for r in range(SR):
        value = fine_g[r] + jnp.where(lane == 0, roll(left_q[...], -r), 0.0)
        fine_g[r] = value
        squares += value * value
    for j in range(CR):
        value = coarse_g[j] + jnp.where(lane == 0, roll(left_q[...], -(SR + j)), 0.0)
        coarse_g[j] = value
        squares += value * value
    total = squares[:SUBLANES]
    for part in range(1, CH // SUBLANES):
        total = total + squares[part * SUBLANES : (part + 1) * SUBLANES]
    total_mine[...] = jnp.sum(total, axis=0, keepdims=True)
    totals = Total(links, total_mine, total_lands, (axis_core, axis_chips))
    totals.start()
    advance((parts,), 0)
    settle((2, 3))
    totals.finish()
    regain((0, 1), 2)
    settle((parts,))
    out_full[...] = outs.finish()
    regain((2, 3), 2)
    regain((0, 1), 1)
    regain((2, 3), 1)
    regain((parts,), 1)
    grid_total = totals.finish()

    for load in loads_late:
        load.wait()
    fine_first, fine_second, coarse_first, coarse_second = late
    entries = CH * (SR * SC + CR * CC) * rows_n * cols_n
    grid_scale = clip_factor(jnp.sum(grid_total, keepdims=True), entries)
    for r in range(SR):
        span = pl.ds(r, CH, stride=SR)
        fine_out[span, :] = adam_step(fine_g[r], fine_first[span, :], fine_second[span, :], grid_scale)
    for j in range(CR):
        span = pl.ds(j, CH, stride=CR)
        coarse_out[span, :] = adam_step(
            coarse_g[j, :, :CC], coarse_first[span, :], coarse_second[span, :], grid_scale
        )
    def across_pair(k):
        block = mid_full.at[core, part_span(k)]
        copy = links.copy(block, block, partner, links.take(1))
        copy.start()
        return copy

    lasts = []
    for k in range(parts):
        gathers[k].finish(0)
        lasts.append(across_pair(k))
        if k == 1:
            gathers[parts].finish(0)
            last_in = links.copy(in_full.at[core], in_full.at[core], partner, links.take(1))
            last_in.start()
            lasts.append(last_in)
    for copy in lasts:
        copy.wait()
    assert links.used <= dims["COPIES"]


def adam_kernel(
    fine_step,
    coarse_step,
    mid_full,
    in_full,
    out_full,
    in_first,
    in_second,
    mid_first,
    mid_second,
    out_first,
    out_second,
    fine_out,
    coarse_out,
    in_out,
    mid_out,
    out_out,
    in_step,
    mid_step,
    out_step,
    sems,
):
    writes = []

    def write(source, target):
        copy = pltpu.make_async_copy(source, target, sems.at[len(writes)])
        copy.start()
        writes.append(copy)

    write(fine_step, fine_out)
    write(coarse_step, coarse_out)
    inputs, hidden = in_step.shape
    outputs = out_step.shape[0]
    half, blocks = hidden // 2, hidden // LANES
    parts = [mid_full[which, :, :] for which in range(2)]
    parts += [in_full[which, : inputs * blocks // 2, :] for which in range(2)]
    squares = jnp.zeros((SUBLANES, LANES), F32)
    for value in parts:
        value = (value * value).reshape(-1, SUBLANES, LANES)
        squares += jnp.sum(value, axis=0)
    total = jnp.sum(squares, keepdims=True) + jnp.sum(out_full[...] * out_full[...], keepdims=True)
    scale = clip_factor(total, hidden * (hidden + inputs + outputs))
    for which in range(2):
        span = slice(which * half, (which + 1) * half)
        for part in range(blocks):
            lanes = slice(part * LANES, (part + 1) * LANES)
            mid_step[span, lanes] = adam_step(
                mid_full[which, part * half : (part + 1) * half, :],
                mid_first[span, lanes],
                mid_second[span, lanes],
                scale,
            )
        write(mid_step.at[pl.ds(which * half, half)], mid_out.at[pl.ds(which * half, half)])
    out_step[...] = adam_step(out_full[...], out_first[...], out_second[...], scale)
    write(out_step, out_out)
    for which in range(2):
        for part in range(blocks // 2):
            at = (which * (blocks // 2) + part) * LANES
            lanes = slice(at, at + LANES)
            in_step[:, lanes] = adam_step(
                in_full[which, part * inputs : (part + 1) * inputs, :],
                in_first[:, lanes],
                in_second[:, lanes],
                scale,
            )
    write(in_step, in_out)
    for copy in writes:
        copy.wait()


def shards(
    offsets,
    targets,
    grid_fine,
    grid_coarse,
    weight_in,
    weight_mid,
    weight_out,
    fine_first,
    fine_second,
    coarse_first,
    coarse_second,
    in_first,
    in_second,
    mid_first,
    mid_second,
    out_first,
    out_second,
):
    CH, SR, SC = grid_fine.shape
    CR, CC = grid_coarse.shape[1:]
    HID = weight_in.shape[0]
    OUT = weight_out.shape[0]
    S = SR * SC
    rows_n, cols_n = lax.axis_size("row"), lax.axis_size("col")
    sizes_x, sizes_y, sizes_z = 2, cols_n // 2, rows_n // 2
    peers = (sizes_x - 1) + (sizes_y - 1) + (sizes_z - 1)
    parts = 4
    copies = 2 * parts * (peers + 1) + 2 * (sizes_x * sizes_y + sizes_z) + 24
    chips = sizes_x * sizes_y * sizes_z
    in_rows = CH * HID // LANES
    in_rows = -(-in_rows // (chips * SUBLANES)) * chips * SUBLANES
    mid_rows = HID * HID // 2 // LANES
    dims = dict(CH=CH, SR=SR, SC=SC, CR=CR, CC=CC, HID=HID, OUT=OUT, COPIES=copies, GROUP=8)

    flat = lambda grid: grid.reshape(-1, grid.shape[-1])
    early = (
        flat(targets),
        flat(grid_fine),
        flat(grid_coarse),
        weight_in.T,
        weight_mid[0],
        weight_out,
    )
    late = (flat(fine_first), flat(fine_second), flat(coarse_first), flat(coarse_second))
    vmem = lambda *shape: pltpu.VMEM(shape, F32)
    low = lambda *shape: pltpu.VMEM(shape, BF16)

    def landing(rows, sizes):
        found = []
        for size in sizes:
            rows = rows // size
            found.append(vmem(max(size - 1, 1), rows, LANES))
        return found

    orders = ((sizes_x, sizes_y, sizes_z), (sizes_y, sizes_x, sizes_z))
    kept = (in_first.T, in_second.T, mid_first[0], mid_second[0], out_first, out_second)
    scratch = [pltpu.SMEM(offsets.shape, jnp.int32)]
    scratch += [pltpu.VMEM(a.shape, F32) for a in early + late]
    scratch += [
        vmem(2, CH, LANES),
        vmem(CH, LANES),
        vmem(2, CH, LANES),
        vmem(CH, LANES),
        vmem(CH, LANES),
        vmem(CR + 1, CH, LANES),
        vmem(SR + 1, CH, LANES),
        vmem(CR + 1, CH, LANES),
        low(HID, 2 * CH),
        low(2 * CH, HID),
        low(HID, HID),
        low(HID, HID),
        low(SUBLANES, HID),
        low(HID, SUBLANES),
        low(2 * CH, S),
        low(HID, S),
        low(HID, S),
        vmem(HID, S),
        vmem(HID, S),
        low(HID, S),
        vmem(SR + 2, SUBLANES, LANES),
        vmem(2, 2, SUBLANES, LANES),
        vmem(2, 2, SUBLANES, LANES),
        vmem(2, 3, SUBLANES, LANES),
        vmem(2, 3, SUBLANES, LANES),
        low(SUBLANES, S),
        vmem(SR, 2 * CH, LANES),
        vmem(2, CH, LANES),
        vmem(CH, LANES),
        vmem(2, CH, LANES),
        vmem(CH, LANES),
        vmem(CH, LANES),
        vmem(SR, CH, LANES),
        vmem(CR, CH, LANES),
        vmem(2 * CH, HID),
        vmem(OUT, HID),
        vmem(mid_rows, LANES),
        vmem(mid_rows, LANES),
        vmem(mid_rows, LANES),
        vmem(in_rows, LANES),
        vmem(in_rows, LANES),
        vmem(in_rows, LANES),
        vmem(1, LANES),
    ]
    scratch += [vmem(size, OUT, HID) for size in (2, sizes_x, sizes_y, sizes_z)]
    scratch += [vmem(size, 1, LANES) for size in (2, chips)]
    for part in range(parts):
        scratch += landing(mid_rows // parts, orders[part % 2])
    scratch += landing(in_rows, (sizes_x * sizes_y, sizes_z))
    scratch += [
        pltpu.SemaphoreType.DMA((len(early) + len(late) + len(kept) + 1,)),
        pltpu.SemaphoreType.DMA((copies,)),
        pltpu.SemaphoreType.DMA((copies,)),
        pltpu.SemaphoreType.REGULAR((2,)),
    ]
    outs = (
        (CH * SR, SC),
        (CH * CR, CC),
        (2, mid_rows, LANES),
        (2, in_rows, LANES),
        (OUT, HID),
    ) + tuple(a.shape for a in kept)
    far = pl.BlockSpec(memory_space=pltpu.HBM)
    whole = pl.BlockSpec(memory_space=pltpu.VMEM)
    found = pl.pallas_call(
        functools.partial(step_kernel, dims),
        out_shape=[jax.ShapeDtypeStruct(shape, F32) for shape in outs],
        in_specs=[far] * (1 + len(early) + len(late) + len(kept)),
        out_specs=[whole] * len(outs),
        scratch_shapes=scratch,
        compiler_params=pltpu.CompilerParams(
            collective_id=0, has_side_effects=True, vmem_limit_bytes=48 * 1024 * 1024
        ),
        name="field",
    )(*[pltpu.with_memory_space_constraint(a, pltpu.HBM) for a in (offsets, *early, *late, *kept)])
    steps = ((CH * SR, SC), (CH * CR, CC), (2 * CH, HID), (HID, HID), (OUT, HID))
    fine_step, coarse_step, in_step, mid_step, out_step = pl.pallas_call(
        adam_kernel,
        out_shape=[jax.ShapeDtypeStruct(shape, F32) for shape in steps],
        in_specs=[whole] * len(found),
        out_specs=[far] * len(steps),
        scratch_shapes=[pltpu.VMEM(shape, F32) for shape in steps[2:]]
        + [pltpu.SemaphoreType.DMA((4 + 2 * HID // LANES,))],
        compiler_params=pltpu.CompilerParams(vmem_limit_bytes=8 * 1024 * 1024),
        name="adam",
    )(*found)
    return (
        fine_step.reshape(grid_fine.shape),
        coarse_step.reshape(grid_coarse.shape),
        in_step.T,
        mid_step[None],
        out_step,
    )


def solution(mesh):
    tile, copied = P(None, "row", "col"), P()
    placed = (P("row", "col", None), P(None, None, "row", "col"), tile, tile)
    placed += (copied,) * 3 + (tile,) * 4 + (copied,) * 6
    return jax.shard_map(
        shards,
        mesh=mesh,
        in_specs=placed,
        out_specs=(tile, tile, copied, copied, copied),
        check_vma=False,
    )
```

```python
import functools

import jax
import jax.numpy as jnp
from jax import lax
from jax.experimental import pallas as pl
from jax.experimental.pallas import tpu as pltpu
from jax.sharding import PartitionSpec as P

SUB = 4
RATIO = 4
ADAM_STEP = 10
BETA_ONE = 0.9
BETA_TWO = 0.99
ADAM_EPSILON = 1e-08
CLIP_RMS = 0.01
LOSS_VALUE = 0.25
MEAN_EPSILON = 1e-06

MESH = pl.DeviceIdType.MESH
LANES = 128
SUBLANES = 8
F32 = jnp.float32
BF16 = jnp.bfloat16


def clip_factor(total, entries):
    return jnp.minimum(1.0, CLIP_RMS / jnp.sqrt(total / entries + MEAN_EPSILON))


def adam_step(gradient, moment_one, moment_two, clip_scale):
    rise_one = 1.0 / (1.0 - BETA_ONE**ADAM_STEP)
    rise_two = 1.0 / (1.0 - BETA_TWO**ADAM_STEP)
    new_one = (BETA_ONE * rise_one) * moment_one + gradient * (
        clip_scale * ((1.0 - BETA_ONE) * rise_one)
    )
    root = gradient * (clip_scale * ((1.0 - BETA_TWO) * rise_two) ** 0.5)
    new_two = (BETA_TWO * rise_two) * moment_two + root * root
    return new_one / (jnp.sqrt(new_two) + ADAM_EPSILON)


def dot(former, latter, dims=((1,), (0,)), precision=None):
    return lax.dot_general(
        former, latter, (dims, ((), ())), preferred_element_type=F32, precision=precision
    )


def dot_t(former, latter, precision=None):
    return dot(former, latter, ((1,), (1,)), precision)


def silu_of_half(half):
    return half + half * jnp.tanh(half)


def slope_of_half(half):
    bend = jnp.tanh(half)
    return (1.0 + bend) * ((1.0 + half) - half * bend)


class Axis:
    def __init__(self, me, size, device):
        self.me, self.size, self.device = me, size, device

    def peer(self, step):
        return lax.rem(self.me + step, self.size)


def aligned(start):
    return pl.multiple_of(start, SUBLANES)


class Links:
    def __init__(self, send, recv):
        self.send, self.recv, self.sends, self.recvs = send, recv, 0, 0

    def take(self):
        self.recvs += 1
        return self.recvs - 1

    def take_send(self):
        self.sends += 1
        return self.sends - 1

    def copy(self, source, target, device, slot, send):
        return pltpu.make_async_remote_copy(
            src_ref=source,
            dst_ref=target,
            send_sem=self.send.at[send],
            recv_sem=self.recv.at[slot],
            device_id=device,
            device_id_type=MESH,
        )

    def wait(self, sent, landed, device, slot, send):
        self.copy(sent, sent, device, slot, send).wait_send()
        self.copy(landed, landed, device, slot, send).wait_recv()


class Scatter:
    def __init__(self, links, own, start, rows, axes, lands):
        self.links, self.own, self.axes, self.lands = links, own, axes, lands
        self.spans = [(start, rows)]
        for axis in axes:
            start, rows = self.spans[-1]
            part = rows // axis.size
            self.spans.append((start + axis.me * part, part))
        self.slots = [links.take() for axis in axes]
        self.send = links.take_send()

    def start(self, stage):
        axis, start, part = self.axes[stage], self.spans[stage][0], self.spans[stage + 1][1]
        for step in range(1, axis.size):
            peer = axis.peer(step)
            self.links.copy(
                self.own.at[pl.ds(aligned(start + peer * part), part)],
                self.lands[stage].at[step - 1],
                axis.device(peer),
                self.slots[stage],
                self.send,
            ).start()

    def finish(self, stage):
        axis, land = self.axes[stage], self.lands[stage]
        start, part = self.spans[stage + 1]
        if axis.size > 1:
            sent = self.own.at[pl.ds(0, (axis.size - 1) * part)]
            device = axis.device(axis.peer(1))
            self.links.wait(sent, land, device, self.slots[stage], self.send)
        span = pl.ds(aligned(start), part)
        found = self.own[span]
        for step in range(axis.size - 1):
            found = found + land[step]
        self.own[span] = found


class Gather:
    def __init__(self, scatter, full):
        self.scatter, self.full = scatter, full
        self.slots = [scatter.links.take() for axis in scatter.axes]

    def place(self):
        start, rows = self.scatter.spans[-1]
        span = pl.ds(aligned(start), rows)
        self.full[span] = self.scatter.own[span]

    def start(self, stage):
        axis = self.scatter.axes[stage]
        start, rows = self.scatter.spans[stage + 1]
        block = self.full.at[pl.ds(aligned(start), rows)]
        for step in range(1, axis.size):
            device = axis.device(axis.peer(step))
            self.scatter.links.copy(
                block, block, device, self.slots[stage], self.scatter.send
            ).start()

    def finish(self, stage):
        axis, rows = self.scatter.axes[stage], self.scatter.spans[stage + 1][1]
        if axis.size > 1:
            span = self.full.at[pl.ds(0, (axis.size - 1) * rows)]
            device = axis.device(axis.peer(1))
            self.scatter.links.wait(span, span, device, self.slots[stage], self.scatter.send)


class Total:
    def __init__(self, links, mine, lands, axes):
        self.links, self.mine, self.lands, self.axes = links, mine, lands, axes
        self.slots = [links.take() for axis in axes]
        self.send = links.take_send()
        self.stage = 0

    def start(self):
        axis, land, slot = self.axes[self.stage], self.lands[self.stage], self.slots[self.stage]
        land[axis.me] = self.mine[...]

        @pl.loop(1, axis.size)
        def _(step):
            device = axis.device(axis.peer(step))
            self.links.copy(self.mine, land.at[axis.me], device, slot, self.send).start()

    def finish(self):
        axis, land, slot = self.axes[self.stage], self.lands[self.stage], self.slots[self.stage]
        if axis.size > 1:
            span = land.at[pl.ds(0, axis.size - 1)]
            self.links.wait(span, span, axis.device(axis.peer(1)), slot, self.send)
        total = land[0]
        for place in range(1, axis.size):
            total = total + land[place]
        self.stage += 1
        if self.stage < len(self.axes):
            self.mine[...] = total
            self.start()
        return total


def step_kernel(dims, *refs):
    refs = iter(refs)
    take = lambda count: [next(refs) for _ in range(count)]
    (offsets_hbm,) = take(1)
    early_hbm = take(6)
    late_hbm = take(4)
    kept_hbm = take(6)
    fine_out, coarse_out, mid_full, in_full, out_full = take(5)
    kept = take(6)
    (offsets_ref,) = take(1)
    targets, fine, coarse, w_in, w_mid, w_out = early = take(6)
    late = take(4)
    (
        up_buf,
        cp_buf,
        below_buf,
        right_cp,
        diag_cp,
        coarse_s,
        across,
        across_c,
        b_in,
        b_in_t,
        b_mid,
        b_mid_t,
        b_out,
        b_out_t,
        feats,
        act_0,
        act_1,
        half_0,
        half_1,
        delta_1,
        pred,
        edge_send,
        edge_recv,
        col_send,
        col_recv,
        cot_s,
        fgrad,
        down_buf,
        q_buf,
        above_buf,
        left_q,
        diag_q,
        fine_g,
        coarse_g,
        grad_in,
        grad_out,
        mid_away,
        mid_own,
        mid_pair,
        in_away,
        in_own,
        in_pair,
        total_mine,
    ) = take(43)
    out_lands = take(4)
    total_lands = take(2)
    lands = take(14)
    load_sem, send_sem, recv_sem, know_sem = take(4)

    rows_n, cols_n = lax.axis_size("row"), lax.axis_size("col")
    row, col = lax.axis_index("row"), lax.axis_index("col")
    CH, SR, SC, CR, CC, HID, OUT = (dims[k] for k in ("CH", "SR", "SC", "CR", "CC", "HID", "OUT"))
    S = SR * SC
    CHUNK = dims["GROUP"] * SC
    CHUNKS = S // CHUNK
    GROUP = dims["GROUP"]

    core, plane = lax.rem(col, 2), lax.div(col, 2)
    x_at, z_at = lax.rem(row, 2), lax.div(row, 2)
    axis_core = Axis(core, 2, lambda p: (row, plane * 2 + p))
    axis_x = Axis(x_at, 2, lambda p: (z_at * 2 + p, col))
    axis_y = Axis(plane, cols_n // 2, lambda p: (row, p * 2 + core))
    axis_z = Axis(z_at, rows_n // 2, lambda p: (p * 2 + x_at, col))
    axes = (axis_core, axis_x, axis_y, axis_z)
    planes = cols_n // 2
    axis_plane = Axis(
        x_at * planes + plane,
        2 * planes,
        lambda p: (z_at * 2 + lax.div(p, planes), lax.rem(p, planes) * 2 + core),
    )
    axis_chips = Axis(
        row * planes + plane,
        rows_n * planes,
        lambda p: (lax.div(p, planes), lax.rem(p, planes) * 2 + core),
    )

    has_up, has_down = row > 0, row < rows_n - 1
    has_left, has_right = col > 0, col < cols_n - 1
    near = {
        "up": (has_up, (row - 1, col)),
        "down": (has_down, (row + 1, col)),
        "left": (has_left, (row, col - 1)),
        "right": (has_right, (row, col + 1)),
        "up_left": (jnp.logical_and(has_up, has_left), (row - 1, col - 1)),
        "down_right": (jnp.logical_and(has_down, has_right), (row + 1, col + 1)),
    }
    links = Links(send_sem, recv_sem)

    loads = [
        pltpu.make_async_copy(source, target, load_sem.at[place])
        for place, (source, target) in enumerate(
            zip(
                early_hbm + late_hbm + kept_hbm + [offsets_hbm],
                early + late + kept + [offsets_ref],
            )
        )
    ]
    loads_early, loads_late, load_offsets = loads[:6], loads[6:-1], loads[-1]
    load_offsets.start()
    for place in (1, 2, 3, 4, 5, 0):
        loads_early[place].start()
    barrier = pltpu.get_barrier_semaphore()
    z_near = ((z_at > 0, (row - 2, col)), (z_at < axis_z.size - 1, (row + 2, col)))
    expected = sum(axis.size - 1 for axis in axes[:3])
    for axis in axes[:3]:
        for step in range(1, axis.size):
            pl.semaphore_signal(
                barrier, inc=1, device_id=axis.device(axis.peer(step)), device_id_type=MESH
            )
    for there, device in list(near.values()) + list(z_near):
        expected = expected + there.astype(jnp.int32)

        @pl.when(there)
        def _():
            pl.semaphore_signal(barrier, inc=1, device_id=device, device_id_type=MESH)

    for load in loads_late:
        load.start()

    lane = lax.broadcasted_iota(jnp.int32, (CH, LANES), 1)
    lane_8 = lax.broadcasted_iota(jnp.int32, (SUBLANES, LANES), 1)
    load_offsets.wait()
    off_y = offsets_ref[0, 0, 0].astype(F32) / SUB
    off_x = offsets_ref[0, 0, 1].astype(F32) / SUB

    def fine_row(r):
        return fine[pl.ds(r, CH, stride=SR), :]

    def roll(value, shift):
        return pltpu.roll(value, shift % LANES, 1)

    coarse_s[...] = jnp.zeros(coarse_s.shape, F32)
    loads_early[1].wait()
    loads_early[2].wait()
    for r in range(CR):
        coarse_s[r, :, :CC] = coarse[pl.ds(r, CH, stride=CR), :]
    up_buf[:CH] = fine_row(0)
    group = CH * CC // LANES
    side = [slice(k * group, (k + 1) * group) for k in range(LANES // CC)]

    def pack(value):
        return sum(roll(value[side[k]], k * CC) for k in range(LANES // CC))

    def unpack(value, target):
        kept = lax.broadcasted_iota(jnp.int32, (group, LANES), 1) < CC
        for k in range(LANES // CC):
            target[side[k]] = jnp.where(kept, roll(value, -k * CC), 0.0)

    up_buf[CH:] = pack(coarse_s[0])
    packed = jnp.zeros((CH, LANES), F32)
    for r in range(SR):
        packed = jnp.where(lane == r, roll(fine_row(r), r), packed)
    for r in range(CR):
        packed = jnp.where(lane == SR + r, roll(coarse_s[r], SR + r), packed)
    cp_buf[...] = packed

    pl.semaphore_wait(barrier, expected)

    halo_sends = [links.take_send() for _ in range(6)]
    halos_used = [0]

    def halo(source, target, towards, back):
        slot, send = links.take(), halo_sends[halos_used[0] % 6]
        halos_used[0] += 1
        copy = links.copy(source, target, near[towards][1], slot, send)
        arriving = links.copy(source, target, near[back][1], slot, send)

        @pl.when(near[towards][0])
        def _():
            copy.start()

        def finish():
            @pl.when(near[towards][0])
            def _():
                copy.wait_send()

            @pl.when(near[back][0])
            def _():
                arriving.wait_recv()

        return finish

    waits = [
        halo(up_buf, below_buf, "up", "down"),
        halo(cp_buf, right_cp, "left", "right"),
        halo(cp_buf, diag_cp, "up_left", "down_right"),
    ]
    for target, back in ((below_buf, "down"), (right_cp, "right"), (diag_cp, "down_right")):

        @pl.when(jnp.logical_not(near[back][0]))
        def _():
            target[...] = jnp.zeros(target.shape, F32)

    loads_early[3].wait()
    loads_early[4].wait()
    loads_early[5].wait()
    b_in_t[...] = w_in[...].astype(BF16)
    b_in[...] = (0.5 * w_in[...]).T.astype(BF16)
    halved = 0.5 * w_mid[...]
    b_mid[...] = halved.astype(BF16)
    b_mid_t[...] = halved.T.astype(BF16)
    padded_out = jnp.concatenate([w_out[...], jnp.zeros((SUBLANES - OUT, HID), F32)], axis=0)
    b_out[...] = padded_out.astype(BF16)
    b_out_t[...] = (0.5 * padded_out).T.astype(BF16)
    cot_s[...] = jnp.zeros(cot_s.shape, BF16)
    vertex = lax.broadcasted_iota(jnp.int32, (LANES, LANES), 0)
    sample = lax.broadcasted_iota(jnp.int32, (LANES, LANES), 1)
    base = lax.div(sample, RATIO)
    fraction = (lax.rem(sample, RATIO).astype(F32) + off_x) / RATIO
    table = jnp.where(vertex == base, 1.0 - fraction, 0.0) + jnp.where(
        vertex == base + 1, fraction, 0.0
    )
    for wait in waits:
        wait()

    for r in range(SR + 1):
        value = fine_row(r) if r < SR else below_buf[:CH]
        edge = roll(right_cp[...], LANES - 1 - r) if r < SR else roll(diag_cp[...], LANES - 1)
        shifted = jnp.where(lane == LANES - 1, edge, roll(value, LANES - 1))
        across[r] = (1.0 - off_x) * value + off_x * shifted
    unpack(below_buf[CH:], coarse_s.at[CR])
    for r in range(CR + 1):
        value = coarse_s[r]
        edge = roll(right_cp[...], CC - SR - r) if r < CR else roll(diag_cp[...], CC - SR)
        coarse_s[r] = jnp.where(lane == CC, edge, value)
    across_c[...] = dot(
        coarse_s[...].reshape((CR + 1) * CH, LANES), table, precision=lax.Precision.HIGHEST
    ).reshape(CR + 1, CH, LANES)

    def chunk_span(c):
        return slice(c * CHUNK, (c + 1) * CHUNK)

    def tell(place, targets):
        for there, device in targets:

            @pl.when(there)
            def _():
                pl.semaphore_signal(
                    know_sem.at[place], inc=1, device_id=device, device_id_type=MESH
                )

    def hear(place, targets):
        pl.semaphore_wait(know_sem.at[place], sum(there.astype(jnp.int32) for there, _ in targets))

    def peers_of(axis):
        always = row >= 0
        return [(always, axis.device(axis.peer(step))) for step in range(1, axis.size)]

    words = [z_near] * max(axis_z.size - 2, 0) + [peers_of(axis_x), peers_of(axis_y)]
    words = [targets for targets in words if targets]
    heard = [0]

    def pass_word(count):
        for _ in range(count):
            if heard[0] < len(words):
                hear(heard[0], words[heard[0]])
                heard[0] += 1
                if heard[0] < len(words):
                    tell(heard[0], words[heard[0]])

    def forward(c):
        for k in range(GROUP):
            i = c * GROUP + k
            j = c * (GROUP // RATIO) + k // RATIO
            span = slice(i * SC, (i + 1) * SC)
            part = (k % RATIO + off_y) / RATIO
            feats[:CH, span] = ((1.0 - off_y) * across[i] + off_y * across[i + 1]).astype(BF16)
            feats[CH:, span] = ((1.0 - part) * across_c[j] + part * across_c[j + 1]).astype(BF16)
        span = chunk_span(c)
        half_0[:, span] = dot(b_in[...], feats[:, span])
        act_0[:, span] = silu_of_half(half_0[:, span]).astype(BF16)
        half_1[:, span] = dot(b_mid[...], act_0[:, span])
        act_1[:, span] = silu_of_half(half_1[:, span]).astype(BF16)
        colours = dot(b_out[...], act_1[:, span])
        for k in range(GROUP):
            pred[c * GROUP + k + 1] = colours[:, k * SC : (k + 1) * SC]

    order = [0, CHUNKS - 1] + list(range(1, CHUNKS - 1))

    def target_row(kind, r):
        found = targets[pl.ds(kind * OUT * SR + r, OUT, stride=SR), :]
        return jnp.concatenate([found, jnp.zeros((SUBLANES - OUT, LANES), F32)], axis=0)

    def send_columns(batch, groups):
        first_col = last_col = last_aim = jnp.zeros((SUBLANES, LANES), F32)
        for c in groups:
            for r in range(c * GROUP, (c + 1) * GROUP):
                first_col = jnp.where(lane_8 == r, roll(pred[r + 1], r), first_col)
                last_col = jnp.where(lane_8 == r, roll(pred[r + 1], r + 1), last_col)
                last_aim = jnp.where(lane_8 == r, roll(target_row(2, r), r + 1), last_aim)
        col_send[batch, 0] = first_col
        col_send[batch, 1] = last_col
        col_send[batch, 2] = last_aim
        return [
            halo(col_send.at[batch, 0], col_recv.at[batch, 0], "left", "right"),
            halo(col_send.at[batch, pl.ds(1, 2)], col_recv.at[batch, pl.ds(1, 2)], "right", "left"),
        ]

    tell(0, words[0])
    for place in range(CHUNKS - 1):
        forward(order[place])
        pass_word(-(-len(words) // CHUNKS))
    loads_early[0].wait()
    edge_send[0, 0] = pred[1]
    edge_send[1, 0] = pred[SR]
    edge_send[1, 1] = target_row(1, SR - 1)
    halos_used[0] = 0
    early_waits = [
        halo(edge_send.at[0, 0], edge_recv.at[0, 0], "up", "down"),
        halo(edge_send.at[1], edge_recv.at[1], "down", "up"),
    ]
    early_waits += send_columns(0, order[:-1])
    for place, back in enumerate(("down", "up")):

        @pl.when(jnp.logical_not(near[back][0]))
        def _():
            edge_recv[place] = jnp.zeros(edge_recv.shape[1:], F32)

    forward(order[-1])
    pass_word(len(words))
    last_waits = send_columns(1, order[-1:])
    for place, back in ((0, "right"), (1, "left"), (2, "left")):

        @pl.when(jnp.logical_not(near[back][0]))
        def _():
            for batch in range(2):
                col_recv[batch, place] = jnp.zeros(col_recv.shape[2:], F32)

    ready = order[:2]
    for c in ready:
        half_1[:, chunk_span(c)] = slope_of_half(half_1[:, chunk_span(c)])
    for wait in early_waits:
        wait()
    pred[SR + 1] = edge_recv[0, 0]
    above_error = jnp.where(has_up, (pred[1] - edge_recv[1, 0]) - edge_recv[1, 1], 0.0)

    def row_error(r):
        if r < 0:
            return above_error
        error = (pred[r + 2] - pred[r + 1]) - target_row(1, r)
        return jnp.where(has_down, error, 0.0) if r == SR - 1 else error

    def cotangent(c, batch):
        prior = row_error(c * GROUP - 1)
        for r in range(c * GROUP, (c + 1) * GROUP):
            here = pred[r + 1]
            error = row_error(r)
            edge = roll(col_recv[batch, 0], LANES - 1 - r)
            beside = jnp.where(lane_8 == LANES - 1, edge, roll(here, -1))
            col_error = (beside - here) - target_row(2, r)
            closed = jnp.logical_and(lane_8 == LANES - 1, jnp.logical_not(has_right))
            col_error = jnp.where(closed, 0.0, col_error)
            before = (here - roll(col_recv[batch, 1], -r)) - roll(col_recv[batch, 2], -r)
            before = jnp.where(has_left, before, 0.0)
            col_prior = jnp.where(lane_8 == 0, before, roll(col_error, 1))
            value_error = here - target_row(0, r)
            cot = (
                2.0 * LOSS_VALUE * value_error
                + 2.0 * (prior - error)
                + 2.0 * (col_prior - col_error)
            )
            kept = lax.broadcasted_iota(jnp.int32, (SUBLANES, LANES), 0) < OUT
            cot_s[:, r * SC : (r + 1) * SC] = jnp.where(kept, cot, 0.0).astype(BF16)
            prior = error

    def upper(c):
        span = chunk_span(c)
        slope = half_1[:, span] if c in ready else slope_of_half(half_1[:, span])
        delta_1[:, span] = (dot(b_out_t[...], cot_s[:, span]) * slope).astype(BF16)

    for c in order[:-1]:
        cotangent(c, 0)
    for c in order[:-1]:
        upper(c)
    for wait in last_waits:
        wait()
    cotangent(order[-1], 1)
    upper(order[-1])

    half = HID // 2
    mid_rows = HID * half // LANES
    parts = 4
    part_rows = mid_rows // parts
    orders = ((axis_x, axis_y, axis_z), (axis_y, axis_x, axis_z))
    mids = [
        Scatter(links, mid_own, k * part_rows, part_rows, orders[k % 2], lands[k * 3 : k * 3 + 3])
        for k in range(parts)
    ]
    mids.append(
        Scatter(links, in_own, 0, in_own.shape[0], (axis_plane, axis_z), lands[3 * parts :])
    )

    def mid_half(which, target):
        upper = delta_1[pl.ds(pl.multiple_of(which * half, half), half), :]
        block = dot_t(upper, act_0[...])
        for part in range(HID // LANES):
            target[part * half : (part + 1) * half, :] = block[:, part * LANES : (part + 1) * LANES]

    partner = axis_core.device(1 - core)
    part_span = lambda k: pl.ds(k * part_rows, part_rows)
    pairs = [
        links.copy(
            mid_away.at[part_span(k)],
            mid_pair.at[part_span(k)],
            partner,
            links.take(),
            mids[k].send,
        )
        for k in range(parts)
    ]
    mid_half(1 - core, mid_away)
    for pair in pairs:
        pair.start()
    mid_half(core, mid_own)
    for k in range(parts):
        pairs[k].wait()
        mid_own[part_span(k)] += mid_pair[part_span(k)]
        mids[k].start(0)

    grad_out[...] = dot_t(cot_s[...], act_1[...])[:OUT]
    outs = Total(links, grad_out, out_lands, axes)
    outs.start()
    grad_in[...] = jnp.zeros(grad_in.shape, F32)

    def lower(c):
        span = chunk_span(c)
        slope = slope_of_half(half_0[:, span])
        delta = (dot(b_mid_t[...], delta_1[:, span]) * slope).astype(BF16)
        grad_in[...] += dot_t(feats[:, span], delta)
        spread = dot(b_in_t[...], delta)
        for k in range(GROUP):
            fgrad[c * GROUP + k] = spread[:, k * SC : (k + 1) * SC]

    def advance(which, stage):
        for k in which:
            mids[k].finish(stage)
            if stage + 1 < len(mids[k].axes):
                mids[k].start(stage + 1)

    half_chunks = CHUNKS // 2
    for c in range(half_chunks):
        lower(c)
    outs.finish()
    advance((0, 1), 0)
    for c in range(half_chunks, CHUNKS - 1):
        lower(c)
    outs.finish()
    advance((2, 3), 0)
    lower(CHUNKS - 1)

    blocks = HID // LANES
    inputs = 2 * CH
    in_rows = inputs * blocks // 2

    def in_half(which, target):
        for choice in range(2):

            @pl.when(which == choice)
            def _():
                for part in range(blocks // 2):
                    at = (choice * (blocks // 2) + part) * LANES
                    target[part * inputs : (part + 1) * inputs, :] = grad_in[:, at : at + LANES]
        if target.shape[0] > in_rows:
            target[in_rows:, :] = jnp.zeros((target.shape[0] - in_rows, LANES), F32)

    in_half(1 - core, in_away)
    pair_in = links.copy(in_away, in_pair, partner, links.take(), mids[parts].send)
    pair_in.start()
    in_half(core, in_own)

    advance((0, 1), 1)

    last = SR
    bottom = None
    packed = jnp.zeros((CH, LANES), F32)
    zero = jnp.zeros((CH, LANES), F32)
    for r in range(SR + 1):
        value = zero
        if r < SR:
            value = (1.0 - off_y) * fgrad[r, :CH]
        if r > 0:
            value = value + off_y * fgrad[r - 1, :CH]
        moved = off_x * roll(value, 1)
        out = (1.0 - off_x) * value + jnp.where(lane == 0, 0.0, moved)
        at = r if r < SR else SR + CR
        packed = jnp.where(lane == at, roll(moved, at), packed)
        if r < SR:
            fine_g[r] = out
        else:
            down_buf[:CH] = out
    for j in range(CR + 1):
        value = zero
        for k in range(RATIO):
            part = (k + off_y) / RATIO
            if j < CR:
                value = value + (1.0 - part) * fgrad[j * RATIO + k, CH:]
            if j > 0:
                value = value + part * fgrad[(j - 1) * RATIO + k, CH:]
        coarse_s[j] = value
    spread = dot_t(
        coarse_s[...].reshape((CR + 1) * CH, LANES), table, precision=lax.Precision.HIGHEST
    ).reshape(CR + 1, CH, LANES)
    for j in range(CR + 1):
        value = spread[j]
        at = SR + j if j < CR else SR + CR + 1
        packed = jnp.where(lane == at, roll(value, at - CC), packed)
        value = jnp.where(lane < CC, value, 0.0)
        if j < CR:
            coarse_g[j] = value
        else:
            down_buf[CH:] = pack(value)
    q_buf[...] = packed
    halos_used[0] = 0
    waits = [
        halo(down_buf, above_buf, "down", "up"),
        halo(q_buf, left_q, "right", "left"),
        halo(q_buf, diag_q, "down_right", "up_left"),
    ]
    for target, back in ((above_buf, "up"), (left_q, "left"), (diag_q, "up_left")):

        @pl.when(jnp.logical_not(near[back][0]))
        def _():
            target[...] = jnp.zeros(target.shape, F32)

    advance((2, 3), 1)
    outs.finish()
    pair_in.wait()
    in_own[...] += in_pair[...]
    mids[parts].start(0)
    gathers = [Gather(scatter, mid_full.at[core]) for scatter in mids[:parts]]
    gathers.append(Gather(mids[parts], in_full.at[core]))

    def settle(which):
        for k in which:
            last_stage = len(mids[k].axes) - 1
            mids[k].finish(last_stage)
            gathers[k].place()
            gathers[k].start(last_stage)

    def regain(which, stage):
        for k in which:
            gathers[k].finish(stage)
            if stage > 0:
                gathers[k].start(stage - 1)

    settle((0, 1))
    for wait in waits:
        wait()
    fine_g[0] += above_buf[:CH] + jnp.where(lane == 0, roll(diag_q[...], -(SR + CR)), 0.0)
    unpack(above_buf[CH:], coarse_s.at[0])
    coarse_g[0] += coarse_s[0] + jnp.where(lane == 0, roll(diag_q[...], -(SR + CR + 1)), 0.0)
    squares = jnp.zeros((CH, LANES), F32)
    for r in range(SR):
        value = fine_g[r] + jnp.where(lane == 0, roll(left_q[...], -r), 0.0)
        fine_g[r] = value
        squares += value * value
    for j in range(CR):
        value = coarse_g[j] + jnp.where(lane == 0, roll(left_q[...], -(SR + j)), 0.0)
        coarse_g[j] = value
        squares += value * value
    total = squares[:SUBLANES]
    for part in range(1, CH // SUBLANES):
        total = total + squares[part * SUBLANES : (part + 1) * SUBLANES]
    total_mine[...] = jnp.sum(total, axis=0, keepdims=True)
    totals = Total(links, total_mine, total_lands, (axis_core, axis_chips))
    totals.start()
    advance((parts,), 0)
    settle((2, 3))
    totals.finish()
    regain((0, 1), 2)
    settle((parts,))
    out_full[...] = outs.finish()
    regain((2, 3), 2)
    regain((0, 1), 1)
    regain((2, 3), 1)
    regain((parts,), 1)
    grid_total = totals.finish()

    for load in loads_late:
        load.wait()
    fine_first, fine_second, coarse_first, coarse_second = late
    entries = CH * (SR * SC + CR * CC) * rows_n * cols_n
    grid_scale = clip_factor(jnp.sum(grid_total, keepdims=True), entries)
    for r in range(SR):
        span = pl.ds(r, CH, stride=SR)
        fine_out[span, :] = adam_step(fine_g[r], fine_first[span, :], fine_second[span, :], grid_scale)
    for j in range(CR):
        span = pl.ds(j, CH, stride=CR)
        coarse_out[span, :] = adam_step(
            coarse_g[j, :, :CC], coarse_first[span, :], coarse_second[span, :], grid_scale
        )
    def across_pair(k):
        block = mid_full.at[core, part_span(k)]
        copy = links.copy(block, block, partner, links.take(), mids[k].send)
        copy.start()
        return copy

    lasts = []
    for k in range(parts):
        gathers[k].finish(0)
        lasts.append(across_pair(k))
        if k == 1:
            gathers[parts].finish(0)
            block = in_full.at[core]
            last_in = links.copy(block, block, partner, links.take(), mids[parts].send)
            last_in.start()
            lasts.append(last_in)
    for copy in lasts:
        copy.wait()
    assert (links.sends, links.recvs) == (dims["SENDS"], dims["RECVS"])


def adam_kernel(
    fine_step,
    coarse_step,
    mid_full,
    in_full,
    out_full,
    in_first,
    in_second,
    mid_first,
    mid_second,
    out_first,
    out_second,
    fine_out,
    coarse_out,
    in_out,
    mid_out,
    out_out,
    in_step,
    mid_step,
    out_step,
    sems,
):
    writes = []

    def write(source, target):
        copy = pltpu.make_async_copy(source, target, sems.at[len(writes)])
        copy.start()
        writes.append(copy)

    write(fine_step, fine_out)
    write(coarse_step, coarse_out)
    inputs, hidden = in_step.shape
    outputs = out_step.shape[0]
    half, blocks = hidden // 2, hidden // LANES
    parts = [mid_full[which, :, :] for which in range(2)]
    parts += [in_full[which, : inputs * blocks // 2, :] for which in range(2)]
    squares = jnp.zeros((SUBLANES, LANES), F32)
    for value in parts:
        value = (value * value).reshape(-1, SUBLANES, LANES)
        squares += jnp.sum(value, axis=0)
    total = jnp.sum(squares, keepdims=True) + jnp.sum(out_full[...] * out_full[...], keepdims=True)
    scale = clip_factor(total, hidden * (hidden + inputs + outputs))
    for which in range(2):
        span = slice(which * half, (which + 1) * half)
        for part in range(blocks):
            lanes = slice(part * LANES, (part + 1) * LANES)
            mid_step[span, lanes] = adam_step(
                mid_full[which, part * half : (part + 1) * half, :],
                mid_first[span, lanes],
                mid_second[span, lanes],
                scale,
            )
        write(mid_step.at[pl.ds(which * half, half)], mid_out.at[pl.ds(which * half, half)])
    out_step[...] = adam_step(out_full[...], out_first[...], out_second[...], scale)
    write(out_step, out_out)
    for which in range(2):
        for part in range(blocks // 2):
            at = (which * (blocks // 2) + part) * LANES
            lanes = slice(at, at + LANES)
            in_step[:, lanes] = adam_step(
                in_full[which, part * inputs : (part + 1) * inputs, :],
                in_first[:, lanes],
                in_second[:, lanes],
                scale,
            )
    write(in_step, in_out)
    for copy in writes:
        copy.wait()


def shards(
    offsets,
    targets,
    grid_fine,
    grid_coarse,
    weight_in,
    weight_mid,
    weight_out,
    fine_first,
    fine_second,
    coarse_first,
    coarse_second,
    in_first,
    in_second,
    mid_first,
    mid_second,
    out_first,
    out_second,
):
    CH, SR, SC = grid_fine.shape
    CR, CC = grid_coarse.shape[1:]
    HID = weight_in.shape[0]
    OUT = weight_out.shape[0]
    S = SR * SC
    rows_n, cols_n = lax.axis_size("row"), lax.axis_size("col")
    sizes_x, sizes_y, sizes_z = 2, cols_n // 2, rows_n // 2
    parts = 4
    sends, recvs = 6 + parts + 1 + 2, 12 + 6 + 2 * (parts + 1) + 2 * (3 * parts + 2)
    chips = sizes_x * sizes_y * sizes_z
    in_rows = CH * HID // LANES
    in_rows = -(-in_rows // (chips * SUBLANES)) * chips * SUBLANES
    mid_rows = HID * HID // 2 // LANES
    dims = dict(CH=CH, SR=SR, SC=SC, CR=CR, CC=CC, HID=HID, OUT=OUT, SENDS=sends, RECVS=recvs, GROUP=8)

    flat = lambda grid: grid.reshape(-1, grid.shape[-1])
    early = (
        flat(targets),
        flat(grid_fine),
        flat(grid_coarse),
        weight_in.T,
        weight_mid[0],
        weight_out,
    )
    late = (flat(fine_first), flat(fine_second), flat(coarse_first), flat(coarse_second))
    vmem = lambda *shape: pltpu.VMEM(shape, F32)
    low = lambda *shape: pltpu.VMEM(shape, BF16)

    def landing(rows, sizes):
        found = []
        for size in sizes:
            rows = rows // size
            found.append(vmem(max(size - 1, 1), rows, LANES))
        return found

    orders = ((sizes_x, sizes_y, sizes_z), (sizes_y, sizes_x, sizes_z))
    kept = (in_first.T, in_second.T, mid_first[0], mid_second[0], out_first, out_second)
    edge = CH + CH * CC // LANES
    scratch = [pltpu.SMEM(offsets.shape, jnp.int32)]
    scratch += [pltpu.VMEM(a.shape, F32) for a in early + late]
    scratch += [
        vmem(edge, LANES),
        vmem(CH, LANES),
        vmem(edge, LANES),
        vmem(CH, LANES),
        vmem(CH, LANES),
        vmem(CR + 1, CH, LANES),
        vmem(SR + 1, CH, LANES),
        vmem(CR + 1, CH, LANES),
        low(HID, 2 * CH),
        low(2 * CH, HID),
        low(HID, HID),
        low(HID, HID),
        low(SUBLANES, HID),
        low(HID, SUBLANES),
        low(2 * CH, S),
        low(HID, S),
        low(HID, S),
        vmem(HID, S),
        vmem(HID, S),
        low(HID, S),
        vmem(SR + 2, SUBLANES, LANES),
        vmem(2, 2, SUBLANES, LANES),
        vmem(2, 2, SUBLANES, LANES),
        vmem(2, 3, SUBLANES, LANES),
        vmem(2, 3, SUBLANES, LANES),
        low(SUBLANES, S),
        vmem(SR, 2 * CH, LANES),
        vmem(edge, LANES),
        vmem(CH, LANES),
        vmem(edge, LANES),
        vmem(CH, LANES),
        vmem(CH, LANES),
        vmem(SR, CH, LANES),
        vmem(CR, CH, LANES),
        vmem(2 * CH, HID),
        vmem(OUT, HID),
        vmem(mid_rows, LANES),
        vmem(mid_rows, LANES),
        vmem(mid_rows, LANES),
        vmem(in_rows, LANES),
        vmem(in_rows, LANES),
        vmem(in_rows, LANES),
        vmem(1, LANES),
    ]
    scratch += [vmem(size, OUT, HID) for size in (2, sizes_x, sizes_y, sizes_z)]
    scratch += [vmem(size, 1, LANES) for size in (2, chips)]
    for part in range(parts):
        scratch += landing(mid_rows // parts, orders[part % 2])
    scratch += landing(in_rows, (sizes_x * sizes_y, sizes_z))
    scratch += [
        pltpu.SemaphoreType.DMA((len(early) + len(late) + len(kept) + 1,)),
        pltpu.SemaphoreType.DMA((sends,)),
        pltpu.SemaphoreType.DMA((recvs,)),
        pltpu.SemaphoreType.REGULAR((max(sizes_z - 2, 0) + 2,)),
    ]
    outs = (
        (CH * SR, SC),
        (CH * CR, CC),
        (2, mid_rows, LANES),
        (2, in_rows, LANES),
        (OUT, HID),
    ) + tuple(a.shape for a in kept)
    far = pl.BlockSpec(memory_space=pltpu.HBM)
    whole = pl.BlockSpec(memory_space=pltpu.VMEM)
    found = pl.pallas_call(
        functools.partial(step_kernel, dims),
        out_shape=[jax.ShapeDtypeStruct(shape, F32) for shape in outs],
        in_specs=[far] * (1 + len(early) + len(late) + len(kept)),
        out_specs=[whole] * len(outs),
        scratch_shapes=scratch,
        compiler_params=pltpu.CompilerParams(
            collective_id=0, has_side_effects=True, vmem_limit_bytes=48 * 1024 * 1024
        ),
        name="field",
    )(*[pltpu.with_memory_space_constraint(a, pltpu.HBM) for a in (offsets, *early, *late, *kept)])
    steps = ((CH * SR, SC), (CH * CR, CC), (2 * CH, HID), (HID, HID), (OUT, HID))
    fine_step, coarse_step, in_step, mid_step, out_step = pl.pallas_call(
        adam_kernel,
        out_shape=[jax.ShapeDtypeStruct(shape, F32) for shape in steps],
        in_specs=[whole] * len(found),
        out_specs=[far] * len(steps),
        scratch_shapes=[pltpu.VMEM(shape, F32) for shape in steps[2:]]
        + [pltpu.SemaphoreType.DMA((6,))],
        compiler_params=pltpu.CompilerParams(vmem_limit_bytes=8 * 1024 * 1024),
        name="adam",
    )(*found)
    return (
        fine_step.reshape(grid_fine.shape),
        coarse_step.reshape(grid_coarse.shape),
        in_step.T,
        mid_step[None],
        out_step,
    )


def solution(mesh):
    tile, copied = P(None, "row", "col"), P()
    placed = (P("row", "col", None), P(None, None, "row", "col"), tile, tile)
    placed += (copied,) * 3 + (tile,) * 4 + (copied,) * 6
    return jax.shard_map(
        shards,
        mesh=mesh,
        in_specs=placed,
        out_specs=(tile, tile, copied, copied, copied),
        check_vma=False,
    )
```

```python
import functools

import jax
import jax.numpy as jnp
from jax import lax
from jax.experimental import pallas as pl
from jax.experimental.pallas import tpu as pltpu
from jax.sharding import PartitionSpec as P

SUB = 4
RATIO = 4
ADAM_STEP = 10
BETA_ONE = 0.9
BETA_TWO = 0.99
ADAM_EPSILON = 1e-08
CLIP_RMS = 0.01
LOSS_VALUE = 0.25
MEAN_EPSILON = 1e-06

MESH = pl.DeviceIdType.MESH
LANES = 128
SUBLANES = 8
F32 = jnp.float32
BF16 = jnp.bfloat16


def clip_factor(total, entries):
    return jnp.minimum(1.0, CLIP_RMS / jnp.sqrt(total / entries + MEAN_EPSILON))


def adam_step(gradient, moment_one, moment_two, clip_scale):
    rise_one = 1.0 / (1.0 - BETA_ONE**ADAM_STEP)
    rise_two = 1.0 / (1.0 - BETA_TWO**ADAM_STEP)
    new_one = (BETA_ONE * rise_one) * moment_one + gradient * (
        clip_scale * ((1.0 - BETA_ONE) * rise_one)
    )
    root = gradient * (clip_scale * ((1.0 - BETA_TWO) * rise_two) ** 0.5)
    new_two = (BETA_TWO * rise_two) * moment_two + root * root
    return new_one / (new_two * lax.rsqrt(new_two) + ADAM_EPSILON)


def dot(former, latter, dims=((1,), (0,)), precision=None):
    return lax.dot_general(
        former, latter, (dims, ((), ())), preferred_element_type=F32, precision=precision
    )


def dot_t(former, latter, precision=None):
    return dot(former, latter, ((1,), (1,)), precision)


def silu_of_half(half):
    return half + half * jnp.tanh(half)


def slope_of_half(half):
    bend = jnp.tanh(half)
    return (1.0 + bend) * ((1.0 + half) - half * bend)


class Axis:
    def __init__(self, me, size, device):
        self.me, self.size, self.device = me, size, device

    def peer(self, step):
        return lax.rem(self.me + step, self.size)


def aligned(start):
    return pl.multiple_of(start, SUBLANES)


class Links:
    def __init__(self, send, recv):
        self.send, self.recv, self.sends, self.recvs = send, recv, 0, 0

    def take(self):
        self.recvs += 1
        return self.recvs - 1

    def take_send(self):
        self.sends += 1
        return self.sends - 1

    def copy(self, source, target, device, slot, send):
        return pltpu.make_async_remote_copy(
            src_ref=source,
            dst_ref=target,
            send_sem=self.send.at[send],
            recv_sem=self.recv.at[slot],
            device_id=device,
            device_id_type=MESH,
        )

    def wait(self, sent, landed, device, slot, send):
        self.copy(sent, sent, device, slot, send).wait_send()
        self.copy(landed, landed, device, slot, send).wait_recv()


class Scatter:
    def __init__(self, links, own, start, rows, axes, lands):
        self.links, self.own, self.axes, self.lands = links, own, axes, lands
        self.spans = [(start, rows)]
        for axis in axes:
            start, rows = self.spans[-1]
            part = rows // axis.size
            self.spans.append((start + axis.me * part, part))
        self.slots = [links.take() for axis in axes]
        self.send = links.take_send()

    def start(self, stage):
        axis, start, part = self.axes[stage], self.spans[stage][0], self.spans[stage + 1][1]
        for step in range(1, axis.size):
            peer = axis.peer(step)
            self.links.copy(
                self.own.at[pl.ds(aligned(start + peer * part), part)],
                self.lands[stage].at[step - 1],
                axis.device(peer),
                self.slots[stage],
                self.send,
            ).start()

    def finish(self, stage):
        axis, land = self.axes[stage], self.lands[stage]
        start, part = self.spans[stage + 1]
        if axis.size > 1:
            sent = self.own.at[pl.ds(0, (axis.size - 1) * part)]
            device = axis.device(axis.peer(1))
            self.links.wait(sent, land, device, self.slots[stage], self.send)
        span = pl.ds(aligned(start), part)
        found = self.own[span]
        for step in range(axis.size - 1):
            found = found + land[step]
        self.own[span] = found


class Gather:
    def __init__(self, scatter, full):
        self.scatter, self.full = scatter, full
        self.axes, self.spans = scatter.axes, scatter.spans
        self.slots = [scatter.links.take() for axis in scatter.axes]

    def flatten(self, axis):
        self.axes, self.spans = [axis], [None, self.scatter.spans[-1]]
        return self

    def place(self):
        start, rows = self.scatter.spans[-1]
        span = pl.ds(aligned(start), rows)
        self.full[span] = self.scatter.own[span]

    def start(self, stage):
        axis = self.axes[stage]
        start, rows = self.spans[stage + 1]
        block = self.full.at[pl.ds(aligned(start), rows)]
        for step in range(1, axis.size):
            device = axis.device(axis.peer(step))
            self.scatter.links.copy(
                block, block, device, self.slots[stage], self.scatter.send
            ).start()

    def finish(self, stage):
        axis, rows = self.axes[stage], self.spans[stage + 1][1]
        if axis.size > 1:
            span = self.full.at[pl.ds(0, (axis.size - 1) * rows)]
            device = axis.device(axis.peer(1))
            self.scatter.links.wait(span, span, device, self.slots[stage], self.scatter.send)


class Total:
    def __init__(self, links, mine, lands, axes):
        self.links, self.mine, self.lands, self.axes = links, mine, lands, axes
        self.slots = [links.take() for axis in axes]
        self.send = links.take_send()
        self.stage = 0

    def start(self):
        axis, land, slot = self.axes[self.stage], self.lands[self.stage], self.slots[self.stage]
        land[axis.me] = self.mine[...]

        @pl.loop(1, axis.size)
        def _(step):
            device = axis.device(axis.peer(step))
            self.links.copy(self.mine, land.at[axis.me], device, slot, self.send).start()

    def finish(self):
        axis, land, slot = self.axes[self.stage], self.lands[self.stage], self.slots[self.stage]
        if axis.size > 1:
            span = land.at[pl.ds(0, axis.size - 1)]
            self.links.wait(span, span, axis.device(axis.peer(1)), slot, self.send)
        total = land[0]
        for place in range(1, axis.size):
            total = total + land[place]
        self.stage += 1
        if self.stage < len(self.axes):
            self.mine[...] = total
            self.start()
        return total


def step_kernel(dims, *refs):
    refs = iter(refs)
    take = lambda count: [next(refs) for _ in range(count)]
    (offsets_hbm,) = take(1)
    early_hbm = take(6)
    late_hbm = take(4)
    kept_hbm = take(6)
    fine_out, coarse_out, mid_full, in_full, out_full = take(5)
    kept = take(6)
    (offsets_ref,) = take(1)
    targets, fine, coarse, w_in, w_mid, w_out = early = take(6)
    late = take(4)
    (
        up_buf,
        cp_buf,
        below_buf,
        right_cp,
        diag_cp,
        coarse_s,
        across,
        across_c,
        b_in,
        b_in_t,
        b_mid,
        b_mid_t,
        b_out,
        b_out_t,
        feats,
        act_0,
        act_1,
        half_0,
        half_1,
        delta_1,
        pred,
        edge_send,
        edge_recv,
        col_send,
        col_recv,
        cot_s,
        fgrad,
        down_buf,
        q_buf,
        above_buf,
        left_q,
        diag_q,
        fine_g,
        coarse_g,
        grad_in,
        grad_out,
        mid_away,
        mid_own,
        mid_pair,
        in_away,
        in_own,
        in_pair,
        total_mine,
    ) = take(43)
    out_lands = take(4)
    total_lands = take(2)
    lands = take(2 * dims["PARTS"] + 2)
    load_sem, send_sem, recv_sem, know_sem = take(4)

    rows_n, cols_n = lax.axis_size("row"), lax.axis_size("col")
    row, col = lax.axis_index("row"), lax.axis_index("col")
    CH, SR, SC, CR, CC, HID, OUT = (dims[k] for k in ("CH", "SR", "SC", "CR", "CC", "HID", "OUT"))
    S = SR * SC
    CHUNK = dims["GROUP"] * SC
    CHUNKS = S // CHUNK
    GROUP = dims["GROUP"]

    core, plane = lax.rem(col, 2), lax.div(col, 2)
    x_at, z_at = lax.rem(row, 2), lax.div(row, 2)
    axis_core = Axis(core, 2, lambda p: (row, plane * 2 + p))
    axis_x = Axis(x_at, 2, lambda p: (z_at * 2 + p, col))
    axis_y = Axis(plane, cols_n // 2, lambda p: (row, p * 2 + core))
    axis_z = Axis(z_at, rows_n // 2, lambda p: (p * 2 + x_at, col))
    axes = (axis_core, axis_x, axis_y, axis_z)
    planes = cols_n // 2
    axis_plane = Axis(
        x_at * planes + plane,
        2 * planes,
        lambda p: (z_at * 2 + lax.div(p, planes), lax.rem(p, planes) * 2 + core),
    )
    axis_chips = Axis(
        row * planes + plane,
        rows_n * planes,
        lambda p: (lax.div(p, planes), lax.rem(p, planes) * 2 + core),
    )

    has_up, has_down = row > 0, row < rows_n - 1
    has_left, has_right = col > 0, col < cols_n - 1
    near = {
        "up": (has_up, (row - 1, col)),
        "down": (has_down, (row + 1, col)),
        "left": (has_left, (row, col - 1)),
        "right": (has_right, (row, col + 1)),
        "up_left": (jnp.logical_and(has_up, has_left), (row - 1, col - 1)),
        "down_right": (jnp.logical_and(has_down, has_right), (row + 1, col + 1)),
    }
    links = Links(send_sem, recv_sem)

    loads = [
        pltpu.make_async_copy(source, target, load_sem.at[place])
        for place, (source, target) in enumerate(
            zip(
                early_hbm + late_hbm + kept_hbm + [offsets_hbm],
                early + late + kept + [offsets_ref],
            )
        )
    ]
    loads_early, loads_late, load_offsets = loads[:6], loads[6:-1], loads[-1]
    load_offsets.start()
    for place in (1, 2, 3, 4, 5, 0):
        loads_early[place].start()
    barrier = pltpu.get_barrier_semaphore()
    z_near = ((z_at > 0, (row - 2, col)), (z_at < axis_z.size - 1, (row + 2, col)))
    expected = sum(axis.size - 1 for axis in axes[:3])
    for axis in axes[:3]:
        for step in range(1, axis.size):
            pl.semaphore_signal(
                barrier, inc=1, device_id=axis.device(axis.peer(step)), device_id_type=MESH
            )
    for there, device in list(near.values()) + list(z_near):
        expected = expected + there.astype(jnp.int32)

        @pl.when(there)
        def _():
            pl.semaphore_signal(barrier, inc=1, device_id=device, device_id_type=MESH)

    for load in loads_late:
        load.start()

    lane = lax.broadcasted_iota(jnp.int32, (CH, LANES), 1)
    lane_8 = lax.broadcasted_iota(jnp.int32, (SUBLANES, LANES), 1)
    load_offsets.wait()
    off_y = offsets_ref[0, 0, 0].astype(F32) / SUB
    off_x = offsets_ref[0, 0, 1].astype(F32) / SUB

    def fine_row(r):
        return fine[pl.ds(r, CH, stride=SR), :]

    def roll(value, shift):
        return pltpu.roll(value, shift % LANES, 1)

    coarse_s[...] = jnp.zeros(coarse_s.shape, F32)
    loads_early[1].wait()
    loads_early[2].wait()
    for r in range(CR):
        coarse_s[r, :, :CC] = coarse[pl.ds(r, CH, stride=CR), :]
    up_buf[:CH] = fine_row(0)
    group = CH * CC // LANES
    side = [slice(k * group, (k + 1) * group) for k in range(LANES // CC)]

    def pack(value):
        return sum(roll(value[side[k]], k * CC) for k in range(LANES // CC))

    def unpack(value, target):
        kept = lax.broadcasted_iota(jnp.int32, (group, LANES), 1) < CC
        for k in range(LANES // CC):
            target[side[k]] = jnp.where(kept, roll(value, -k * CC), 0.0)

    up_buf[CH:] = pack(coarse_s[0])
    packed = jnp.zeros((CH, LANES), F32)
    for r in range(SR):
        packed = jnp.where(lane == r, roll(fine_row(r), r), packed)
    for r in range(CR):
        packed = jnp.where(lane == SR + r, roll(coarse_s[r], SR + r), packed)
    cp_buf[...] = packed

    pl.semaphore_wait(barrier, expected)

    halo_sends = [links.take_send() for _ in range(6)]
    halos_used = [0]

    def halo(source, target, towards, back):
        slot, send = links.take(), halo_sends[halos_used[0] % 6]
        halos_used[0] += 1
        copy = links.copy(source, target, near[towards][1], slot, send)
        arriving = links.copy(source, target, near[back][1], slot, send)

        @pl.when(near[towards][0])
        def _():
            copy.start()

        def finish():
            @pl.when(near[towards][0])
            def _():
                copy.wait_send()

            @pl.when(near[back][0])
            def _():
                arriving.wait_recv()

        return finish

    waits = [
        halo(up_buf, below_buf, "up", "down"),
        halo(cp_buf, right_cp, "left", "right"),
        halo(cp_buf, diag_cp, "up_left", "down_right"),
    ]
    for target, back in ((below_buf, "down"), (right_cp, "right"), (diag_cp, "down_right")):

        @pl.when(jnp.logical_not(near[back][0]))
        def _():
            target[...] = jnp.zeros(target.shape, F32)

    loads_early[3].wait()
    loads_early[4].wait()
    loads_early[5].wait()
    b_in_t[...] = w_in[...].astype(BF16)
    b_in[...] = (0.5 * w_in[...]).T.astype(BF16)
    halved = 0.5 * w_mid[...]
    b_mid[...] = halved.astype(BF16)
    b_mid_t[...] = halved.T.astype(BF16)
    padded_out = jnp.concatenate([w_out[...], jnp.zeros((SUBLANES - OUT, HID), F32)], axis=0)
    b_out[...] = padded_out.astype(BF16)
    b_out_t[...] = (0.5 * padded_out).T.astype(BF16)
    cot_s[...] = jnp.zeros(cot_s.shape, BF16)
    vertex = lax.broadcasted_iota(jnp.int32, (LANES, LANES), 0)
    sample = lax.broadcasted_iota(jnp.int32, (LANES, LANES), 1)
    base = lax.div(sample, RATIO)
    fraction = (lax.rem(sample, RATIO).astype(F32) + off_x) / RATIO
    table = jnp.where(vertex == base, 1.0 - fraction, 0.0) + jnp.where(
        vertex == base + 1, fraction, 0.0
    )
    for wait in waits:
        wait()

    for r in range(SR + 1):
        value = fine_row(r) if r < SR else below_buf[:CH]
        edge = roll(right_cp[...], LANES - 1 - r) if r < SR else roll(diag_cp[...], LANES - 1)
        shifted = jnp.where(lane == LANES - 1, edge, roll(value, LANES - 1))
        across[r] = (1.0 - off_x) * value + off_x * shifted
    unpack(below_buf[CH:], coarse_s.at[CR])
    for r in range(CR + 1):
        value = coarse_s[r]
        edge = roll(right_cp[...], CC - SR - r) if r < CR else roll(diag_cp[...], CC - SR)
        coarse_s[r] = jnp.where(lane == CC, edge, value)
    across_c[...] = dot(
        coarse_s[...].reshape((CR + 1) * CH, LANES), table, precision=lax.Precision.HIGHEST
    ).reshape(CR + 1, CH, LANES)

    def chunk_span(c):
        return slice(c * CHUNK, (c + 1) * CHUNK)

    def tell(place, targets):
        for there, device in targets:

            @pl.when(there)
            def _():
                pl.semaphore_signal(
                    know_sem.at[place], inc=1, device_id=device, device_id_type=MESH
                )

    def hear(place, targets):
        pl.semaphore_wait(know_sem.at[place], sum(there.astype(jnp.int32) for there, _ in targets))

    def peers_of(axis):
        always = row >= 0
        return [(always, axis.device(axis.peer(step))) for step in range(1, axis.size)]

    words = [z_near] * max(axis_z.size - 2, 0) + [peers_of(axis_x), peers_of(axis_y)]
    words = [targets for targets in words if targets]
    heard = [0]

    def pass_word(count):
        for _ in range(count):
            if heard[0] < len(words):
                hear(heard[0], words[heard[0]])
                heard[0] += 1
                if heard[0] < len(words):
                    tell(heard[0], words[heard[0]])

    def forward(c):
        for k in range(GROUP):
            i = c * GROUP + k
            j = c * (GROUP // RATIO) + k // RATIO
            span = slice(i * SC, (i + 1) * SC)
            part = (k % RATIO + off_y) / RATIO
            feats[:CH, span] = ((1.0 - off_y) * across[i] + off_y * across[i + 1]).astype(BF16)
            feats[CH:, span] = ((1.0 - part) * across_c[j] + part * across_c[j + 1]).astype(BF16)
        span = chunk_span(c)
        half_0[:, span] = dot(b_in[...], feats[:, span])
        act_0[:, span] = silu_of_half(half_0[:, span]).astype(BF16)
        half_1[:, span] = dot(b_mid[...], act_0[:, span])
        act_1[:, span] = silu_of_half(half_1[:, span]).astype(BF16)
        colours = dot(b_out[...], act_1[:, span])
        for k in range(GROUP):
            pred[c * GROUP + k + 1] = colours[:, k * SC : (k + 1) * SC]

    order = [0, CHUNKS - 1] + list(range(1, CHUNKS - 1))

    def target_row(kind, r):
        found = targets[pl.ds(kind * OUT * SR + r, OUT, stride=SR), :]
        return jnp.concatenate([found, jnp.zeros((SUBLANES - OUT, LANES), F32)], axis=0)

    def send_columns(batch, groups):
        first_col = last_col = last_aim = jnp.zeros((SUBLANES, LANES), F32)
        for c in groups:
            for r in range(c * GROUP, (c + 1) * GROUP):
                first_col = jnp.where(lane_8 == r, roll(pred[r + 1], r), first_col)
                last_col = jnp.where(lane_8 == r, roll(pred[r + 1], r + 1), last_col)
                last_aim = jnp.where(lane_8 == r, roll(target_row(2, r), r + 1), last_aim)
        col_send[batch, 0] = first_col
        col_send[batch, 1] = last_col
        col_send[batch, 2] = last_aim
        return [
            halo(col_send.at[batch, 0], col_recv.at[batch, 0], "left", "right"),
            halo(col_send.at[batch, pl.ds(1, 2)], col_recv.at[batch, pl.ds(1, 2)], "right", "left"),
        ]

    tell(0, words[0])
    for place in range(CHUNKS - 1):
        forward(order[place])
        pass_word(-(-len(words) // CHUNKS))
    loads_early[0].wait()
    edge_send[0, 0] = pred[1]
    edge_send[1, 0] = pred[SR]
    edge_send[1, 1] = target_row(1, SR - 1)
    halos_used[0] = 0
    early_waits = [
        halo(edge_send.at[0, 0], edge_recv.at[0, 0], "up", "down"),
        halo(edge_send.at[1], edge_recv.at[1], "down", "up"),
    ]
    early_waits += send_columns(0, order[:-1])
    for place, back in enumerate(("down", "up")):

        @pl.when(jnp.logical_not(near[back][0]))
        def _():
            edge_recv[place] = jnp.zeros(edge_recv.shape[1:], F32)

    forward(order[-1])
    pass_word(len(words))
    last_waits = send_columns(1, order[-1:])
    for place, back in ((0, "right"), (1, "left"), (2, "left")):

        @pl.when(jnp.logical_not(near[back][0]))
        def _():
            for batch in range(2):
                col_recv[batch, place] = jnp.zeros(col_recv.shape[2:], F32)

    ready = order[:2]
    for c in ready:
        half_1[:, chunk_span(c)] = slope_of_half(half_1[:, chunk_span(c)])
    for wait in early_waits:
        wait()
    pred[SR + 1] = edge_recv[0, 0]
    above_error = jnp.where(has_up, (pred[1] - edge_recv[1, 0]) - edge_recv[1, 1], 0.0)

    def row_error(r):
        if r < 0:
            return above_error
        error = (pred[r + 2] - pred[r + 1]) - target_row(1, r)
        return jnp.where(has_down, error, 0.0) if r == SR - 1 else error

    def cotangent(c, batch):
        prior = row_error(c * GROUP - 1)
        for r in range(c * GROUP, (c + 1) * GROUP):
            here = pred[r + 1]
            error = row_error(r)
            edge = roll(col_recv[batch, 0], LANES - 1 - r)
            beside = jnp.where(lane_8 == LANES - 1, edge, roll(here, -1))
            col_error = (beside - here) - target_row(2, r)
            closed = jnp.logical_and(lane_8 == LANES - 1, jnp.logical_not(has_right))
            col_error = jnp.where(closed, 0.0, col_error)
            before = (here - roll(col_recv[batch, 1], -r)) - roll(col_recv[batch, 2], -r)
            before = jnp.where(has_left, before, 0.0)
            col_prior = jnp.where(lane_8 == 0, before, roll(col_error, 1))
            value_error = here - target_row(0, r)
            cot = (
                2.0 * LOSS_VALUE * value_error
                + 2.0 * (prior - error)
                + 2.0 * (col_prior - col_error)
            )
            kept = lax.broadcasted_iota(jnp.int32, (SUBLANES, LANES), 0) < OUT
            cot_s[:, r * SC : (r + 1) * SC] = jnp.where(kept, cot, 0.0).astype(BF16)
            prior = error

    def upper(c):
        span = chunk_span(c)
        slope = half_1[:, span] if c in ready else slope_of_half(half_1[:, span])
        delta_1[:, span] = (dot(b_out_t[...], cot_s[:, span]) * slope).astype(BF16)

    for c in order[:-1]:
        cotangent(c, 0)
    for c in order[:-1]:
        upper(c)
    for wait in last_waits:
        wait()
    cotangent(order[-1], 1)
    upper(order[-1])

    half = HID // 2
    mid_rows = HID * half // LANES
    parts = dims["PARTS"]
    part_rows = mid_rows // parts
    ahead, behind = tuple(range(-(-parts // 2))), tuple(range(-(-parts // 2), parts))
    mids = [
        Scatter(links, mid_own, k * part_rows, part_rows, (axis_plane, axis_z), lands[k * 2 : k * 2 + 2])
        for k in range(parts)
    ]
    mids.append(
        Scatter(links, in_own, 0, in_own.shape[0], (axis_plane, axis_z), lands[2 * parts :])
    )

    def mid_half(which, target):
        upper = delta_1[pl.ds(pl.multiple_of(which * half, half), half), :]
        block = dot_t(upper, act_0[...])
        for part in range(HID // LANES):
            target[part * half : (part + 1) * half, :] = block[:, part * LANES : (part + 1) * LANES]

    partner = axis_core.device(1 - core)
    part_span = lambda k: pl.ds(k * part_rows, part_rows)
    pairs = [
        links.copy(
            mid_away.at[part_span(k)],
            mid_pair.at[part_span(k)],
            partner,
            links.take(),
            mids[k].send,
        )
        for k in range(parts)
    ]
    mid_half(1 - core, mid_away)
    for pair in pairs:
        pair.start()
    mid_half(core, mid_own)
    for k in range(parts):
        pairs[k].wait()
        mid_own[part_span(k)] += mid_pair[part_span(k)]
        mids[k].start(0)

    grad_out[...] = dot_t(cot_s[...], act_1[...])[:OUT]
    outs = Total(links, grad_out, out_lands, axes)
    outs.start()
    grad_in[...] = jnp.zeros(grad_in.shape, F32)

    def lower(c):
        span = chunk_span(c)
        slope = slope_of_half(half_0[:, span])
        delta = (dot(b_mid_t[...], delta_1[:, span]) * slope).astype(BF16)
        grad_in[...] += dot_t(feats[:, span], delta)
        spread = dot(b_in_t[...], delta)
        for k in range(GROUP):
            fgrad[c * GROUP + k] = spread[:, k * SC : (k + 1) * SC]

    def advance(which, stage):
        for k in which:
            mids[k].finish(stage)
            if stage + 1 < len(mids[k].axes):
                mids[k].start(stage + 1)

    half_chunks = CHUNKS // 2
    for c in range(half_chunks):
        lower(c)
    for c in range(half_chunks, CHUNKS - 1):
        lower(c)
    outs.finish()
    advance(ahead, 0)
    lower(CHUNKS - 1)

    blocks = HID // LANES
    inputs = 2 * CH
    in_rows = inputs * blocks // 2

    def in_half(which, target):
        for choice in range(2):

            @pl.when(which == choice)
            def _():
                for part in range(blocks // 2):
                    at = (choice * (blocks // 2) + part) * LANES
                    target[part * inputs : (part + 1) * inputs, :] = grad_in[:, at : at + LANES]
        if target.shape[0] > in_rows:
            target[in_rows:, :] = jnp.zeros((target.shape[0] - in_rows, LANES), F32)

    in_half(1 - core, in_away)
    pair_in = links.copy(in_away, in_pair, partner, links.take(), mids[parts].send)
    pair_in.start()
    in_half(core, in_own)

    last = SR
    bottom = None
    packed = jnp.zeros((CH, LANES), F32)
    zero = jnp.zeros((CH, LANES), F32)
    for r in range(SR + 1):
        value = zero
        if r < SR:
            value = (1.0 - off_y) * fgrad[r, :CH]
        if r > 0:
            value = value + off_y * fgrad[r - 1, :CH]
        moved = off_x * roll(value, 1)
        out = (1.0 - off_x) * value + jnp.where(lane == 0, 0.0, moved)
        at = r if r < SR else SR + CR
        packed = jnp.where(lane == at, roll(moved, at), packed)
        if r < SR:
            fine_g[r] = out
        else:
            down_buf[:CH] = out
    outs.finish()
    advance(behind, 0)
    pair_in.wait()
    in_own[...] += in_pair[...]
    mids[parts].start(0)
    for j in range(CR + 1):
        value = zero
        for k in range(RATIO):
            part = (k + off_y) / RATIO
            if j < CR:
                value = value + (1.0 - part) * fgrad[j * RATIO + k, CH:]
            if j > 0:
                value = value + part * fgrad[(j - 1) * RATIO + k, CH:]
        coarse_s[j] = value
    spread = dot_t(
        coarse_s[...].reshape((CR + 1) * CH, LANES), table, precision=lax.Precision.HIGHEST
    ).reshape(CR + 1, CH, LANES)
    for j in range(CR + 1):
        value = spread[j]
        at = SR + j if j < CR else SR + CR + 1
        packed = jnp.where(lane == at, roll(value, at - CC), packed)
        value = jnp.where(lane < CC, value, 0.0)
        if j < CR:
            coarse_g[j] = value
        else:
            down_buf[CH:] = pack(value)
    q_buf[...] = packed
    halos_used[0] = 0
    waits = [
        halo(down_buf, above_buf, "down", "up"),
        halo(q_buf, left_q, "right", "left"),
        halo(q_buf, diag_q, "down_right", "up_left"),
    ]
    for target, back in ((above_buf, "up"), (left_q, "left"), (diag_q, "up_left")):

        @pl.when(jnp.logical_not(near[back][0]))
        def _():
            target[...] = jnp.zeros(target.shape, F32)

    gathers = [Gather(scatter, mid_full.at[core]) for scatter in mids[:parts]]
    gathers.append(Gather(mids[parts], in_full.at[core]).flatten(axis_chips))

    def settle(which):
        for k in which:
            last_stage = len(mids[k].axes) - 1
            mids[k].finish(last_stage)
            gathers[k].place()
            gathers[k].start(len(gathers[k].axes) - 1)

    def regain(which, stage):
        for k in which:
            gathers[k].finish(stage)
            if stage > 0:
                gathers[k].start(stage - 1)

    settle(ahead)
    for wait in waits:
        wait()
    fine_g[0] += above_buf[:CH] + jnp.where(lane == 0, roll(diag_q[...], -(SR + CR)), 0.0)
    unpack(above_buf[CH:], coarse_s.at[0])
    coarse_g[0] += coarse_s[0] + jnp.where(lane == 0, roll(diag_q[...], -(SR + CR + 1)), 0.0)
    squares = jnp.zeros((CH, LANES), F32)
    for r in range(SR):
        value = fine_g[r] + jnp.where(lane == 0, roll(left_q[...], -r), 0.0)
        fine_g[r] = value
        squares += value * value
    for j in range(CR):
        value = coarse_g[j] + jnp.where(lane == 0, roll(left_q[...], -(SR + j)), 0.0)
        coarse_g[j] = value
        squares += value * value
    total = squares[:SUBLANES]
    for part in range(1, CH // SUBLANES):
        total = total + squares[part * SUBLANES : (part + 1) * SUBLANES]
    total_mine[...] = jnp.sum(total, axis=0, keepdims=True)
    totals = Total(links, total_mine, total_lands, (axis_core, axis_chips))
    totals.start()
    outs.finish()
    settle(behind)
    advance((parts,), 0)
    totals.finish()
    regain(ahead, 1)
    regain(behind, 1)
    settle((parts,))
    out_full[...] = outs.finish()
    grid_total = totals.finish()

    for load in loads_late:
        load.wait()
    fine_first, fine_second, coarse_first, coarse_second = late
    entries = CH * (SR * SC + CR * CC) * rows_n * cols_n
    grid_scale = clip_factor(jnp.sum(grid_total, keepdims=True), entries)
    for r in range(SR):
        span = pl.ds(r, CH, stride=SR)
        fine_out[span, :] = adam_step(fine_g[r], fine_first[span, :], fine_second[span, :], grid_scale)
    for j in range(CR):
        span = pl.ds(j, CH, stride=CR)
        coarse_out[span, :] = adam_step(
            coarse_g[j, :, :CC], coarse_first[span, :], coarse_second[span, :], grid_scale
        )
    def across_pair(k):
        block = mid_full.at[core, part_span(k)]
        copy = links.copy(block, block, partner, links.take(), mids[k].send)
        copy.start()
        return copy

    lasts = []
    for k in ahead:
        gathers[k].finish(0)
        lasts.append(across_pair(k))
    for k in behind:
        gathers[k].finish(0)
        lasts.append(across_pair(k))
    gathers[parts].finish(0)
    block = in_full.at[core]
    last_in = links.copy(block, block, partner, links.take(), mids[parts].send)
    last_in.start()
    lasts.append(last_in)
    for copy in lasts:
        copy.wait()
    assert (links.sends, links.recvs) == (dims["SENDS"], dims["RECVS"])


def adam_kernel(
    fine_step,
    coarse_step,
    mid_full,
    in_full,
    out_full,
    in_first,
    in_second,
    mid_first,
    mid_second,
    out_first,
    out_second,
    fine_out,
    coarse_out,
    in_out,
    mid_out,
    out_out,
    in_step,
    mid_step,
    out_step,
    sems,
):
    writes = []

    def write(source, target):
        copy = pltpu.make_async_copy(source, target, sems.at[len(writes)])
        copy.start()
        writes.append(copy)

    write(fine_step, fine_out)
    write(coarse_step, coarse_out)
    inputs, hidden = in_step.shape
    outputs = out_step.shape[0]
    half, blocks = hidden // 2, hidden // LANES
    parts = [mid_full[which, :, :] for which in range(2)]
    parts += [in_full[which, : inputs * blocks // 2, :] for which in range(2)]
    squares = jnp.zeros((SUBLANES, LANES), F32)
    for value in parts:
        value = (value * value).reshape(-1, SUBLANES, LANES)
        squares += jnp.sum(value, axis=0)
    total = jnp.sum(squares, keepdims=True) + jnp.sum(out_full[...] * out_full[...], keepdims=True)
    scale = clip_factor(total, hidden * (hidden + inputs + outputs))
    for which in range(2):
        span = slice(which * half, (which + 1) * half)
        for part in range(blocks):
            lanes = slice(part * LANES, (part + 1) * LANES)
            mid_step[span, lanes] = adam_step(
                mid_full[which, part * half : (part + 1) * half, :],
                mid_first[span, lanes],
                mid_second[span, lanes],
                scale,
            )
        write(mid_step.at[pl.ds(which * half, half)], mid_out.at[pl.ds(which * half, half)])
    out_step[...] = adam_step(out_full[...], out_first[...], out_second[...], scale)
    write(out_step, out_out)
    for which in range(2):
        for part in range(blocks // 2):
            at = (which * (blocks // 2) + part) * LANES
            lanes = slice(at, at + LANES)
            in_step[:, lanes] = adam_step(
                in_full[which, part * inputs : (part + 1) * inputs, :],
                in_first[:, lanes],
                in_second[:, lanes],
                scale,
            )
    write(in_step, in_out)
    for copy in writes:
        copy.wait()


def shards(
    offsets,
    targets,
    grid_fine,
    grid_coarse,
    weight_in,
    weight_mid,
    weight_out,
    fine_first,
    fine_second,
    coarse_first,
    coarse_second,
    in_first,
    in_second,
    mid_first,
    mid_second,
    out_first,
    out_second,
):
    CH, SR, SC = grid_fine.shape
    CR, CC = grid_coarse.shape[1:]
    HID = weight_in.shape[0]
    OUT = weight_out.shape[0]
    S = SR * SC
    rows_n, cols_n = lax.axis_size("row"), lax.axis_size("col")
    sizes_x, sizes_y, sizes_z = 2, cols_n // 2, rows_n // 2
    parts = max(1, min(4, HID * HID // 2 // LANES // (sizes_x * sizes_y * sizes_z * SUBLANES)))
    sends, recvs = 6 + parts + 1 + 2, 12 + 6 + 2 * (parts + 1) + 2 * (2 * parts + 2)
    chips = sizes_x * sizes_y * sizes_z
    in_rows = CH * HID // LANES
    in_rows = -(-in_rows // (chips * SUBLANES)) * chips * SUBLANES
    mid_rows = HID * HID // 2 // LANES
    dims = dict(CH=CH, SR=SR, SC=SC, CR=CR, CC=CC, HID=HID, OUT=OUT, PARTS=parts, SENDS=sends, RECVS=recvs, GROUP=8)

    flat = lambda grid: grid.reshape(-1, grid.shape[-1])
    early = (
        flat(targets),
        flat(grid_fine),
        flat(grid_coarse),
        weight_in.T,
        weight_mid[0],
        weight_out,
    )
    late = (flat(fine_first), flat(fine_second), flat(coarse_first), flat(coarse_second))
    vmem = lambda *shape: pltpu.VMEM(shape, F32)
    low = lambda *shape: pltpu.VMEM(shape, BF16)

    def landing(rows, sizes):
        found = []
        for size in sizes:
            rows = rows // size
            found.append(vmem(max(size - 1, 1), rows, LANES))
        return found

    kept = (in_first.T, in_second.T, mid_first[0], mid_second[0], out_first, out_second)
    edge = CH + CH * CC // LANES
    scratch = [pltpu.SMEM(offsets.shape, jnp.int32)]
    scratch += [pltpu.VMEM(a.shape, F32) for a in early + late]
    scratch += [
        vmem(edge, LANES),
        vmem(CH, LANES),
        vmem(edge, LANES),
        vmem(CH, LANES),
        vmem(CH, LANES),
        vmem(CR + 1, CH, LANES),
        vmem(SR + 1, CH, LANES),
        vmem(CR + 1, CH, LANES),
        low(HID, 2 * CH),
        low(2 * CH, HID),
        low(HID, HID),
        low(HID, HID),
        low(SUBLANES, HID),
        low(HID, SUBLANES),
        low(2 * CH, S),
        low(HID, S),
        low(HID, S),
        vmem(HID, S),
        vmem(HID, S),
        low(HID, S),
        vmem(SR + 2, SUBLANES, LANES),
        vmem(2, 2, SUBLANES, LANES),
        vmem(2, 2, SUBLANES, LANES),
        vmem(2, 3, SUBLANES, LANES),
        vmem(2, 3, SUBLANES, LANES),
        low(SUBLANES, S),
        vmem(SR, 2 * CH, LANES),
        vmem(edge, LANES),
        vmem(CH, LANES),
        vmem(edge, LANES),
        vmem(CH, LANES),
        vmem(CH, LANES),
        vmem(SR, CH, LANES),
        vmem(CR, CH, LANES),
        vmem(2 * CH, HID),
        vmem(OUT, HID),
        vmem(mid_rows, LANES),
        vmem(mid_rows, LANES),
        vmem(mid_rows, LANES),
        vmem(in_rows, LANES),
        vmem(in_rows, LANES),
        vmem(in_rows, LANES),
        vmem(1, LANES),
    ]
    scratch += [vmem(size, OUT, HID) for size in (2, sizes_x, sizes_y, sizes_z)]
    scratch += [vmem(size, 1, LANES) for size in (2, chips)]
    for part in range(parts):
        scratch += landing(mid_rows // parts, (sizes_x * sizes_y, sizes_z))
    scratch += landing(in_rows, (sizes_x * sizes_y, sizes_z))
    scratch += [
        pltpu.SemaphoreType.DMA((len(early) + len(late) + len(kept) + 1,)),
        pltpu.SemaphoreType.DMA((sends,)),
        pltpu.SemaphoreType.DMA((recvs,)),
        pltpu.SemaphoreType.REGULAR((max(sizes_z - 2, 0) + 2,)),
    ]
    outs = (
        (CH * SR, SC),
        (CH * CR, CC),
        (2, mid_rows, LANES),
        (2, in_rows, LANES),
        (OUT, HID),
    ) + tuple(a.shape for a in kept)
    far = pl.BlockSpec(memory_space=pltpu.HBM)
    whole = pl.BlockSpec(memory_space=pltpu.VMEM)
    found = pl.pallas_call(
        functools.partial(step_kernel, dims),
        out_shape=[jax.ShapeDtypeStruct(shape, F32) for shape in outs],
        in_specs=[far] * (1 + len(early) + len(late) + len(kept)),
        out_specs=[whole] * len(outs),
        scratch_shapes=scratch,
        compiler_params=pltpu.CompilerParams(
            collective_id=0, has_side_effects=True, vmem_limit_bytes=48 * 1024 * 1024
        ),
        name="field",
    )(*[pltpu.with_memory_space_constraint(a, pltpu.HBM) for a in (offsets, *early, *late, *kept)])
    steps = ((CH * SR, SC), (CH * CR, CC), (2 * CH, HID), (HID, HID), (OUT, HID))
    fine_step, coarse_step, in_step, mid_step, out_step = pl.pallas_call(
        adam_kernel,
        out_shape=[jax.ShapeDtypeStruct(shape, F32) for shape in steps],
        in_specs=[whole] * len(found),
        out_specs=[far] * len(steps),
        scratch_shapes=[pltpu.VMEM(shape, F32) for shape in steps[2:]]
        + [pltpu.SemaphoreType.DMA((6,))],
        compiler_params=pltpu.CompilerParams(vmem_limit_bytes=8 * 1024 * 1024),
        name="adam",
    )(*found)
    return (
        fine_step.reshape(grid_fine.shape),
        coarse_step.reshape(grid_coarse.shape),
        in_step.T,
        mid_step[None],
        out_step,
    )


def solution(mesh):
    tile, copied = P(None, "row", "col"), P()
    placed = (P("row", "col", None), P(None, None, "row", "col"), tile, tile)
    placed += (copied,) * 3 + (tile,) * 4 + (copied,) * 6
    return jax.shard_map(
        shards,
        mesh=mesh,
        in_specs=placed,
        out_specs=(tile, tile, copied, copied, copied),
        check_vma=False,
    )
```

```python
import functools

import jax
import jax.numpy as jnp
from jax import lax
from jax.experimental import pallas as pl
from jax.experimental.pallas import tpu as pltpu
from jax.sharding import PartitionSpec as P

SUB = 4
RATIO = 4
ADAM_STEP = 10
BETA_ONE = 0.9
BETA_TWO = 0.99
ADAM_EPSILON = 1e-08
CLIP_RMS = 0.01
LOSS_VALUE = 0.25
MEAN_EPSILON = 1e-06

MESH = pl.DeviceIdType.MESH
LANES = 128
SUBLANES = 8
F32 = jnp.float32
BF16 = jnp.bfloat16


def clip_factor(total, entries):
    return jnp.minimum(1.0, CLIP_RMS / jnp.sqrt(total / entries + MEAN_EPSILON))


def adam_step(gradient, moment_one, moment_two, clip_scale):
    rise_one = 1.0 / (1.0 - BETA_ONE**ADAM_STEP)
    rise_two = 1.0 / (1.0 - BETA_TWO**ADAM_STEP)
    new_one = (BETA_ONE * rise_one) * moment_one + gradient * (
        clip_scale * ((1.0 - BETA_ONE) * rise_one)
    )
    root = gradient * (clip_scale * ((1.0 - BETA_TWO) * rise_two) ** 0.5)
    new_two = (BETA_TWO * rise_two) * moment_two + root * root
    return new_one / (new_two * lax.rsqrt(new_two) + ADAM_EPSILON)


def dot(former, latter, dims=((1,), (0,)), precision=None):
    return lax.dot_general(
        former, latter, (dims, ((), ())), preferred_element_type=F32, precision=precision
    )


def dot_t(former, latter, precision=None):
    return dot(former, latter, ((1,), (1,)), precision)


def silu_of_half(half):
    return half + half * jnp.tanh(half)


def slope_of_half(half):
    bend = jnp.tanh(half)
    return (1.0 + bend) * ((1.0 + half) - half * bend)


class Axis:
    def __init__(self, me, size, device):
        self.me, self.size, self.device = me, size, device

    def peer(self, step):
        return lax.rem(self.me + step, self.size)


def aligned(start):
    return pl.multiple_of(start, SUBLANES)


class Links:
    def __init__(self, send, recv):
        self.send, self.recv, self.sends, self.recvs = send, recv, 0, 0

    def take(self):
        self.recvs += 1
        return self.recvs - 1

    def take_send(self):
        self.sends += 1
        return self.sends - 1

    def copy(self, source, target, device, slot, send):
        return pltpu.make_async_remote_copy(
            src_ref=source,
            dst_ref=target,
            send_sem=self.send.at[send],
            recv_sem=self.recv.at[slot],
            device_id=device,
            device_id_type=MESH,
        )

    def wait(self, sent, landed, device, slot, send):
        self.copy(sent, sent, device, slot, send).wait_send()
        self.copy(landed, landed, device, slot, send).wait_recv()


class Scatter:
    def __init__(self, links, own, start, rows, axes, lands):
        self.links, self.own, self.axes, self.lands = links, own, axes, lands
        self.spans = [(start, rows)]
        for axis in axes:
            start, rows = self.spans[-1]
            part = rows // axis.size
            self.spans.append((start + axis.me * part, part))
        self.slots = [links.take() for axis in axes]
        self.send = links.take_send()

    def start(self, stage):
        axis, start, part = self.axes[stage], self.spans[stage][0], self.spans[stage + 1][1]
        for step in range(1, axis.size):
            peer = axis.peer(step)
            self.links.copy(
                self.own.at[pl.ds(aligned(start + peer * part), part)],
                self.lands[stage].at[step - 1],
                axis.device(peer),
                self.slots[stage],
                self.send,
            ).start()

    def finish(self, stage):
        axis, land = self.axes[stage], self.lands[stage]
        start, part = self.spans[stage + 1]
        if axis.size > 1:
            sent = self.own.at[pl.ds(0, (axis.size - 1) * part)]
            device = axis.device(axis.peer(1))
            self.links.wait(sent, land, device, self.slots[stage], self.send)
        span = pl.ds(aligned(start), part)
        found = self.own[span]
        for step in range(axis.size - 1):
            found = found + land[step]
        self.own[span] = found


class Gather:
    def __init__(self, scatter, full):
        self.scatter, self.full = scatter, full
        self.axes, self.spans = scatter.axes, scatter.spans
        self.slots = [scatter.links.take() for axis in scatter.axes]

    def flatten(self, axis):
        self.axes, self.spans = [axis], [None, self.scatter.spans[-1]]
        return self

    def place(self):
        start, rows = self.scatter.spans[-1]
        span = pl.ds(aligned(start), rows)
        self.full[span] = self.scatter.own[span]

    def start(self, stage):
        axis = self.axes[stage]
        start, rows = self.spans[stage + 1]
        block = self.full.at[pl.ds(aligned(start), rows)]
        for step in range(1, axis.size):
            device = axis.device(axis.peer(step))
            self.scatter.links.copy(
                block, block, device, self.slots[stage], self.scatter.send
            ).start()

    def finish(self, stage):
        axis, rows = self.axes[stage], self.spans[stage + 1][1]
        if axis.size > 1:
            span = self.full.at[pl.ds(0, (axis.size - 1) * rows)]
            device = axis.device(axis.peer(1))
            self.scatter.links.wait(span, span, device, self.slots[stage], self.scatter.send)


class Total:
    def __init__(self, links, mine, lands, axes):
        self.links, self.mine, self.lands, self.axes = links, mine, lands, axes
        self.slots = [links.take() for axis in axes]
        self.send = links.take_send()
        self.stage = 0

    def start(self):
        axis, land, slot = self.axes[self.stage], self.lands[self.stage], self.slots[self.stage]
        land[axis.me] = self.mine[...]

        @pl.loop(1, axis.size)
        def _(step):
            device = axis.device(axis.peer(step))
            self.links.copy(self.mine, land.at[axis.me], device, slot, self.send).start()

    def finish(self):
        axis, land, slot = self.axes[self.stage], self.lands[self.stage], self.slots[self.stage]
        if axis.size > 1:
            span = land.at[pl.ds(0, axis.size - 1)]
            self.links.wait(span, span, axis.device(axis.peer(1)), slot, self.send)
        total = land[0]
        for place in range(1, axis.size):
            total = total + land[place]
        self.stage += 1
        if self.stage < len(self.axes):
            self.mine[...] = total
            self.start()
        return total


def step_kernel(dims, *refs):
    refs = iter(refs)
    take = lambda count: [next(refs) for _ in range(count)]
    (offsets_hbm,) = take(1)
    early_hbm = take(6)
    late_hbm = take(4)
    kept_hbm = take(6)
    fine_out, coarse_out, mid_full, in_full, out_full = take(5)
    kept = take(6)
    (offsets_ref,) = take(1)
    targets, fine, coarse, w_in, w_mid, w_out = early = take(6)
    late = take(4)
    (
        up_buf,
        cp_buf,
        below_buf,
        right_cp,
        diag_cp,
        coarse_s,
        across,
        across_c,
        b_in,
        b_in_t,
        b_mid,
        b_mid_t,
        b_out,
        b_out_t,
        feats,
        act_0,
        act_1,
        half_0,
        half_1,
        delta_1,
        pred,
        edge_send,
        edge_recv,
        col_send,
        col_recv,
        cot_s,
        fgrad,
        down_buf,
        q_buf,
        above_buf,
        left_q,
        diag_q,
        fine_g,
        coarse_g,
        grad_in,
        grad_out,
        mid_away,
        mid_own,
        mid_pair,
        in_away,
        in_own,
        in_pair,
        total_mine,
    ) = take(43)
    out_lands = take(4)
    total_lands = take(2)
    lands = take(2 * dims["PARTS"] + 2)
    load_sem, send_sem, recv_sem, know_sem = take(4)

    rows_n, cols_n = lax.axis_size("row"), lax.axis_size("col")
    row, col = lax.axis_index("row"), lax.axis_index("col")
    CH, SR, SC, CR, CC, HID, OUT = (dims[k] for k in ("CH", "SR", "SC", "CR", "CC", "HID", "OUT"))
    S = SR * SC
    CHUNK = dims["GROUP"] * SC
    CHUNKS = S // CHUNK
    GROUP = dims["GROUP"]

    core, plane = lax.rem(col, 2), lax.div(col, 2)
    x_at, z_at = lax.rem(row, 2), lax.div(row, 2)
    axis_core = Axis(core, 2, lambda p: (row, plane * 2 + p))
    axis_x = Axis(x_at, 2, lambda p: (z_at * 2 + p, col))
    axis_y = Axis(plane, cols_n // 2, lambda p: (row, p * 2 + core))
    axis_z = Axis(z_at, rows_n // 2, lambda p: (p * 2 + x_at, col))
    axes = (axis_core, axis_x, axis_y, axis_z)
    planes = cols_n // 2
    axis_plane = Axis(
        x_at * planes + plane,
        2 * planes,
        lambda p: (z_at * 2 + lax.div(p, planes), lax.rem(p, planes) * 2 + core),
    )
    axis_chips = Axis(
        row * planes + plane,
        rows_n * planes,
        lambda p: (lax.div(p, planes), lax.rem(p, planes) * 2 + core),
    )

    has_up, has_down = row > 0, row < rows_n - 1
    has_left, has_right = col > 0, col < cols_n - 1
    near = {
        "up": (has_up, (row - 1, col)),
        "down": (has_down, (row + 1, col)),
        "left": (has_left, (row, col - 1)),
        "right": (has_right, (row, col + 1)),
        "up_left": (jnp.logical_and(has_up, has_left), (row - 1, col - 1)),
        "down_right": (jnp.logical_and(has_down, has_right), (row + 1, col + 1)),
    }
    links = Links(send_sem, recv_sem)

    loads = [
        pltpu.make_async_copy(source, target, load_sem.at[place])
        for place, (source, target) in enumerate(
            zip(
                early_hbm + late_hbm + kept_hbm + [offsets_hbm],
                early + late + kept + [offsets_ref],
            )
        )
    ]
    loads_early, loads_late, load_offsets = loads[:6], loads[6:-1], loads[-1]
    load_offsets.start()
    for place in (1, 2, 3, 4, 5, 0):
        loads_early[place].start()
    barrier = pltpu.get_barrier_semaphore()
    z_near = ((z_at > 0, (row - 2, col)), (z_at < axis_z.size - 1, (row + 2, col)))
    expected = sum(axis.size - 1 for axis in axes[:3])
    for axis in axes[:3]:
        for step in range(1, axis.size):
            pl.semaphore_signal(
                barrier, inc=1, device_id=axis.device(axis.peer(step)), device_id_type=MESH
            )
    for there, device in list(near.values()) + list(z_near):
        expected = expected + there.astype(jnp.int32)

        @pl.when(there)
        def _():
            pl.semaphore_signal(barrier, inc=1, device_id=device, device_id_type=MESH)

    for load in loads_late:
        load.start()

    lane = lax.broadcasted_iota(jnp.int32, (CH, LANES), 1)
    lane_8 = lax.broadcasted_iota(jnp.int32, (SUBLANES, LANES), 1)
    load_offsets.wait()
    off_y = offsets_ref[0, 0, 0].astype(F32) / SUB
    off_x = offsets_ref[0, 0, 1].astype(F32) / SUB

    def fine_row(r):
        return fine[pl.ds(r, CH, stride=SR), :]

    def roll(value, shift):
        return pltpu.roll(value, shift % LANES, 1)

    coarse_s[...] = jnp.zeros(coarse_s.shape, F32)
    loads_early[1].wait()
    loads_early[2].wait()
    for r in range(CR):
        coarse_s[r, :, :CC] = coarse[pl.ds(r, CH, stride=CR), :]
    up_buf[:CH] = fine_row(0)
    group = CH * CC // LANES
    side = [slice(k * group, (k + 1) * group) for k in range(LANES // CC)]

    def pack(value):
        return sum(roll(value[side[k]], k * CC) for k in range(LANES // CC))

    def unpack(value, target):
        kept = lax.broadcasted_iota(jnp.int32, (group, LANES), 1) < CC
        for k in range(LANES // CC):
            target[side[k]] = jnp.where(kept, roll(value, -k * CC), 0.0)

    up_buf[CH:] = pack(coarse_s[0])
    packed = jnp.zeros((CH, LANES), F32)
    for r in range(SR):
        packed = jnp.where(lane == r, roll(fine_row(r), r), packed)
    for r in range(CR):
        packed = jnp.where(lane == SR + r, roll(coarse_s[r], SR + r), packed)
    cp_buf[...] = packed

    pl.semaphore_wait(barrier, expected)

    halo_sends = [links.take_send() for _ in range(6)]
    halos_used = [0]

    def halo(source, target, towards, back):
        slot, send = links.take(), halo_sends[halos_used[0] % 6]
        halos_used[0] += 1
        copy = links.copy(source, target, near[towards][1], slot, send)
        arriving = links.copy(source, target, near[back][1], slot, send)

        @pl.when(near[towards][0])
        def _():
            copy.start()

        def finish():
            @pl.when(near[towards][0])
            def _():
                copy.wait_send()

            @pl.when(near[back][0])
            def _():
                arriving.wait_recv()

        return finish

    waits = [
        halo(up_buf, below_buf, "up", "down"),
        halo(cp_buf, right_cp, "left", "right"),
        halo(cp_buf, diag_cp, "up_left", "down_right"),
    ]
    for target, back in ((below_buf, "down"), (right_cp, "right"), (diag_cp, "down_right")):

        @pl.when(jnp.logical_not(near[back][0]))
        def _():
            target[...] = jnp.zeros(target.shape, F32)

    loads_early[3].wait()
    loads_early[4].wait()
    loads_early[5].wait()
    b_in_t[...] = w_in[...].astype(BF16)
    b_in[...] = (0.5 * w_in[...]).T.astype(BF16)
    halved = 0.5 * w_mid[...]
    b_mid[...] = halved.astype(BF16)
    b_mid_t[...] = halved.T.astype(BF16)
    padded_out = jnp.concatenate([w_out[...], jnp.zeros((SUBLANES - OUT, HID), F32)], axis=0)
    b_out[...] = padded_out.astype(BF16)
    b_out_t[...] = (0.5 * padded_out).T.astype(BF16)
    cot_s[...] = jnp.zeros(cot_s.shape, BF16)
    vertex = lax.broadcasted_iota(jnp.int32, (LANES, LANES), 0)
    sample = lax.broadcasted_iota(jnp.int32, (LANES, LANES), 1)
    base = lax.div(sample, RATIO)
    fraction = (lax.rem(sample, RATIO).astype(F32) + off_x) / RATIO
    table = jnp.where(vertex == base, 1.0 - fraction, 0.0) + jnp.where(
        vertex == base + 1, fraction, 0.0
    )
    for wait in waits:
        wait()

    for r in range(SR + 1):
        value = fine_row(r) if r < SR else below_buf[:CH]
        edge = roll(right_cp[...], LANES - 1 - r) if r < SR else roll(diag_cp[...], LANES - 1)
        shifted = jnp.where(lane == LANES - 1, edge, roll(value, LANES - 1))
        across[r] = (1.0 - off_x) * value + off_x * shifted
    unpack(below_buf[CH:], coarse_s.at[CR])
    for r in range(CR + 1):
        value = coarse_s[r]
        edge = roll(right_cp[...], CC - SR - r) if r < CR else roll(diag_cp[...], CC - SR)
        coarse_s[r] = jnp.where(lane == CC, edge, value)
    across_c[...] = dot(
        coarse_s[...].reshape((CR + 1) * CH, LANES), table, precision=lax.Precision.HIGHEST
    ).reshape(CR + 1, CH, LANES)

    def chunk_span(c):
        return slice(c * CHUNK, (c + 1) * CHUNK)

    def tell(place, targets):
        for there, device in targets:

            @pl.when(there)
            def _():
                pl.semaphore_signal(
                    know_sem.at[place], inc=1, device_id=device, device_id_type=MESH
                )

    def hear(place, targets):
        pl.semaphore_wait(know_sem.at[place], sum(there.astype(jnp.int32) for there, _ in targets))

    def peers_of(axis):
        always = row >= 0
        return [(always, axis.device(axis.peer(step))) for step in range(1, axis.size)]

    words = [z_near] * max(axis_z.size - 2, 0) + [peers_of(axis_x), peers_of(axis_y)]
    words = [targets for targets in words if targets]
    heard = [0]

    def pass_word(count):
        for _ in range(count):
            if heard[0] < len(words):
                hear(heard[0], words[heard[0]])
                heard[0] += 1
                if heard[0] < len(words):
                    tell(heard[0], words[heard[0]])

    def forward(c):
        for k in range(GROUP):
            i = c * GROUP + k
            j = c * (GROUP // RATIO) + k // RATIO
            span = slice(i * SC, (i + 1) * SC)
            part = (k % RATIO + off_y) / RATIO
            feats[:CH, span] = ((1.0 - off_y) * across[i] + off_y * across[i + 1]).astype(BF16)
            feats[CH:, span] = ((1.0 - part) * across_c[j] + part * across_c[j + 1]).astype(BF16)
        span = chunk_span(c)
        half_0[:, span] = dot(b_in[...], feats[:, span])
        act_0[:, span] = silu_of_half(half_0[:, span]).astype(BF16)
        half_1[:, span] = dot(b_mid[...], act_0[:, span])
        act_1[:, span] = silu_of_half(half_1[:, span]).astype(BF16)
        colours = dot(b_out[...], act_1[:, span])
        for k in range(GROUP):
            pred[c * GROUP + k + 1] = colours[:, k * SC : (k + 1) * SC]

    order = [0, CHUNKS - 1] + list(range(1, CHUNKS - 1))

    def target_row(kind, r):
        found = targets[pl.ds(kind * OUT * SR + r, OUT, stride=SR), :]
        return jnp.concatenate([found, jnp.zeros((SUBLANES - OUT, LANES), F32)], axis=0)

    def send_columns(batch, groups):
        first_col = last_col = last_aim = jnp.zeros((SUBLANES, LANES), F32)
        for c in groups:
            for r in range(c * GROUP, (c + 1) * GROUP):
                first_col = jnp.where(lane_8 == r, roll(pred[r + 1], r), first_col)
                last_col = jnp.where(lane_8 == r, roll(pred[r + 1], r + 1), last_col)
                last_aim = jnp.where(lane_8 == r, roll(target_row(2, r), r + 1), last_aim)
        col_send[batch, 0] = first_col
        col_send[batch, 1] = last_col
        col_send[batch, 2] = last_aim
        return [
            halo(col_send.at[batch, 0], col_recv.at[batch, 0], "left", "right"),
            halo(col_send.at[batch, pl.ds(1, 2)], col_recv.at[batch, pl.ds(1, 2)], "right", "left"),
        ]

    tell(0, words[0])
    for place in range(CHUNKS - 1):
        forward(order[place])
        pass_word(-(-len(words) // CHUNKS))
    loads_early[0].wait()
    edge_send[0, 0] = pred[1]
    edge_send[1, 0] = pred[SR]
    edge_send[1, 1] = target_row(1, SR - 1)
    halos_used[0] = 0
    early_waits = [
        halo(edge_send.at[0, 0], edge_recv.at[0, 0], "up", "down"),
        halo(edge_send.at[1], edge_recv.at[1], "down", "up"),
    ]
    early_waits += send_columns(0, order[:-1])
    for place, back in enumerate(("down", "up")):

        @pl.when(jnp.logical_not(near[back][0]))
        def _():
            edge_recv[place] = jnp.zeros(edge_recv.shape[1:], F32)

    forward(order[-1])
    pass_word(len(words))
    last_waits = send_columns(1, order[-1:])
    for place, back in ((0, "right"), (1, "left"), (2, "left")):

        @pl.when(jnp.logical_not(near[back][0]))
        def _():
            for batch in range(2):
                col_recv[batch, place] = jnp.zeros(col_recv.shape[2:], F32)

    ready = order[:2]
    for c in ready:
        half_1[:, chunk_span(c)] = slope_of_half(half_1[:, chunk_span(c)])
    for wait in early_waits:
        wait()
    pred[SR + 1] = edge_recv[0, 0]
    above_error = jnp.where(has_up, (pred[1] - edge_recv[1, 0]) - edge_recv[1, 1], 0.0)

    def row_error(r):
        if r < 0:
            return above_error
        error = (pred[r + 2] - pred[r + 1]) - target_row(1, r)
        return jnp.where(has_down, error, 0.0) if r == SR - 1 else error

    def cotangent(c, batch):
        prior = row_error(c * GROUP - 1)
        for r in range(c * GROUP, (c + 1) * GROUP):
            here = pred[r + 1]
            error = row_error(r)
            edge = roll(col_recv[batch, 0], LANES - 1 - r)
            beside = jnp.where(lane_8 == LANES - 1, edge, roll(here, -1))
            col_error = (beside - here) - target_row(2, r)
            closed = jnp.logical_and(lane_8 == LANES - 1, jnp.logical_not(has_right))
            col_error = jnp.where(closed, 0.0, col_error)
            before = (here - roll(col_recv[batch, 1], -r)) - roll(col_recv[batch, 2], -r)
            before = jnp.where(has_left, before, 0.0)
            col_prior = jnp.where(lane_8 == 0, before, roll(col_error, 1))
            value_error = here - target_row(0, r)
            cot = (
                2.0 * LOSS_VALUE * value_error
                + 2.0 * (prior - error)
                + 2.0 * (col_prior - col_error)
            )
            kept = lax.broadcasted_iota(jnp.int32, (SUBLANES, LANES), 0) < OUT
            cot_s[:, r * SC : (r + 1) * SC] = jnp.where(kept, cot, 0.0).astype(BF16)
            prior = error

    def upper(c):
        span = chunk_span(c)
        slope = half_1[:, span] if c in ready else slope_of_half(half_1[:, span])
        delta_1[:, span] = (dot(b_out_t[...], cot_s[:, span]) * slope).astype(BF16)

    for c in order[:-1]:
        cotangent(c, 0)
    for c in order[:-1]:
        upper(c)
    for wait in last_waits:
        wait()
    cotangent(order[-1], 1)
    upper(order[-1])

    half = HID // 2
    mid_rows = HID * half // LANES
    parts = dims["PARTS"]
    part_rows = mid_rows // parts
    ahead, behind = tuple(range(-(-parts // 2))), tuple(range(-(-parts // 2), parts))
    mids = [
        Scatter(links, mid_own, k * part_rows, part_rows, (axis_plane, axis_z), lands[k * 2 : k * 2 + 2])
        for k in range(parts)
    ]
    mids.append(
        Scatter(links, in_own, 0, in_own.shape[0], (axis_plane, axis_z), lands[2 * parts :])
    )

    def mid_half(which, target):
        upper = delta_1[pl.ds(pl.multiple_of(which * half, half), half), :]
        block = dot_t(upper, act_0[...])
        for part in range(HID // LANES):
            target[part * half : (part + 1) * half, :] = block[:, part * LANES : (part + 1) * LANES]

    partner = axis_core.device(1 - core)
    part_span = lambda k: pl.ds(k * part_rows, part_rows)
    pairs = [
        links.copy(
            mid_away.at[part_span(k)],
            mid_pair.at[part_span(k)],
            partner,
            links.take(),
            mids[k].send,
        )
        for k in range(parts)
    ]
    mid_half(1 - core, mid_away)
    for pair in pairs:
        pair.start()
    mid_half(core, mid_own)
    for k in range(parts):
        pairs[k].wait()
        mid_own[part_span(k)] += mid_pair[part_span(k)]
        mids[k].start(0)

    grad_out[...] = dot_t(cot_s[...], act_1[...])[:OUT]
    outs = Total(links, grad_out, out_lands, axes)
    outs.start()
    grad_in[...] = jnp.zeros(grad_in.shape, F32)

    def lower(c):
        span = chunk_span(c)
        slope = slope_of_half(half_0[:, span])
        delta = (dot(b_mid_t[...], delta_1[:, span]) * slope).astype(BF16)
        grad_in[...] += dot_t(feats[:, span], delta)
        spread = dot(b_in_t[...], delta)
        for k in range(GROUP):
            fgrad[c * GROUP + k] = spread[:, k * SC : (k + 1) * SC]

    def advance(which, stage):
        for k in which:
            mids[k].finish(stage)
            if stage + 1 < len(mids[k].axes):
                mids[k].start(stage + 1)

    half_chunks = CHUNKS // 2
    for c in range(half_chunks):
        lower(c)
    for c in range(half_chunks, CHUNKS - 1):
        lower(c)
    outs.finish()
    advance(ahead, 0)
    lower(CHUNKS - 1)

    blocks = HID // LANES
    inputs = 2 * CH
    in_rows = inputs * blocks // 2

    def in_half(which, target):
        for choice in range(2):

            @pl.when(which == choice)
            def _():
                for part in range(blocks // 2):
                    at = (choice * (blocks // 2) + part) * LANES
                    target[part * inputs : (part + 1) * inputs, :] = grad_in[:, at : at + LANES]
        if target.shape[0] > in_rows:
            target[in_rows:, :] = jnp.zeros((target.shape[0] - in_rows, LANES), F32)

    in_half(1 - core, in_away)
    pair_in = links.copy(in_away, in_pair, partner, links.take(), mids[parts].send)
    pair_in.start()
    in_half(core, in_own)

    last = SR
    bottom = None
    packed = jnp.zeros((CH, LANES), F32)
    zero = jnp.zeros((CH, LANES), F32)
    for r in range(SR + 1):
        if r == SR // 2:
            outs.finish()
            advance(behind, 0)
        value = zero
        if r < SR:
            value = (1.0 - off_y) * fgrad[r, :CH]
        if r > 0:
            value = value + off_y * fgrad[r - 1, :CH]
        moved = off_x * roll(value, 1)
        out = (1.0 - off_x) * value + jnp.where(lane == 0, 0.0, moved)
        at = r if r < SR else SR + CR
        packed = jnp.where(lane == at, roll(moved, at), packed)
        if r < SR:
            fine_g[r] = out
        else:
            down_buf[:CH] = out
    pair_in.wait()
    in_own[...] += in_pair[...]
    mids[parts].start(0)
    for j in range(CR + 1):
        value = zero
        for k in range(RATIO):
            part = (k + off_y) / RATIO
            if j < CR:
                value = value + (1.0 - part) * fgrad[j * RATIO + k, CH:]
            if j > 0:
                value = value + part * fgrad[(j - 1) * RATIO + k, CH:]
        coarse_s[j] = value
    spread = dot_t(
        coarse_s[...].reshape((CR + 1) * CH, LANES), table, precision=lax.Precision.HIGHEST
    ).reshape(CR + 1, CH, LANES)
    for j in range(CR + 1):
        value = spread[j]
        at = SR + j if j < CR else SR + CR + 1
        packed = jnp.where(lane == at, roll(value, at - CC), packed)
        value = jnp.where(lane < CC, value, 0.0)
        if j < CR:
            coarse_g[j] = value
        else:
            down_buf[CH:] = pack(value)
    q_buf[...] = packed
    halos_used[0] = 0
    waits = [
        halo(down_buf, above_buf, "down", "up"),
        halo(q_buf, left_q, "right", "left"),
        halo(q_buf, diag_q, "down_right", "up_left"),
    ]
    for target, back in ((above_buf, "up"), (left_q, "left"), (diag_q, "up_left")):

        @pl.when(jnp.logical_not(near[back][0]))
        def _():
            target[...] = jnp.zeros(target.shape, F32)

    gathers = [Gather(scatter, mid_full.at[core]) for scatter in mids[:parts]]
    gathers.append(Gather(mids[parts], in_full.at[core]).flatten(axis_chips))

    def settle(which):
        for k in which:
            last_stage = len(mids[k].axes) - 1
            mids[k].finish(last_stage)
            gathers[k].place()
            gathers[k].start(len(gathers[k].axes) - 1)

    def regain(which, stage):
        for k in which:
            gathers[k].finish(stage)
            if stage > 0:
                gathers[k].start(stage - 1)

    settle(ahead)
    settle(behind)
    for wait in waits:
        wait()
    fine_g[0] += above_buf[:CH] + jnp.where(lane == 0, roll(diag_q[...], -(SR + CR)), 0.0)
    unpack(above_buf[CH:], coarse_s.at[0])
    coarse_g[0] += coarse_s[0] + jnp.where(lane == 0, roll(diag_q[...], -(SR + CR + 1)), 0.0)
    squares = jnp.zeros((CH, LANES), F32)
    for r in range(SR):
        value = fine_g[r] + jnp.where(lane == 0, roll(left_q[...], -r), 0.0)
        fine_g[r] = value
        squares += value * value
    for j in range(CR):
        value = coarse_g[j] + jnp.where(lane == 0, roll(left_q[...], -(SR + j)), 0.0)
        coarse_g[j] = value
        squares += value * value
    total = squares[:SUBLANES]
    for part in range(1, CH // SUBLANES):
        total = total + squares[part * SUBLANES : (part + 1) * SUBLANES]
    total_mine[...] = jnp.sum(total, axis=0, keepdims=True)
    totals = Total(links, total_mine, total_lands, (axis_core, axis_chips))
    totals.start()
    outs.finish()
    advance((parts,), 0)
    totals.finish()
    regain(ahead, 1)
    regain(behind, 1)
    settle((parts,))
    out_full[...] = outs.finish()
    grid_total = totals.finish()

    for load in loads_late:
        load.wait()
    fine_first, fine_second, coarse_first, coarse_second = late
    entries = CH * (SR * SC + CR * CC) * rows_n * cols_n
    grid_scale = clip_factor(jnp.sum(grid_total, keepdims=True), entries)
    for r in range(SR):
        span = pl.ds(r, CH, stride=SR)
        fine_out[span, :] = adam_step(fine_g[r], fine_first[span, :], fine_second[span, :], grid_scale)
    for j in range(CR):
        span = pl.ds(j, CH, stride=CR)
        coarse_out[span, :] = adam_step(
            coarse_g[j, :, :CC], coarse_first[span, :], coarse_second[span, :], grid_scale
        )
    def across_pair(k):
        block = mid_full.at[core, part_span(k)]
        copy = links.copy(block, block, partner, links.take(), mids[k].send)
        copy.start()
        return copy

    lasts = []
    for k in ahead:
        gathers[k].finish(0)
        lasts.append(across_pair(k))
    for k in behind:
        gathers[k].finish(0)
        lasts.append(across_pair(k))
    gathers[parts].finish(0)
    block = in_full.at[core]
    last_in = links.copy(block, block, partner, links.take(), mids[parts].send)
    last_in.start()
    lasts.append(last_in)
    for copy in lasts:
        copy.wait()
    assert (links.sends, links.recvs) == (dims["SENDS"], dims["RECVS"])


def adam_kernel(
    fine_step,
    coarse_step,
    mid_full,
    in_full,
    out_full,
    in_first,
    in_second,
    mid_first,
    mid_second,
    out_first,
    out_second,
    fine_out,
    coarse_out,
    in_out,
    mid_out,
    out_out,
    in_step,
    mid_step,
    out_step,
    sems,
):
    writes = []

    def write(source, target):
        copy = pltpu.make_async_copy(source, target, sems.at[len(writes)])
        copy.start()
        writes.append(copy)

    write(fine_step, fine_out)
    write(coarse_step, coarse_out)
    inputs, hidden = in_step.shape
    outputs = out_step.shape[0]
    half, blocks = hidden // 2, hidden // LANES
    parts = [mid_full[which, :, :] for which in range(2)]
    parts += [in_full[which, : inputs * blocks // 2, :] for which in range(2)]
    squares = jnp.zeros((SUBLANES, LANES), F32)
    for value in parts:
        value = (value * value).reshape(-1, SUBLANES, LANES)
        squares += jnp.sum(value, axis=0)
    total = jnp.sum(squares, keepdims=True) + jnp.sum(out_full[...] * out_full[...], keepdims=True)
    scale = clip_factor(total, hidden * (hidden + inputs + outputs))
    for which in range(2):
        span = slice(which * half, (which + 1) * half)
        for part in range(blocks):
            lanes = slice(part * LANES, (part + 1) * LANES)
            mid_step[span, lanes] = adam_step(
                mid_full[which, part * half : (part + 1) * half, :],
                mid_first[span, lanes],
                mid_second[span, lanes],
                scale,
            )
        write(mid_step.at[pl.ds(which * half, half)], mid_out.at[pl.ds(which * half, half)])
    out_step[...] = adam_step(out_full[...], out_first[...], out_second[...], scale)
    write(out_step, out_out)
    for which in range(2):
        for part in range(blocks // 2):
            at = (which * (blocks // 2) + part) * LANES
            lanes = slice(at, at + LANES)
            in_step[:, lanes] = adam_step(
                in_full[which, part * inputs : (part + 1) * inputs, :],
                in_first[:, lanes],
                in_second[:, lanes],
                scale,
            )
    write(in_step, in_out)
    for copy in writes:
        copy.wait()


def shards(
    offsets,
    targets,
    grid_fine,
    grid_coarse,
    weight_in,
    weight_mid,
    weight_out,
    fine_first,
    fine_second,
    coarse_first,
    coarse_second,
    in_first,
    in_second,
    mid_first,
    mid_second,
    out_first,
    out_second,
):
    CH, SR, SC = grid_fine.shape
    CR, CC = grid_coarse.shape[1:]
    HID = weight_in.shape[0]
    OUT = weight_out.shape[0]
    S = SR * SC
    rows_n, cols_n = lax.axis_size("row"), lax.axis_size("col")
    sizes_x, sizes_y, sizes_z = 2, cols_n // 2, rows_n // 2
    parts = max(1, min(4, HID * HID // 2 // LANES // (sizes_x * sizes_y * sizes_z * SUBLANES)))
    sends, recvs = 6 + parts + 1 + 2, 12 + 6 + 2 * (parts + 1) + 2 * (2 * parts + 2)
    chips = sizes_x * sizes_y * sizes_z
    in_rows = CH * HID // LANES
    in_rows = -(-in_rows // (chips * SUBLANES)) * chips * SUBLANES
    mid_rows = HID * HID // 2 // LANES
    dims = dict(CH=CH, SR=SR, SC=SC, CR=CR, CC=CC, HID=HID, OUT=OUT, PARTS=parts, SENDS=sends, RECVS=recvs, GROUP=8)

    flat = lambda grid: grid.reshape(-1, grid.shape[-1])
    early = (
        flat(targets),
        flat(grid_fine),
        flat(grid_coarse),
        weight_in.T,
        weight_mid[0],
        weight_out,
    )
    late = (flat(fine_first), flat(fine_second), flat(coarse_first), flat(coarse_second))
    vmem = lambda *shape: pltpu.VMEM(shape, F32)
    low = lambda *shape: pltpu.VMEM(shape, BF16)

    def landing(rows, sizes):
        found = []
        for size in sizes:
            rows = rows // size
            found.append(vmem(max(size - 1, 1), rows, LANES))
        return found

    kept = (in_first.T, in_second.T, mid_first[0], mid_second[0], out_first, out_second)
    edge = CH + CH * CC // LANES
    scratch = [pltpu.SMEM(offsets.shape, jnp.int32)]
    scratch += [pltpu.VMEM(a.shape, F32) for a in early + late]
    scratch += [
        vmem(edge, LANES),
        vmem(CH, LANES),
        vmem(edge, LANES),
        vmem(CH, LANES),
        vmem(CH, LANES),
        vmem(CR + 1, CH, LANES),
        vmem(SR + 1, CH, LANES),
        vmem(CR + 1, CH, LANES),
        low(HID, 2 * CH),
        low(2 * CH, HID),
        low(HID, HID),
        low(HID, HID),
        low(SUBLANES, HID),
        low(HID, SUBLANES),
        low(2 * CH, S),
        low(HID, S),
        low(HID, S),
        vmem(HID, S),
        vmem(HID, S),
        low(HID, S),
        vmem(SR + 2, SUBLANES, LANES),
        vmem(2, 2, SUBLANES, LANES),
        vmem(2, 2, SUBLANES, LANES),
        vmem(2, 3, SUBLANES, LANES),
        vmem(2, 3, SUBLANES, LANES),
        low(SUBLANES, S),
        vmem(SR, 2 * CH, LANES),
        vmem(edge, LANES),
        vmem(CH, LANES),
        vmem(edge, LANES),
        vmem(CH, LANES),
        vmem(CH, LANES),
        vmem(SR, CH, LANES),
        vmem(CR, CH, LANES),
        vmem(2 * CH, HID),
        vmem(OUT, HID),
        vmem(mid_rows, LANES),
        vmem(mid_rows, LANES),
        vmem(mid_rows, LANES),
        vmem(in_rows, LANES),
        vmem(in_rows, LANES),
        vmem(in_rows, LANES),
        vmem(1, LANES),
    ]
    scratch += [vmem(size, OUT, HID) for size in (2, sizes_x, sizes_y, sizes_z)]
    scratch += [vmem(size, 1, LANES) for size in (2, chips)]
    for part in range(parts):
        scratch += landing(mid_rows // parts, (sizes_x * sizes_y, sizes_z))
    scratch += landing(in_rows, (sizes_x * sizes_y, sizes_z))
    scratch += [
        pltpu.SemaphoreType.DMA((len(early) + len(late) + len(kept) + 1,)),
        pltpu.SemaphoreType.DMA((sends,)),
        pltpu.SemaphoreType.DMA((recvs,)),
        pltpu.SemaphoreType.REGULAR((max(sizes_z - 2, 0) + 2,)),
    ]
    outs = (
        (CH * SR, SC),
        (CH * CR, CC),
        (2, mid_rows, LANES),
        (2, in_rows, LANES),
        (OUT, HID),
    ) + tuple(a.shape for a in kept)
    far = pl.BlockSpec(memory_space=pltpu.HBM)
    whole = pl.BlockSpec(memory_space=pltpu.VMEM)
    found = pl.pallas_call(
        functools.partial(step_kernel, dims),
        out_shape=[jax.ShapeDtypeStruct(shape, F32) for shape in outs],
        in_specs=[far] * (1 + len(early) + len(late) + len(kept)),
        out_specs=[whole] * len(outs),
        scratch_shapes=scratch,
        compiler_params=pltpu.CompilerParams(
            collective_id=0, has_side_effects=True, vmem_limit_bytes=48 * 1024 * 1024
        ),
        name="field",
    )(*[pltpu.with_memory_space_constraint(a, pltpu.HBM) for a in (offsets, *early, *late, *kept)])
    steps = ((CH * SR, SC), (CH * CR, CC), (2 * CH, HID), (HID, HID), (OUT, HID))
    fine_step, coarse_step, in_step, mid_step, out_step = pl.pallas_call(
        adam_kernel,
        out_shape=[jax.ShapeDtypeStruct(shape, F32) for shape in steps],
        in_specs=[whole] * len(found),
        out_specs=[far] * len(steps),
        scratch_shapes=[pltpu.VMEM(shape, F32) for shape in steps[2:]]
        + [pltpu.SemaphoreType.DMA((6,))],
        compiler_params=pltpu.CompilerParams(vmem_limit_bytes=8 * 1024 * 1024),
        name="adam",
    )(*found)
    return (
        fine_step.reshape(grid_fine.shape),
        coarse_step.reshape(grid_coarse.shape),
        in_step.T,
        mid_step[None],
        out_step,
    )


def solution(mesh):
    tile, copied = P(None, "row", "col"), P()
    placed = (P("row", "col", None), P(None, None, "row", "col"), tile, tile)
    placed += (copied,) * 3 + (tile,) * 4 + (copied,) * 6
    return jax.shard_map(
        shards,
        mesh=mesh,
        in_specs=placed,
        out_specs=(tile, tile, copied, copied, copied),
        check_vma=False,
    )
```
